128 devices in a mesh: row: 8 (over y, core), col: 16 (over x, z).
Axes of the slice: x: 4, y: 4, z: 4, core: 2. Of those that a mesh axis runs over, the one named last changes fastest.
Arguments:
- points: bfloat16 [262144, 512], P(('row', 'col')), may hold values from -6 to 6
- factor: bfloat16 [262144, 2048], P(('row', 'col')), may hold values from -0.15625 to 0.15625
- targets: bfloat16 [262144, 256], P(('row', 'col')), may hold values from -6 to 6
- pivot_slots: int32 [128, 8], P(('row', 'col')), may hold values from 0 to 2047, as said below
- pivot_counts: int32 [128], replicated, may hold values from 1 to 8, 512 in all
Outputs:
- new_columns: bfloat16 [512, 262144], P(None, ('row', 'col'))
- residual_next: float32 [262144, 256], P(('row', 'col'))
The draws below stay inside these ranges and needn't reach their ends.
Inputs may be any that keep to these rules, and one draw needn't show every extreme that they name: `pivot_slots`: each row holds 8 different local row numbers; row d's first pivot_counts[d] entries are device d's pivots, the rest are unused. `pivot_counts`: the counts sum to 512; one of them is 8.
All inputs are finite; a program needn't handle non-finite values.
Results may differ from the reference program's by a relative error of at most 0.0029.
Values may be sent and summed in bfloat16 or wider, within the bound.
A program may use at most 128 MiB of HBM per device.

```python
import math
import jax
import jax.numpy as jnp
import numpy as np
from jax import lax

D = 512
K_HELD = 2048
BLOCK = 512
NT = 256
PTS_DEV = 2048
CAP = 8
NPTS = 262144
DEVICES = 128


def draw_pivot_slots(key, part):
    device_keys = jax.random.split(jax.random.fold_in(key, 17), DEVICES)

    def device_draw(device_key):
        return jax.random.permutation(device_key, PTS_DEV)[:CAP]
    return jax.vmap(device_draw)(device_keys).astype(jnp.int32)


def spiked(array, own_key, source, target, parts, factor):
    def block_of(axis_at):
        return (jnp.arange(array.shape[axis_at]) // (array.shape[axis_at] // parts)).reshape((-1,) + (1,) * (array.ndim - 1 - axis_at))

    near = jax.random.permutation(own_key, parts)[block_of(target)]
    far = (block_of(target) + parts // 2) % parts
    return jnp.where((block_of(source) == near) | (block_of(source) == far), factor * array, array)


def level_of(rng, dims, pieces, low, high):
    gain = 1.0
    for dim, parts in pieces:
        steps = jax.random.uniform(jax.random.fold_in(jax.random.fold_in(rng, 6), dim), (parts,), jnp.float32, low / len(pieces), high / len(pieces))
        gain = gain * jnp.repeat(jnp.exp(steps), dims[dim] // parts).reshape((-1,) + (1,) * (len(dims) - 1 - dim))
    return gain


def profile(number_of, total, limit, skew):
    portions = [(1 << 20) // math.isqrt(grade ** skew) + 1 for grade in range(2, number_of + 1)]
    surplus, counts = total - limit - (number_of - 1), [1] * (number_of - 1)
    while surplus > 0:
        free = [i for i in range(number_of - 1) if counts[i] < limit]
        whole, remaining = sum([portions[i] for i in free]), surplus
        for i in free:
            addition = min(limit - counts[i], max(1, remaining * portions[i] // whole), surplus)
            counts[i] = counts[i] + addition
            surplus = surplus - addition
    return np.array([limit] + counts)


def ragged(own_key, number_of, total, reach, skew):
    if number_of == 2:
        one = jax.random.randint(own_key, (), max(1, total - reach), min(reach, total - 1) + 1)
        return jnp.stack([one, total - one])
    sizes = jnp.asarray(profile(number_of, total, reach, skew), jnp.int32)
    pairs = (number_of - 1) // 2
    giver, receiver = sizes[1:1 + 2 * pairs:2], sizes[2:2 + 2 * pairs:2]
    slack = jnp.minimum(giver - 1, reach - receiver)
    passed = jax.random.randint(jax.random.fold_in(own_key, 1), (pairs,), 0, 1 << 20) % (slack + 1)
    sizes = sizes.at[1:1 + 2 * pairs:2].set(giver - passed).at[2:2 + 2 * pairs:2].set(receiver + passed)
    return sizes[jax.random.permutation(jax.random.fold_in(own_key, 2), number_of)]


def gaussian(stream_key, extent, deviation, bound, cuts=(), held_as=jnp.bfloat16):
    result = jax.random.normal(stream_key, extent, jnp.float32) * deviation
    if len(cuts) > 0:
        result = level_of(stream_key, extent, cuts, -0.22, 0.18) * result
    return jnp.clip(result, min=-bound, max=bound).astype(held_as)


def gaussian_with(own_key, dims, spread, reach, pieces, heavy, kind=jnp.bfloat16):
    array = spread * jax.random.normal(own_key, dims, jnp.float32)
    if pieces:
        array = array * level_of(own_key, dims, pieces, -0.22, 0.18)
    return jnp.clip(spiked(array, jax.random.fold_in(own_key, 3), *heavy), -reach, reach).astype(kind)


def setup_inputs(seed: int = 0) -> dict:
    key_of = jax.random.split(jax.random.key(seed), 6)
    return {
        "points": gaussian(key_of[0], (NPTS, D), 1.0, 6.0, ((0, 128),)),
        "factor": gaussian_with(key_of[1], (NPTS, K_HELD), (10 * K_HELD) ** -0.5, 0.15625, ((0, 128),), (0, 1, 128, 5.5)),
        "targets": gaussian(key_of[2], (NPTS, NT), 1.0, 6.0, ((0, 128),)),
        "pivot_slots": draw_pivot_slots(jax.random.fold_in(key_of[5], 71), 0),
        "pivot_counts": ragged(key_of[4], DEVICES, BLOCK, CAP, 2).astype(jnp.int32),
    }


sharpness = 1.0
ridge_shift = 0.01
damping = 1.0
epsilon = 1e-06

def normalize(points):
    values = points.astype(jnp.float32)
    factor_scale = lax.rsqrt(lax.optimization_barrier(jnp.mean(values * values, axis=1, keepdims=True)) + epsilon)
    return (values * factor_scale).astype(jnp.bfloat16)

def kernel(left_rows, right_rows, feature_width):
    cosine = lax.dot_general(left_rows.astype(jnp.float32), right_rows.astype(jnp.float32), (((1,), (1,)), ((), ())), preferred_element_type=jnp.float32) / feature_width
    return jnp.exp(sharpness * (cosine - 1.0))

def compact_index(pivot_counts, block_size):
    owners_count = pivot_counts.shape[0]
    run_ends = jnp.cumsum(pivot_counts).astype(jnp.int32)
    run_starts = (run_ends - pivot_counts).astype(jnp.int32)
    position = jnp.arange(block_size, dtype=jnp.int32)
    owners = lax.optimization_barrier(jnp.sum((position[:, None] >= run_ends[None, :]).astype(jnp.int32), axis=1)).astype(jnp.int32)
    onehot = (owners[:, None] == jnp.arange(owners_count, dtype=jnp.int32)[None, :]).astype(jnp.int32)
    first_row = lax.optimization_barrier(jnp.sum(onehot * run_starts[None, :], axis=1)).astype(jnp.int32)
    return (owners, (position - first_row).astype(jnp.int32))

def block_factor(pivot_scaled, pivot_factor):
    intersection = lax.dot_general(pivot_factor.astype(jnp.float32), pivot_factor.astype(jnp.float32), (((1,), (1,)), ((), ())), preferred_element_type=jnp.float32)
    diag_shift = ridge_shift + jnp.max(lax.optimization_barrier(jnp.sum(jnp.abs(intersection), axis=1)))
    ridged = kernel(pivot_scaled, pivot_scaled, pivot_scaled.shape[1]) - intersection + diag_shift * jnp.eye(intersection.shape[0], dtype=jnp.float32)
    return jnp.linalg.cholesky(ridged)

def reference(points, factor, targets, pivot_slots, pivot_counts):
    scaled = normalize(points)
    owners, slot_index = compact_index(pivot_counts, BLOCK)
    local_rows = pivot_slots[owners, slot_index].astype(jnp.int32)
    pivot_rows = (owners * PTS_DEV + local_rows).astype(jnp.int32)
    pivot_scaled = jnp.take(scaled, pivot_rows, axis=0)
    pivot_factor = jnp.take(factor, pivot_rows, axis=0)
    lower_factor = block_factor(pivot_scaled, pivot_factor)

    def columns(block_number):
        start_row = (block_number * PTS_DEV).astype(jnp.int32)
        part_scaled = lax.dynamic_slice_in_dim(scaled, start_row, PTS_DEV, 0)
        part_factor = lax.dynamic_slice_in_dim(factor, start_row, PTS_DEV, 0)
        downdated = kernel(pivot_scaled, part_scaled, part_scaled.shape[1]) - lax.dot_general(pivot_factor.astype(jnp.float32), part_factor.astype(jnp.float32), (((1,), (1,)), ((), ())), preferred_element_type=jnp.float32)
        return lax.linalg.triangular_solve(lower_factor, downdated, left_side=True, lower=True).astype(jnp.bfloat16)
    new_blocks = lax.map(columns, jnp.arange(NPTS // PTS_DEV, dtype=jnp.int32))
    new_columns = jnp.transpose(new_blocks, (1, 0, 2)).reshape(BLOCK, NPTS)
    cross_terms = jnp.concatenate([lax.dot_general(factor.astype(jnp.float32), targets.astype(jnp.float32), (((0,), (0,)), ((), ())), preferred_element_type=jnp.float32), lax.dot_general(new_columns.astype(jnp.float32), targets.astype(jnp.float32), (((1,), (0,)), ((), ())), preferred_element_type=jnp.float32)], axis=0)
    col_norms = jnp.concatenate([lax.optimization_barrier(jnp.sum(jnp.square(factor.astype(jnp.float32)), axis=0)), lax.optimization_barrier(jnp.sum(jnp.square(new_columns.astype(jnp.float32)), axis=1))], axis=0)
    coefficients = (cross_terms / (col_norms + damping)[:, None]).astype(jnp.bfloat16)
    fitted = jnp.dot(factor.astype(jnp.float32), coefficients[:K_HELD].astype(jnp.float32), preferred_element_type=jnp.float32)
    fitted = fitted + lax.dot_general(new_columns.astype(jnp.float32), coefficients[K_HELD:].astype(jnp.float32), (((0,), (0,)), ((), ())), preferred_element_type=jnp.float32)
    residual_next = targets.astype(jnp.float32) - fitted
    return (new_columns, residual_next)
```

```python
import functools

import jax
import jax.numpy as jnp
from jax import lax
from jax.experimental import pallas as pl
from jax.experimental.pallas import tpu as pltpu
from jax.sharding import PartitionSpec as P

BLOCK = 512
PANEL = 128
SUB = 8
TILE_PTS = 512
MESH = pl.DeviceIdType.MESH
HIGHEST = lax.Precision.HIGHEST

ridge_shift = 0.01
damping = 1.0
epsilon = 1e-06


def joined_along(blocks, dim):
    shape = list(blocks.shape[1:])
    shape[dim] *= blocks.shape[0]
    return jnp.moveaxis(blocks, 0, dim).reshape(shape)


def sent_to_all(shard, axis):
    copies = jnp.broadcast_to(shard, (lax.axis_size(axis), *shard.shape))
    return lax.all_to_all(copies, axis, split_axis=0, concat_axis=0, tiled=True)


def normalize(points):
    values = points.astype(jnp.float32)
    factor_scale = lax.rsqrt(jnp.mean(values * values, axis=1, keepdims=True) + epsilon)
    return (values * factor_scale).astype(jnp.bfloat16)


def compact_index(pivot_counts, block_size):
    owners_count = pivot_counts.shape[0]
    run_ends = jnp.cumsum(pivot_counts).astype(jnp.int32)
    run_starts = (run_ends - pivot_counts).astype(jnp.int32)
    position = jnp.arange(block_size, dtype=jnp.int32)
    owners = jnp.sum((position[:, None] >= run_ends[None, :]).astype(jnp.int32), axis=1)
    owners = owners.astype(jnp.int32)
    onehot = (owners[:, None] == jnp.arange(owners_count, dtype=jnp.int32)[None, :]).astype(
        jnp.int32
    )
    first_row = jnp.sum(onehot * run_starts[None, :], axis=1)
    return (owners, position - first_row)


def dot_nt(a, b):
    return lax.dot_general(a, b, (((1,), (1,)), ((), ())), preferred_element_type=jnp.float32)


def dot_nn(a, b):
    return jnp.dot(a, b, preferred_element_type=jnp.float32)


def panel_inverse(block):
    groups = PANEL // SUB
    sub = lax.broadcasted_iota(jnp.int32, (SUB, PANEL), 0)
    lane = lax.broadcasted_iota(jnp.int32, (SUB, PANEL), 1)
    rows = [block[SUB * r : SUB * (r + 1), :] for r in range(groups)]
    inv = [(lane == sub + SUB * r).astype(jnp.float32) for r in range(groups)]

    def over_sublanes(value, k):
        return jnp.broadcast_to(value[k : k + 1, :], (SUB, PANEL))

    for m in range(groups):
        live = range(m, groups)
        cols = {
            (r, k): jnp.broadcast_to(
                rows[r][:, SUB * m + k : SUB * m + k + 1], (SUB, PANEL)
            )
            for r in live
            for k in range(SUB)
        }
        pivots = jnp.ones((SUB, PANEL), jnp.float32)
        for k in range(SUB):
            pivot = over_sublanes(cols[m, k], k)
            pivots = jnp.where(sub == k, pivot, pivots)
            scale = 1.0 / pivot
            ahead = {j: over_sublanes(cols[m, j], k) for j in range(k + 1, SUB)}
            row, inv_row = over_sublanes(rows[m], k), over_sublanes(inv[m], k)
            for r in live:
                c = cols[r, k] * scale
                if r == m:
                    c = jnp.where(sub > k, c, 0.0)
                for j in range(k + 1, SUB):
                    cols[r, j] = cols[r, j] - c * ahead[j]
                rows[r] = rows[r] - c * row
                inv[r] = inv[r] - c * inv_row
        inv[m] = inv[m] * lax.rsqrt(pivots)
    return jnp.concatenate(inv, axis=0)


def factor_kernel(ps_ref, pf_ref, hi_ref, lo_ref, a_ref, w_ref):
    total = jnp.zeros((1, BLOCK), jnp.float32)
    for r in range(BLOCK // PANEL):
        at = slice(r * PANEL, (r + 1) * PANEL)
        inter = dot_nt(pf_ref[at, :], pf_ref[...])
        total = total + jnp.sum(jnp.abs(inter), axis=0, keepdims=True)
        kern = jnp.exp(dot_nt(ps_ref[at, :], ps_ref[...]) / ps_ref.shape[1] - 1.0)
        a_ref[at, :] = kern - inter
    shift = ridge_shift + jnp.max(total)
    row_ids = lax.broadcasted_iota(jnp.int32, (PANEL, BLOCK), 0)
    lane_ids = lax.broadcasted_iota(jnp.int32, (PANEL, BLOCK), 1)
    for r in range(BLOCK // PANEL):
        at = slice(r * PANEL, (r + 1) * PANEL)
        eye = lane_ids == row_ids + r * PANEL
        a_ref[at, :] = a_ref[at, :] + jnp.where(eye, shift, 0.0)
        w_ref[at, :] = jnp.where(eye, 1.0, 0.0)

    @pl.loop(0, BLOCK // PANEL)
    def _(j):
        start = pl.multiple_of(j * PANEL, PANEL)
        at = pl.ds(start, PANEL)
        inv = panel_inverse(a_ref[at, at])
        right = jnp.dot(inv, a_ref[at, :], precision=HIGHEST, preferred_element_type=jnp.float32)
        right = jnp.where(lane_ids >= start + PANEL, right, 0.0)
        done = jnp.dot(inv, w_ref[at, :], precision=HIGHEST, preferred_element_type=jnp.float32)
        w_ref[at, :] = done
        for r in range(1, BLOCK // PANEL):
            rows = slice(r * PANEL, (r + 1) * PANEL)

            @pl.when(j < r)
            def _():
                left = right[:, rows].T
                a_ref[rows, :] = a_ref[rows, :] - jnp.dot(
                    left, right, precision=HIGHEST, preferred_element_type=jnp.float32
                )
                w_ref[rows, :] = w_ref[rows, :] - jnp.dot(
                    left, done, precision=HIGHEST, preferred_element_type=jnp.float32
                )

    high = w_ref[...].astype(jnp.bfloat16)
    hi_ref[...] = high
    lo_ref[...] = (w_ref[...] - high.astype(jnp.float32)).astype(jnp.bfloat16)


def block_factor(pivot_scaled, pivot_factor):
    square = jax.ShapeDtypeStruct((BLOCK, BLOCK), jnp.bfloat16)
    return pl.pallas_call(
        factor_kernel,
        out_shape=(square, square),
        in_specs=[pl.BlockSpec(memory_space=pltpu.VMEM)] * 2,
        out_specs=[pl.BlockSpec(memory_space=pltpu.VMEM)] * 2,
        scratch_shapes=[pltpu.VMEM((BLOCK, BLOCK), jnp.float32)] * 2,
        name="block_factor",
    )(pivot_scaled, pivot_factor)


def columns_kernel(
    points_ref, factor_ref, targets_ref, ps_ref, pf_ref, hi_ref, lo_ref,
    new_ref, cross_ref, norm_ref, acc_ref, fsq_ref, nsq_ref,
):
    step = pl.program_id(0)
    held = factor_ref.shape[1]

    @pl.when(step == 0)
    def _():
        acc_ref[...] = jnp.zeros_like(acc_ref)
        fsq_ref[...] = jnp.zeros_like(fsq_ref)
        nsq_ref[...] = jnp.zeros_like(nsq_ref)

    scaled = normalize(points_ref[...])
    factor = factor_ref[...]
    down = jnp.exp(dot_nt(ps_ref[...], scaled) / scaled.shape[1] - 1.0) - dot_nt(
        pf_ref[...], factor
    )
    down_hi = down.astype(jnp.bfloat16)
    down_lo = (down - down_hi.astype(jnp.float32)).astype(jnp.bfloat16)
    half = BLOCK // 2
    for top, wide in ((0, half), (half, BLOCK)):
        at = slice(top, top + half)
        new_ref[at, :] = (
            dot_nn(hi_ref[at, :wide], down_hi[:wide])
            + dot_nn(hi_ref[at, :wide], down_lo[:wide])
            + dot_nn(lo_ref[at, :wide], down_hi[:wide])
        ).astype(jnp.bfloat16)
    new = new_ref[...]
    turned = targets_ref[...].T
    acc_ref[:, :held] += dot_nn(turned, factor)
    acc_ref[:, held:] += dot_nt(turned, new)
    wide_factor = factor.astype(jnp.float32)
    fsq_ref[...] += jnp.sum(
        (wide_factor * wide_factor).reshape(-1, SUB, held), axis=0
    )
    wide_new = new.astype(jnp.float32)
    squares = wide_new * wide_new
    nsq = nsq_ref[...]
    for t in range(new.shape[1] // 128):
        nsq = nsq + squares[:, t * 128 : (t + 1) * 128]
    nsq_ref[...] = nsq

    @pl.when(step == pl.num_programs(0) - 1)
    def _():
        held_norm = jnp.sum(fsq_ref[...], axis=0, keepdims=True)
        new_norm = jnp.sum(nsq_ref[...].T, axis=0, keepdims=True)
        norms = jnp.concatenate([held_norm, new_norm], axis=1)
        for t in range(norms.shape[1] // 128):
            lanes = slice(t * 128, (t + 1) * 128)
            norm_ref[t : t + 1, :] = norms[:, lanes]
            piece = acc_ref[:, lanes].astype(jnp.bfloat16)
            cross_ref[:, t * 8 : (t + 1) * 8] = piece.reshape(2, 8, 16, 128)


def columns_call(points, factor, targets, pivot_scaled, pivot_factor, inv_hi, inv_lo):
    pts, held = factor.shape
    features, wanted = points.shape[1], targets.shape[1]
    tiles = (held + BLOCK) // 128
    whole = lambda i: (0, 0)
    once = pl.Buffered(1)
    return pl.pallas_call(
        columns_kernel,
        grid=(pts // TILE_PTS,),
        out_shape=(
            jax.ShapeDtypeStruct((BLOCK, pts), jnp.bfloat16),
            jax.ShapeDtypeStruct((2, tiles * 8, 16, 128), jnp.bfloat16),
            jax.ShapeDtypeStruct((tiles, 128), jnp.float32),
        ),
        in_specs=[
            pl.BlockSpec((TILE_PTS, features), lambda i: (i, 0)),
            pl.BlockSpec((TILE_PTS, held), lambda i: (i, 0)),
            pl.BlockSpec((TILE_PTS, wanted), lambda i: (i, 0)),
            pl.BlockSpec((BLOCK, features), whole, pipeline_mode=once),
            pl.BlockSpec((BLOCK, held), whole, pipeline_mode=once),
            pl.BlockSpec((BLOCK, BLOCK), whole, pipeline_mode=once),
            pl.BlockSpec((BLOCK, BLOCK), whole, pipeline_mode=once),
        ],
        out_specs=[
            pl.BlockSpec((BLOCK, TILE_PTS), lambda i: (0, i)),
            pl.BlockSpec((2, tiles * 8, 16, 128), lambda i: (0, 0, 0, 0)),
            pl.BlockSpec((tiles, 128), whole),
        ],
        scratch_shapes=[
            pltpu.VMEM((wanted, held + BLOCK), jnp.float32),
            pltpu.VMEM((SUB, held), jnp.float32),
            pltpu.VMEM((BLOCK, 128), jnp.float32),
        ],
        name="new_columns",
    )(points, factor, targets, pivot_scaled, pivot_factor, inv_hi, inv_lo)


PARTS = (((0, 1, 2), 0, 64), ((1, 2, 0), 64, 48), ((2, 0, 1), 112, 48))


def place():
    row, col = lax.axis_index("row"), lax.axis_index("col")
    core = lax.rem(row, 2)
    coords = (lax.div(col, 4), lax.div(row, 2), lax.rem(col, 4))
    return core, coords


def device_at(core, coords, axis=0, offset=0):
    x, y, z = (
        lax.rem(c + offset, 4) if (a == axis and offset) else c for a, c in enumerate(coords)
    )
    return (y * 2 + core, x * 4 + z)


def enter(core, coords):
    barrier = pltpu.get_barrier_semaphore()
    peers = [device_at(1 - core, coords)]
    peers += [device_at(core, coords, a, o) for a in range(3) for o in range(1, 4)]
    for peer in peers:
        pl.semaphore_signal(barrier, inc=1, device_id=peer, device_id_type=MESH)
    pl.semaphore_wait(barrier, len(peers))


def sums_kernel(
    x_ref, n_ref, out_ref, got0, sum0, out0, norm_got0, norm_sum, norm_got, coef, got_last,
    a0, a1, a2, b0, b1, b2, c0, c1, c2, s1, s2, s3, t1, t2, t3, u1, u2, u3,
    send, recv,
):
    core, coords = place()
    partner = device_at(1 - core, coords)
    enter(core, coords)
    count = [0]
    sent = []

    def start(src, dst, device):
        k = count[0]
        count[0] += 1
        copy = pltpu.make_async_remote_copy(
            src_ref=src, dst_ref=dst, send_sem=send.at[k], recv_sem=recv.at[k],
            device_id=device, device_id_type=MESH,
        )
        copy.start()
        sent.append(copy)
        return copy

    def arrive(copies):
        for copy in copies:
            copy.wait_recv()

    wide = lambda v: v.astype(jnp.float32)
    narrow = lambda v: v.astype(jnp.bfloat16)

    arrive([
        start(x_ref.at[1 - core], got0, partner),
        start(n_ref, norm_got0, partner),
    ])
    sum0[...] = wide(x_ref[core]) + wide(got0[...])
    out0[...] = narrow(sum0[...])
    norm_sum[0] = n_ref[...] + norm_got0[...]

    got = ((a0, a1, a2), (b0, b1, b2), (c0, c1, c2))
    sums = ((s1, s2, s3), (t1, t2, t3))
    outs = (u1, u2, u3)

    copies, starts = [], []
    for p, (order, base, size) in enumerate(PARTS):
        here, quarter = coords[order[0]], size // 4
        for o in range(1, 4):
            there = lax.rem(here + o, 4)
            copies.append(
                start(
                    out0.at[pl.ds(base + there * quarter, quarter)],
                    got[0][p].at[o - 1],
                    device_at(core, coords, order[0], o),
                )
            )
        starts.append(base + here * quarter)
    for o in range(1, 4):
        copies.append(
            start(norm_sum.at[0], norm_got.at[0, o - 1], device_at(core, coords, 0, o))
        )
    arrive(copies)
    for p, (order, base, size) in enumerate(PARTS):
        quarter = size // 4
        value = sum0[pl.ds(starts[p], quarter)]
        for o in range(3):
            value = value + wide(got[0][p][o])
        sums[0][p][...] = value
        outs[p][...] = narrow(value)
    norm_sum[1] = norm_sum[0] + norm_got[0, 0] + norm_got[0, 1] + norm_got[0, 2]

    copies = []
    for p, (order, base, size) in enumerate(PARTS):
        here, piece = coords[order[1]], size // 16
        for o in range(1, 4):
            there = lax.rem(here + o, 4)
            copies.append(
                start(
                    outs[p].at[pl.ds(there * piece, piece)],
                    got[1][p].at[o - 1],
                    device_at(core, coords, order[1], o),
                )
            )
        starts[p] = starts[p] + here * piece
    for o in range(1, 4):
        copies.append(
            start(norm_sum.at[1], norm_got.at[1, o - 1], device_at(core, coords, 1, o))
        )
    arrive(copies)
    for p, (order, base, size) in enumerate(PARTS):
        here, piece = coords[order[1]], size // 16
        value = sums[0][p][pl.ds(here * piece, piece)]
        for o in range(3):
            value = value + wide(got[1][p][o])
        sums[1][p][0] = value
        coef[pl.ds(starts[p], piece)] = narrow(value)
    norm_sum[2] = norm_sum[1] + norm_got[1, 0] + norm_got[1, 1] + norm_got[1, 2]

    copies = []
    for p, (order, base, size) in enumerate(PARTS):
        piece = size // 16
        for o in range(1, 4):
            copies.append(
                start(
                    coef.at[pl.ds(starts[p], piece)],
                    got[2][p].at[o - 1],
                    device_at(core, coords, order[2], o),
                )
            )
    for o in range(1, 4):
        copies.append(
            start(norm_sum.at[2], norm_got.at[2, o - 1], device_at(core, coords, 2, o))
        )
    arrive(copies)
    for copy in copies:
        copy.wait_send()
    del sent[-len(copies):]
    norm_sum[3] = norm_sum[2] + norm_got[2, 0] + norm_got[2, 1] + norm_got[2, 2]
    for p, (order, base, size) in enumerate(PARTS):
        piece = size // 16
        value = sums[1][p][0]
        for o in range(3):
            value = value + wide(got[2][p][o])
        for i in range(piece):
            tile = lax.div(starts[p] + i, 8)
            norm = norm_sum[3, pl.ds(tile, 1), :]
            coef[starts[p] + i] = narrow(value[i] / (norm + damping))

    for stage, parts_of in ((1, 16), (0, 4)):
        copies = []
        for p, (order, base, size) in enumerate(PARTS):
            piece = size // parts_of
            if stage == 0:
                starts[p] = base + coords[order[0]] * piece
            block = coef.at[pl.ds(starts[p], piece)]
            for o in range(1, 4):
                copies.append(start(block, block, device_at(core, coords, order[stage], o)))
        arrive(copies)
    last = start(coef, got_last, partner)
    out_ref[core] = coef[...]
    last.wait_recv()
    out_ref[1 - core] = got_last[...]
    for copy in sent:
        copy.wait_send()


def sums_call(cross, norms):
    blocks, tiles = cross.shape[1], norms.shape[0]
    bf, f32, vmem = jnp.bfloat16, jnp.float32, pltpu.VMEM
    piece = lambda lead, n, kind: vmem((*lead, n, 16, 128), kind)
    sizes = [size for _, _, size in PARTS]
    scratch = [
        vmem((blocks, 16, 128), bf), vmem((blocks, 16, 128), f32), vmem((blocks, 16, 128), bf),
        vmem((tiles, 128), f32), vmem((4, tiles, 128), f32), vmem((3, 3, tiles, 128), f32),
        vmem((blocks, 16, 128), bf), vmem((blocks, 16, 128), bf),
    ]
    scratch += [piece((3,), s // 4, bf) for s in sizes]
    scratch += [piece((3,), s // 16, bf) for s in sizes]
    scratch += [piece((3,), s // 16, bf) for s in sizes]
    scratch += [piece((), s // 4, f32) for s in sizes]
    scratch += [piece((1,), s // 16, f32) for s in sizes]
    scratch += [piece((), s // 4, bf) for s in sizes]
    copies = 2 + 12 * 3 + 9 * 2 + 1
    scratch += [pltpu.SemaphoreType.DMA((copies,))] * 2
    return pl.pallas_call(
        sums_kernel,
        out_shape=jax.ShapeDtypeStruct(cross.shape, bf),
        in_specs=[pl.BlockSpec(memory_space=vmem)] * 2,
        out_specs=pl.BlockSpec(memory_space=vmem),
        scratch_shapes=scratch,
        compiler_params=pltpu.CompilerParams(collective_id=1, has_side_effects=True),
        name="sums",
    )(cross, norms)


def residual_kernel(factor_ref, new_ref, targets_ref, coef_ref, out_ref, turned_ref):
    held = factor_ref.shape[1]

    @pl.when(pl.program_id(0) == 0)
    def _():
        for t in range(turned_ref.shape[1] // 128):
            lanes = slice(t * 128, (t + 1) * 128)
            turned_ref[:, lanes] = coef_ref[:, t * 8 : (t + 1) * 8].reshape(-1, 128)

    fitted = dot_nt(factor_ref[...], turned_ref[:, :held])
    fitted = fitted + dot_nn(turned_ref[:, held:], new_ref[...]).T
    out_ref[...] = targets_ref[...].astype(jnp.float32) - fitted


def residual_call(factor, new, targets, coef):
    pts, held = factor.shape
    wanted = targets.shape[1]
    return pl.pallas_call(
        residual_kernel,
        grid=(pts // TILE_PTS,),
        out_shape=jax.ShapeDtypeStruct((pts, wanted), jnp.float32),
        in_specs=[
            pl.BlockSpec((TILE_PTS, held), lambda i: (i, 0)),
            pl.BlockSpec((BLOCK, TILE_PTS), lambda i: (0, i)),
            pl.BlockSpec((TILE_PTS, wanted), lambda i: (i, 0)),
            pl.BlockSpec(coef.shape, lambda i: (0, 0, 0, 0), pipeline_mode=pl.Buffered(1)),
        ],
        out_specs=pl.BlockSpec((TILE_PTS, wanted), lambda i: (i, 0)),
        scratch_shapes=[pltpu.VMEM((wanted, held + BLOCK), jnp.bfloat16)],
        name="residual",
    )(factor, new, targets, coef)


def on_device(points, factor, targets, pivot_slots, pivot_counts):
    local_slots = pivot_slots[0]
    slot_cap = pivot_slots.shape[1]
    own = jnp.concatenate(
        [
            normalize(jnp.take(points, local_slots, axis=0)),
            jnp.take(factor, local_slots, axis=0),
        ],
        axis=1,
    )
    inner = joined_along(sent_to_all(own, "col"), 0)
    padded = lax.all_gather(inner, "row", axis=0, tiled=True)
    owners, slot_index = compact_index(pivot_counts, BLOCK)
    pivots = jnp.take(padded, owners * slot_cap + slot_index, axis=0)
    pivot_scaled = pivots[:, : points.shape[1]]
    pivot_factor = pivots[:, points.shape[1] :]
    inv_hi, inv_lo = block_factor(pivot_scaled, pivot_factor)
    new_columns, cross, norms = columns_call(
        points, factor, targets, pivot_scaled, pivot_factor, inv_hi, inv_lo
    )
    coef = sums_call(cross, norms)
    residual_next = residual_call(factor, new_columns, targets, coef)
    return (new_columns, residual_next)


def solution(mesh):
    return jax.shard_map(
        on_device,
        mesh=mesh,
        in_specs=(
            P(("row", "col"), None),
            P(("row", "col"), None),
            P(("row", "col"), None),
            P(("row", "col"), None),
            P(),
        ),
        out_specs=(P(None, ("row", "col")), P(("row", "col"), None)),
        check_vma=False,
    )
```

```python
import functools

import jax
import jax.numpy as jnp
from jax import lax
from jax.experimental import pallas as pl
from jax.experimental.pallas import tpu as pltpu
from jax.sharding import PartitionSpec as P

BLOCK = 512
PANEL = 128
SUB = 8
TILE_PTS = 512
MESH = pl.DeviceIdType.MESH
HIGHEST = lax.Precision.HIGHEST

ridge_shift = 0.01
damping = 1.0
epsilon = 1e-06


def normalize(points):
    values = points.astype(jnp.float32)
    factor_scale = lax.rsqrt(jnp.mean(values * values, axis=1, keepdims=True) + epsilon)
    return (values * factor_scale).astype(jnp.bfloat16)


def padded_positions(pivot_counts, slot_cap):
    starts = jnp.cumsum(pivot_counts) - pivot_counts
    slot = jnp.arange(slot_cap, dtype=jnp.int32)[None, :]
    place_of = jnp.where(slot < pivot_counts[:, None], starts[:, None] + slot, -1)
    return place_of.astype(jnp.int32).reshape(1, -1)


def dot_nt(a, b):
    return lax.dot_general(a, b, (((1,), (1,)), ((), ())), preferred_element_type=jnp.float32)


def dot_nn(a, b):
    return jnp.dot(a, b, preferred_element_type=jnp.float32)


PARTS = (((0, 1, 2), 0, 64), ((1, 2, 0), 64, 48), ((2, 0, 1), 112, 48))


def place():
    row, col = lax.axis_index("row"), lax.axis_index("col")
    core = lax.rem(row, 2)
    coords = (lax.div(col, 4), lax.div(row, 2), lax.rem(col, 4))
    return core, coords


def device_at(core, coords, axis=0, offset=0):
    x, y, z = (
        lax.rem(c + offset, 4) if (a == axis and offset) else c for a, c in enumerate(coords)
    )
    return (y * 2 + core, x * 4 + z)


def enter(core, coords):
    barrier = pltpu.get_barrier_semaphore()
    peers = [device_at(1 - core, coords)]
    peers += [device_at(core, coords, a, o) for a in range(3) for o in range(1, 4)]
    for peer in peers:
        pl.semaphore_signal(barrier, inc=1, device_id=peer, device_id_type=MESH)
    pl.semaphore_wait(barrier, len(peers))


def rows_kernel(slots_ref, points_ref, factor_ref, out_ref, pbuf, fbuf, psem, fsem):
    cap = pbuf.shape[0]
    copies = []
    for s in range(cap):
        base = pl.multiple_of(lax.div(slots_ref[0, s], SUB) * SUB, SUB)
        for src, buf, sem in ((points_ref, pbuf, psem), (factor_ref, fbuf, fsem)):
            copy = pltpu.make_async_copy(src.at[pl.ds(base, SUB), :], buf.at[s], sem.at[s])
            copy.start()
            copies.append(copy)
    for copy in copies:
        copy.wait()

    def picked(buf):
        sub = lax.broadcasted_iota(jnp.int32, buf.shape[1:], 0)
        out = jnp.zeros(buf.shape[1:], jnp.float32)
        for s in range(cap):
            offset = lax.rem(slots_ref[0, s], SUB)
            row = jnp.sum(
                jnp.where(sub == offset, buf[s].astype(jnp.float32), 0.0), axis=0, keepdims=True
            )
            out = jnp.where(sub == s, row, out)
        return out

    both = (normalize(picked(pbuf)), picked(fbuf).astype(jnp.bfloat16))
    t = 0
    for rows in both:
        for k in range(rows.shape[1] // 128):
            out_ref[t] = rows[:, k * 128 : (k + 1) * 128]
            t += 1


def rows_call(pivot_slots, points, factor):
    cap = pivot_slots.shape[1]
    features, held = points.shape[1], factor.shape[1]
    return pl.pallas_call(
        rows_kernel,
        out_shape=jax.ShapeDtypeStruct(((features + held) // 128, cap, 128), jnp.bfloat16),
        in_specs=[
            pl.BlockSpec(memory_space=pltpu.SMEM),
            pl.BlockSpec(memory_space=pl.ANY),
            pl.BlockSpec(memory_space=pl.ANY),
        ],
        out_specs=pl.BlockSpec(memory_space=pltpu.VMEM),
        scratch_shapes=[
            pltpu.VMEM((cap, SUB, features), jnp.bfloat16),
            pltpu.VMEM((cap, SUB, held), jnp.bfloat16),
            pltpu.SemaphoreType.DMA((cap,)),
            pltpu.SemaphoreType.DMA((cap,)),
        ],
        name="pivot_rows",
    )(pivot_slots, points, factor)


SPANS = ((0, 4, 7), (7, 11, 14), (14, 17, 20))


def gather_kernel(own_ref, out_ref, send, recv):
    core, coords = place()
    partner = device_at(1 - core, coords)
    enter(core, coords)
    count = [0]
    sent = []

    def start(src, dst, device):
        k = count[0]
        count[0] += 1
        copy = pltpu.make_async_remote_copy(
            src_ref=src, dst_ref=dst, send_sem=send.at[k], recv_sem=recv.at[k],
            device_id=device, device_id_type=MESH,
        )
        copy.start()
        sent.append(copy)
        return copy

    def region(low, high, whole=(), axis=None, at=None):
        x, y, z = (
            slice(None) if a in whole else (at if a == axis else c)
            for a, c in enumerate(coords)
        )
        return out_ref.at[y, core, x, z, low:high]

    def push(block, device):
        return start(block, block, device)

    first = []
    for (order, _, _), (low, _, high) in zip(PARTS, SPANS):
        first.append([
            start(own_ref.at[low:high], region(low, high), device_at(core, coords, order[0], o))
            for o in (2, 1, 3)
        ])
    x, y, z = coords
    out_ref[y, core, x, z] = own_ref[...]
    second = []
    for p, ((order, _, _), (low, _, high)) in enumerate(zip(PARTS, SPANS)):
        for copy in first[p]:
            copy.wait_recv()
        block = region(low, high, order[:1])
        second.append([
            push(block, device_at(core, coords, order[1], o)) for o in (2, 1, 3)
        ])
    third, across = [], []
    for p, ((order, _, _), (low, mid, high)) in enumerate(zip(PARTS, SPANS)):
        for copy in second[p]:
            copy.wait_recv()
        left, right = (device_at(core, coords, order[2], o) for o in (3, 1))
        halves = [region(a, b, order[:2]) for a, b in ((low, mid), (mid, high))]
        right_low = push(halves[0], right)
        left_high = push(halves[1], left)
        right_high = push(halves[1], right)
        left_low = push(halves[0], left)
        third.append((right_low, left_high, right_high, left_low))
        across.append(push(region(low, high, order[:2]), partner))
    relays = []
    for p, ((order, _, _), (low, mid, high)) in enumerate(zip(PARTS, SPANS)):
        axis = order[2]
        before, after = (lax.rem(coords[axis] + o, 4) for o in (3, 1))
        left, right = (device_at(core, coords, axis, o) for o in (3, 1))
        third[p][0].wait_recv()
        one = push(region(low, mid, order[:2], axis, before), right)
        third[p][1].wait_recv()
        relays.append((one, push(region(mid, high, order[:2], axis, after), left)))
    for p, ((order, _, _), (low, mid, high)) in enumerate(zip(PARTS, SPANS)):
        axis = order[2]
        before, after = (lax.rem(coords[axis] + o, 4) for o in (3, 1))
        third[p][2].wait_recv()
        across.append(push(region(low, high, order[:2], axis, before), partner))
        third[p][3].wait_recv()
        across.append(push(region(low, high, order[:2], axis, after), partner))
    for p, ((order, _, _), (low, mid, high)) in enumerate(zip(PARTS, SPANS)):
        axis = order[2]
        opposite = lax.rem(coords[axis] + 2, 4)
        for copy, (a, b) in zip(relays[p], ((low, mid), (mid, high))):
            copy.wait_recv()
            across.append(push(region(a, b, order[:2], axis, opposite), partner))
    for copy in across:
        copy.wait_recv()
    for copy in sent:
        copy.wait_send()


def gather_call(own):
    copies = 9 + 9 + 12 + 3 + 6 + 6 + 6
    out = pl.pallas_call(
        gather_kernel,
        out_shape=jax.ShapeDtypeStruct((4, 2, 4, 4, *own.shape), own.dtype),
        in_specs=[pl.BlockSpec(memory_space=pltpu.VMEM)],
        out_specs=pl.BlockSpec(memory_space=pltpu.VMEM),
        scratch_shapes=[pltpu.SemaphoreType.DMA((copies,))] * 2,
        compiler_params=pltpu.CompilerParams(collective_id=2, has_side_effects=True),
        name="gather_rows",
    )(own)
    return out.reshape(128, *own.shape)


def panel_inverse(block):
    groups = PANEL // SUB
    sub = lax.broadcasted_iota(jnp.int32, (SUB, PANEL), 0)
    lane = lax.broadcasted_iota(jnp.int32, (SUB, PANEL), 1)
    rows = [block[SUB * r : SUB * (r + 1), :] for r in range(groups)]
    inv = [(lane == sub + SUB * r).astype(jnp.float32) for r in range(groups)]

    def over_sublanes(value, k):
        return jnp.broadcast_to(value[k : k + 1, :], (SUB, PANEL))

    for m in range(groups):
        live = range(m, groups)
        cols = {
            (r, k): jnp.broadcast_to(
                rows[r][:, SUB * m + k : SUB * m + k + 1], (SUB, PANEL)
            )
            for r in live
            for k in range(SUB)
        }
        pivots = jnp.ones((SUB, PANEL), jnp.float32)
        for k in range(SUB):
            pivot = over_sublanes(cols[m, k], k)
            pivots = jnp.where(sub == k, pivot, pivots)
            scale = 1.0 / pivot
            ahead = {j: over_sublanes(cols[m, j], k) for j in range(k + 1, SUB)}
            row, inv_row = over_sublanes(rows[m], k), over_sublanes(inv[m], k)
            for r in live:
                c = cols[r, k] * scale
                if r == m:
                    c = jnp.where(sub > k, c, 0.0)
                for j in range(k + 1, SUB):
                    cols[r, j] = cols[r, j] - c * ahead[j]
                rows[r] = rows[r] - c * row
                inv[r] = inv[r] - c * inv_row
        inv[m] = inv[m] * lax.rsqrt(pivots)
    return jnp.concatenate(inv, axis=0)


def factor_kernel(pad_ref, pos_ref, ps_ref, pf_ref, hi_ref, lo_ref, a_ref, w_ref, sel_ref):
    padded = pos_ref.shape[1]
    sel_ref[...] = jnp.where(
        lax.broadcasted_iota(jnp.int32, (BLOCK, padded), 0) == pos_ref[...], 1.0, 0.0
    ).astype(jnp.bfloat16)
    ahead = ps_ref.shape[1] // 128
    for t in range(0, pad_ref.shape[1], 2):
        pair = [
            pad_ref[:, k].astype(jnp.float32).reshape(padded, 128).astype(jnp.bfloat16)
            for k in (t, t + 1)
        ]
        rows = dot_nn(sel_ref[...], jnp.concatenate(pair, axis=1)).astype(jnp.bfloat16)
        if t < ahead:
            ps_ref[:, t * 128 : (t + 2) * 128] = rows
        else:
            pf_ref[:, (t - ahead) * 128 : (t - ahead + 2) * 128] = rows
    total = jnp.zeros((1, BLOCK), jnp.float32)
    for r in range(BLOCK // PANEL):
        at = slice(r * PANEL, (r + 1) * PANEL)
        inter = dot_nt(pf_ref[at, :], pf_ref[...])
        total = total + jnp.sum(jnp.abs(inter), axis=0, keepdims=True)
        kern = jnp.exp(dot_nt(ps_ref[at, :], ps_ref[...]) / ps_ref.shape[1] - 1.0)
        a_ref[at, :] = kern - inter
    shift = ridge_shift + jnp.max(total)
    row_ids = lax.broadcasted_iota(jnp.int32, (PANEL, BLOCK), 0)
    lane_ids = lax.broadcasted_iota(jnp.int32, (PANEL, BLOCK), 1)
    for r in range(BLOCK // PANEL):
        at = slice(r * PANEL, (r + 1) * PANEL)
        eye = lane_ids == row_ids + r * PANEL
        a_ref[at, :] = a_ref[at, :] + jnp.where(eye, shift, 0.0)
        w_ref[at, :] = jnp.where(eye, 1.0, 0.0)

    @pl.loop(0, BLOCK // PANEL)
    def _(j):
        start = pl.multiple_of(j * PANEL, PANEL)
        at = pl.ds(start, PANEL)
        inv = panel_inverse(a_ref[at, at])
        right = jnp.dot(inv, a_ref[at, :], precision=HIGHEST, preferred_element_type=jnp.float32)
        right = jnp.where(lane_ids >= start + PANEL, right, 0.0)
        done = jnp.dot(inv, w_ref[at, :], precision=HIGHEST, preferred_element_type=jnp.float32)
        w_ref[at, :] = done
        for r in range(1, BLOCK // PANEL):
            rows = slice(r * PANEL, (r + 1) * PANEL)

            @pl.when(j < r)
            def _():
                left = right[:, rows].T
                a_ref[rows, :] = a_ref[rows, :] - jnp.dot(
                    left, right, precision=HIGHEST, preferred_element_type=jnp.float32
                )
                w_ref[rows, :] = w_ref[rows, :] - jnp.dot(
                    left, done, precision=HIGHEST, preferred_element_type=jnp.float32
                )

    high = w_ref[...].astype(jnp.bfloat16)
    hi_ref[...] = high
    lo_ref[...] = (w_ref[...] - high.astype(jnp.float32)).astype(jnp.bfloat16)


def block_factor(padded, positions, features):
    held = padded.shape[1] * 128 - features
    bf = jnp.bfloat16
    return pl.pallas_call(
        factor_kernel,
        out_shape=(
            jax.ShapeDtypeStruct((BLOCK, features), bf),
            jax.ShapeDtypeStruct((BLOCK, held), bf),
            jax.ShapeDtypeStruct((BLOCK, BLOCK), bf),
            jax.ShapeDtypeStruct((BLOCK, BLOCK), bf),
        ),
        in_specs=[pl.BlockSpec(memory_space=pltpu.VMEM)] * 2,
        out_specs=[pl.BlockSpec(memory_space=pltpu.VMEM)] * 4,
        scratch_shapes=[pltpu.VMEM((BLOCK, BLOCK), jnp.float32)] * 2
        + [pltpu.VMEM((BLOCK, positions.shape[1]), bf)],
        name="block_factor",
    )(padded, positions)


def columns_kernel(
    points_ref, factor_ref, targets_ref, ps_ref, pf_ref, hi_ref, lo_ref,
    new_ref, cross_ref, norm_ref, acc_ref, fsq_ref, nsq_ref,
):
    step = pl.program_id(0)
    held = factor_ref.shape[1]

    @pl.when(step == 0)
    def _():
        acc_ref[...] = jnp.zeros_like(acc_ref)
        fsq_ref[...] = jnp.zeros_like(fsq_ref)
        nsq_ref[...] = jnp.zeros_like(nsq_ref)

    scaled = normalize(points_ref[...])
    factor = factor_ref[...]
    down = jnp.exp(dot_nt(ps_ref[...], scaled) / scaled.shape[1] - 1.0) - dot_nt(
        pf_ref[...], factor
    )
    down_hi = down.astype(jnp.bfloat16)
    down_lo = (down - down_hi.astype(jnp.float32)).astype(jnp.bfloat16)
    half = BLOCK // 2
    for top, wide in ((0, half), (half, BLOCK)):
        at = slice(top, top + half)
        new_ref[at, :] = (
            dot_nn(hi_ref[at, :wide], down_hi[:wide])
            + dot_nn(hi_ref[at, :wide], down_lo[:wide])
            + dot_nn(lo_ref[at, :wide], down_hi[:wide])
        ).astype(jnp.bfloat16)
    new = new_ref[...]
    turned = targets_ref[...].T
    acc_ref[:, :held] += dot_nn(turned, factor)
    acc_ref[:, held:] += dot_nt(turned, new)
    wide_factor = factor.astype(jnp.float32)
    fsq_ref[...] += jnp.sum(
        (wide_factor * wide_factor).reshape(-1, SUB, held), axis=0
    )
    wide_new = new.astype(jnp.float32)
    squares = wide_new * wide_new
    nsq = nsq_ref[...]
    for t in range(new.shape[1] // 128):
        nsq = nsq + squares[:, t * 128 : (t + 1) * 128]
    nsq_ref[...] = nsq

    @pl.when(step == pl.num_programs(0) - 1)
    def _():
        held_norm = jnp.sum(fsq_ref[...], axis=0, keepdims=True)
        new_norm = jnp.sum(nsq_ref[...].T, axis=0, keepdims=True)
        norms = jnp.concatenate([held_norm, new_norm], axis=1)
        for t in range(norms.shape[1] // 128):
            lanes = slice(t * 128, (t + 1) * 128)
            norm_ref[t : t + 1, :] = norms[:, lanes]
            piece = acc_ref[:, lanes].astype(jnp.bfloat16)
            cross_ref[:, t * 8 : (t + 1) * 8] = piece.reshape(2, 8, 16, 128)


def columns_call(points, factor, targets, pivot_scaled, pivot_factor, inv_hi, inv_lo):
    pts, held = factor.shape
    features, wanted = points.shape[1], targets.shape[1]
    tiles = (held + BLOCK) // 128
    whole = lambda i: (0, 0)
    once = pl.Buffered(1)
    return pl.pallas_call(
        columns_kernel,
        grid=(pts // TILE_PTS,),
        out_shape=(
            jax.ShapeDtypeStruct((BLOCK, pts), jnp.bfloat16),
            jax.ShapeDtypeStruct((2, tiles * 8, 16, 128), jnp.bfloat16),
            jax.ShapeDtypeStruct((tiles, 128), jnp.float32),
        ),
        in_specs=[
            pl.BlockSpec((TILE_PTS, features), lambda i: (i, 0)),
            pl.BlockSpec((TILE_PTS, held), lambda i: (i, 0)),
            pl.BlockSpec((TILE_PTS, wanted), lambda i: (i, 0)),
            pl.BlockSpec((BLOCK, features), whole, pipeline_mode=once),
            pl.BlockSpec((BLOCK, held), whole, pipeline_mode=once),
            pl.BlockSpec((BLOCK, BLOCK), whole, pipeline_mode=once),
            pl.BlockSpec((BLOCK, BLOCK), whole, pipeline_mode=once),
        ],
        out_specs=[
            pl.BlockSpec((BLOCK, TILE_PTS), lambda i: (0, i)),
            pl.BlockSpec((2, tiles * 8, 16, 128), lambda i: (0, 0, 0, 0)),
            pl.BlockSpec((tiles, 128), whole),
        ],
        scratch_shapes=[
            pltpu.VMEM((wanted, held + BLOCK), jnp.float32),
            pltpu.VMEM((SUB, held), jnp.float32),
            pltpu.VMEM((BLOCK, 128), jnp.float32),
        ],
        name="new_columns",
    )(points, factor, targets, pivot_scaled, pivot_factor, inv_hi, inv_lo)


def sums_kernel(
    x_ref, n_ref, out_ref, got0, sum0, out0, norm_got0, norm_sum, norm_got, coef, got_last,
    a0, a1, a2, b0, b1, b2, c0, c1, c2, s1, s2, s3, t1, t2, t3, u1, u2, u3,
    send, recv,
):
    core, coords = place()
    partner = device_at(1 - core, coords)
    enter(core, coords)
    count = [0]
    sent = []

    def start(src, dst, device):
        k = count[0]
        count[0] += 1
        copy = pltpu.make_async_remote_copy(
            src_ref=src, dst_ref=dst, send_sem=send.at[k], recv_sem=recv.at[k],
            device_id=device, device_id_type=MESH,
        )
        copy.start()
        sent.append(copy)
        return copy

    def arrive(copies):
        for copy in copies:
            copy.wait_recv()

    wide = lambda v: v.astype(jnp.float32)
    narrow = lambda v: v.astype(jnp.bfloat16)

    arrive([
        start(x_ref.at[1 - core], got0, partner),
        start(n_ref, norm_got0, partner),
    ])
    sum0[...] = wide(x_ref[core]) + wide(got0[...])
    out0[...] = narrow(sum0[...])
    norm_sum[0] = n_ref[...] + norm_got0[...]

    got = ((a0, a1, a2), (b0, b1, b2), (c0, c1, c2))
    sums = ((s1, s2, s3), (t1, t2, t3))
    outs = (u1, u2, u3)

    copies, starts = [], []
    for p, (order, base, size) in enumerate(PARTS):
        here, quarter = coords[order[0]], size // 4
        for o in range(1, 4):
            there = lax.rem(here + o, 4)
            copies.append(
                start(
                    out0.at[pl.ds(base + there * quarter, quarter)],
                    got[0][p].at[o - 1],
                    device_at(core, coords, order[0], o),
                )
            )
        starts.append(base + here * quarter)
    for o in range(1, 4):
        copies.append(
            start(norm_sum.at[0], norm_got.at[0, o - 1], device_at(core, coords, 0, o))
        )
    arrive(copies)
    for p, (order, base, size) in enumerate(PARTS):
        quarter = size // 4
        value = sum0[pl.ds(starts[p], quarter)]
        for o in range(3):
            value = value + wide(got[0][p][o])
        sums[0][p][...] = value
        outs[p][...] = narrow(value)
    norm_sum[1] = norm_sum[0] + norm_got[0, 0] + norm_got[0, 1] + norm_got[0, 2]

    copies = []
    for p, (order, base, size) in enumerate(PARTS):
        here, piece = coords[order[1]], size // 16
        for o in range(1, 4):
            there = lax.rem(here + o, 4)
            copies.append(
                start(
                    outs[p].at[pl.ds(there * piece, piece)],
                    got[1][p].at[o - 1],
                    device_at(core, coords, order[1], o),
                )
            )
        starts[p] = starts[p] + here * piece
    for o in range(1, 4):
        copies.append(
            start(norm_sum.at[1], norm_got.at[1, o - 1], device_at(core, coords, 1, o))
        )
    arrive(copies)
    for p, (order, base, size) in enumerate(PARTS):
        here, piece = coords[order[1]], size // 16
        value = sums[0][p][pl.ds(here * piece, piece)]
        for o in range(3):
            value = value + wide(got[1][p][o])
        sums[1][p][0] = value
        coef[pl.ds(starts[p], piece)] = narrow(value)
    norm_sum[2] = norm_sum[1] + norm_got[1, 0] + norm_got[1, 1] + norm_got[1, 2]

    copies = []
    for p, (order, base, size) in enumerate(PARTS):
        piece = size // 16
        for o in range(1, 4):
            copies.append(
                start(
                    coef.at[pl.ds(starts[p], piece)],
                    got[2][p].at[o - 1],
                    device_at(core, coords, order[2], o),
                )
            )
    for o in range(1, 4):
        copies.append(
            start(norm_sum.at[2], norm_got.at[2, o - 1], device_at(core, coords, 2, o))
        )
    arrive(copies)
    for copy in copies:
        copy.wait_send()
    del sent[-len(copies):]
    norm_sum[3] = norm_sum[2] + norm_got[2, 0] + norm_got[2, 1] + norm_got[2, 2]
    for p, (order, base, size) in enumerate(PARTS):
        piece = size // 16
        value = sums[1][p][0]
        for o in range(3):
            value = value + wide(got[2][p][o])
        for i in range(piece):
            tile = lax.div(starts[p] + i, 8)
            norm = norm_sum[3, pl.ds(tile, 1), :]
            coef[starts[p] + i] = narrow(value[i] / (norm + damping))

    for stage, parts_of in ((1, 16), (0, 4)):
        copies = []
        for p, (order, base, size) in enumerate(PARTS):
            piece = size // parts_of
            if stage == 0:
                starts[p] = base + coords[order[0]] * piece
            block = coef.at[pl.ds(starts[p], piece)]
            for o in range(1, 4):
                copies.append(start(block, block, device_at(core, coords, order[stage], o)))
        arrive(copies)
    last = start(coef, got_last, partner)
    out_ref[core] = coef[...]
    last.wait_recv()
    out_ref[1 - core] = got_last[...]
    for copy in sent:
        copy.wait_send()


def sums_call(cross, norms):
    blocks, tiles = cross.shape[1], norms.shape[0]
    bf, f32, vmem = jnp.bfloat16, jnp.float32, pltpu.VMEM
    piece = lambda lead, n, kind: vmem((*lead, n, 16, 128), kind)
    sizes = [size for _, _, size in PARTS]
    scratch = [
        vmem((blocks, 16, 128), bf), vmem((blocks, 16, 128), f32), vmem((blocks, 16, 128), bf),
        vmem((tiles, 128), f32), vmem((4, tiles, 128), f32), vmem((3, 3, tiles, 128), f32),
        vmem((blocks, 16, 128), bf), vmem((blocks, 16, 128), bf),
    ]
    scratch += [piece((3,), s // 4, bf) for s in sizes]
    scratch += [piece((3,), s // 16, bf) for s in sizes]
    scratch += [piece((3,), s // 16, bf) for s in sizes]
    scratch += [piece((), s // 4, f32) for s in sizes]
    scratch += [piece((1,), s // 16, f32) for s in sizes]
    scratch += [piece((), s // 4, bf) for s in sizes]
    copies = 2 + 12 * 3 + 9 * 2 + 1
    scratch += [pltpu.SemaphoreType.DMA((copies,))] * 2
    return pl.pallas_call(
        sums_kernel,
        out_shape=jax.ShapeDtypeStruct(cross.shape, bf),
        in_specs=[pl.BlockSpec(memory_space=vmem)] * 2,
        out_specs=pl.BlockSpec(memory_space=vmem),
        scratch_shapes=scratch,
        compiler_params=pltpu.CompilerParams(collective_id=1, has_side_effects=True),
        name="sums",
    )(cross, norms)


def residual_kernel(factor_ref, new_ref, targets_ref, coef_ref, out_ref, turned_ref):
    held = factor_ref.shape[1]

    @pl.when(pl.program_id(0) == 0)
    def _():
        for t in range(turned_ref.shape[1] // 128):
            lanes = slice(t * 128, (t + 1) * 128)
            turned_ref[:, lanes] = coef_ref[:, t * 8 : (t + 1) * 8].reshape(-1, 128)

    fitted = dot_nt(factor_ref[...], turned_ref[:, :held])
    fitted = fitted + dot_nn(turned_ref[:, held:], new_ref[...]).T
    out_ref[...] = targets_ref[...].astype(jnp.float32) - fitted


def residual_call(factor, new, targets, coef):
    pts, held = factor.shape
    wanted = targets.shape[1]
    return pl.pallas_call(
        residual_kernel,
        grid=(pts // TILE_PTS,),
        out_shape=jax.ShapeDtypeStruct((pts, wanted), jnp.float32),
        in_specs=[
            pl.BlockSpec((TILE_PTS, held), lambda i: (i, 0)),
            pl.BlockSpec((BLOCK, TILE_PTS), lambda i: (0, i)),
            pl.BlockSpec((TILE_PTS, wanted), lambda i: (i, 0)),
            pl.BlockSpec(coef.shape, lambda i: (0, 0, 0, 0), pipeline_mode=pl.Buffered(1)),
        ],
        out_specs=pl.BlockSpec((TILE_PTS, wanted), lambda i: (i, 0)),
        scratch_shapes=[pltpu.VMEM((wanted, held + BLOCK), jnp.bfloat16)],
        name="residual",
    )(factor, new, targets, coef)


def on_device(points, factor, targets, pivot_slots, pivot_counts):
    own = rows_call(pivot_slots, points, factor)
    padded = gather_call(own)
    positions = padded_positions(pivot_counts, pivot_slots.shape[1])
    pivot_scaled, pivot_factor, inv_hi, inv_lo = block_factor(
        padded, positions, points.shape[1]
    )
    new_columns, cross, norms = columns_call(
        points, factor, targets, pivot_scaled, pivot_factor, inv_hi, inv_lo
    )
    coef = sums_call(cross, norms)
    residual_next = residual_call(factor, new_columns, targets, coef)
    return (new_columns, residual_next)


def solution(mesh):
    return jax.shard_map(
        on_device,
        mesh=mesh,
        in_specs=(
            P(("row", "col"), None),
            P(("row", "col"), None),
            P(("row", "col"), None),
            P(("row", "col"), None),
            P(),
        ),
        out_specs=(P(None, ("row", "col")), P(("row", "col"), None)),
        check_vma=False,
    )
```

```python
import functools

import jax
import jax.numpy as jnp
from jax import lax
from jax.experimental import pallas as pl
from jax.experimental.pallas import tpu as pltpu
from jax.sharding import PartitionSpec as P

BLOCK = 512
PANEL = 128
SUB = 8
TILE_PTS = 512
MESH = pl.DeviceIdType.MESH
HIGHEST = lax.Precision.HIGHEST

ridge_shift = 0.01
damping = 1.0
epsilon = 1e-06


def normalize(points):
    values = points.astype(jnp.float32)
    factor_scale = lax.rsqrt(jnp.mean(values * values, axis=1, keepdims=True) + epsilon)
    return (values * factor_scale).astype(jnp.bfloat16)


def padded_positions(pivot_counts, slot_cap):
    starts = jnp.cumsum(pivot_counts) - pivot_counts
    slot = jnp.arange(slot_cap, dtype=jnp.int32)[None, :]
    place_of = jnp.where(slot < pivot_counts[:, None], starts[:, None] + slot, -1)
    return place_of.astype(jnp.int32).reshape(1, -1)


def dot_nt(a, b):
    return lax.dot_general(a, b, (((1,), (1,)), ((), ())), preferred_element_type=jnp.float32)


def dot_nn(a, b):
    return jnp.dot(a, b, preferred_element_type=jnp.float32)


def put_blocks(acc, norms, cross_ref, norm_ref):
    for t in range(norms.shape[1] // 128):
        lanes = slice(t * 128, (t + 1) * 128)
        norm_ref[t : t + 1, :] = norms[:, lanes]
        cross_ref[:, t * 8 : (t + 1) * 8] = (
            acc[:, lanes].astype(jnp.bfloat16).reshape(2, 8, 16, 128)
        )


PARTS = (((0, 1, 2), 0, 64), ((1, 2, 0), 64, 48), ((2, 0, 1), 112, 48))


def place():
    row, col = lax.axis_index("row"), lax.axis_index("col")
    core = lax.rem(row, 2)
    coords = (lax.div(col, 4), lax.div(row, 2), lax.rem(col, 4))
    return core, coords


def device_at(core, coords, axis=0, offset=0):
    x, y, z = (
        lax.rem(c + offset, 4) if (a == axis and offset) else c for a, c in enumerate(coords)
    )
    return (y * 2 + core, x * 4 + z)


def enter(core, coords):
    barrier = pltpu.get_barrier_semaphore()
    peers = [device_at(1 - core, coords)]
    peers += [device_at(core, coords, a, o) for a in range(3) for o in range(1, 4)]
    for peer in peers:
        pl.semaphore_signal(barrier, inc=1, device_id=peer, device_id_type=MESH)
    pl.semaphore_wait(barrier, len(peers))


def rows_kernel(slots_ref, points_ref, factor_ref, out_ref, pbuf, fbuf, psem, fsem):
    cap = pbuf.shape[0]
    copies = []
    for s in range(cap):
        base = pl.multiple_of(lax.div(slots_ref[0, s], SUB) * SUB, SUB)
        for src, buf, sem in ((points_ref, pbuf, psem), (factor_ref, fbuf, fsem)):
            copy = pltpu.make_async_copy(src.at[pl.ds(base, SUB), :], buf.at[s], sem.at[s])
            copy.start()
            copies.append(copy)
    for copy in copies:
        copy.wait()

    def picked(buf):
        sub = lax.broadcasted_iota(jnp.int32, buf.shape[1:], 0)
        out = jnp.zeros(buf.shape[1:], jnp.float32)
        for s in range(cap):
            offset = lax.rem(slots_ref[0, s], SUB)
            row = jnp.sum(
                jnp.where(sub == offset, buf[s].astype(jnp.float32), 0.0), axis=0, keepdims=True
            )
            out = jnp.where(sub == s, row, out)
        return out

    both = (normalize(picked(pbuf)), picked(fbuf).astype(jnp.bfloat16))
    t = 0
    for rows in both:
        for k in range(rows.shape[1] // 128):
            out_ref[t] = rows[:, k * 128 : (k + 1) * 128]
            t += 1


def rows_call(pivot_slots, points, factor):
    cap = pivot_slots.shape[1]
    features, held = points.shape[1], factor.shape[1]
    return pl.pallas_call(
        rows_kernel,
        out_shape=jax.ShapeDtypeStruct(((features + held) // 128, cap, 128), jnp.bfloat16),
        in_specs=[
            pl.BlockSpec(memory_space=pltpu.SMEM),
            pl.BlockSpec(memory_space=pl.ANY),
            pl.BlockSpec(memory_space=pl.ANY),
        ],
        out_specs=pl.BlockSpec(memory_space=pltpu.VMEM),
        scratch_shapes=[
            pltpu.VMEM((cap, SUB, features), jnp.bfloat16),
            pltpu.VMEM((cap, SUB, held), jnp.bfloat16),
            pltpu.SemaphoreType.DMA((cap,)),
            pltpu.SemaphoreType.DMA((cap,)),
        ],
        name="pivot_rows",
    )(pivot_slots, points, factor)


SPANS = ((0, 4, 7), (7, 11, 14), (14, 17, 20))


def gather_kernel(
    own_ref, targets_ref, factor_ref, out_ref, cross_ref, norm_ref, fbuf, acc_ref, send, recv, fsem
):
    chunks = fbuf.shape[0]
    loads = []
    for i in range(chunks):
        at = pl.ds(i * TILE_PTS, TILE_PTS)
        load = pltpu.make_async_copy(factor_ref.at[at, :], fbuf.at[i], fsem.at[i])
        load.start()
        loads.append(load)
    squares = [jnp.zeros((SUB, fbuf.shape[2]), jnp.float32)]

    def add_chunk(i):
        loads[i].wait()
        value = dot_nn(targets_ref[i * TILE_PTS : (i + 1) * TILE_PTS, :].T, fbuf[i])
        acc_ref[...] = value if i == 0 else acc_ref[...] + value
        wide = fbuf[i].astype(jnp.float32)
        squares[0] = squares[0] + jnp.sum((wide * wide).reshape(-1, SUB, wide.shape[1]), axis=0)

    core, coords = place()
    partner = device_at(1 - core, coords)
    enter(core, coords)
    count = [0]
    sent = []

    def start(src, dst, device):
        k = count[0]
        count[0] += 1
        copy = pltpu.make_async_remote_copy(
            src_ref=src, dst_ref=dst, send_sem=send.at[k], recv_sem=recv.at[k],
            device_id=device, device_id_type=MESH,
        )
        copy.start()
        sent.append(copy)
        return copy

    def region(low, high, whole=(), axis=None, at=None):
        x, y, z = (
            slice(None) if a in whole else (at if a == axis else c)
            for a, c in enumerate(coords)
        )
        return out_ref.at[y, core, x, z, low:high]

    def push(block, device):
        return start(block, block, device)

    first = []
    for (order, _, _), (low, _, high) in zip(PARTS, SPANS):
        first.append([
            start(own_ref.at[low:high], region(low, high), device_at(core, coords, order[0], o))
            for o in (2, 1, 3)
        ])
    x, y, z = coords
    out_ref[y, core, x, z] = own_ref[...]
    add_chunk(0)
    second = []
    for p, ((order, _, _), (low, _, high)) in enumerate(zip(PARTS, SPANS)):
        for copy in first[p]:
            copy.wait_recv()
        block = region(low, high, order[:1])
        second.append([
            push(block, device_at(core, coords, order[1], o)) for o in (2, 1, 3)
        ])
    add_chunk(1)
    add_chunk(2)
    third, across = [], []
    for p, ((order, _, _), (low, mid, high)) in enumerate(zip(PARTS, SPANS)):
        for copy in second[p]:
            copy.wait_recv()
        left, right = (device_at(core, coords, order[2], o) for o in (3, 1))
        halves = [region(a, b, order[:2]) for a, b in ((low, mid), (mid, high))]
        right_low = push(halves[0], right)
        left_high = push(halves[1], left)
        right_high = push(halves[1], right)
        left_low = push(halves[0], left)
        third.append((right_low, left_high, right_high, left_low))
        across.append(push(region(low, high, order[:2]), partner))
    add_chunk(3)
    norms = jnp.sum(squares[0], axis=0, keepdims=True)
    put_blocks(acc_ref[...], norms, cross_ref, norm_ref)
    relays = []
    for p, ((order, _, _), (low, mid, high)) in enumerate(zip(PARTS, SPANS)):
        axis = order[2]
        before, after = (lax.rem(coords[axis] + o, 4) for o in (3, 1))
        left, right = (device_at(core, coords, axis, o) for o in (3, 1))
        third[p][0].wait_recv()
        one = push(region(low, mid, order[:2], axis, before), right)
        third[p][1].wait_recv()
        relays.append((one, push(region(mid, high, order[:2], axis, after), left)))
    for p, ((order, _, _), (low, mid, high)) in enumerate(zip(PARTS, SPANS)):
        axis = order[2]
        before, after = (lax.rem(coords[axis] + o, 4) for o in (3, 1))
        third[p][2].wait_recv()
        across.append(push(region(low, high, order[:2], axis, before), partner))
        third[p][3].wait_recv()
        across.append(push(region(low, high, order[:2], axis, after), partner))
    for p, ((order, _, _), (low, mid, high)) in enumerate(zip(PARTS, SPANS)):
        axis = order[2]
        opposite = lax.rem(coords[axis] + 2, 4)
        for copy, (a, b) in zip(relays[p], ((low, mid), (mid, high))):
            copy.wait_recv()
            across.append(push(region(a, b, order[:2], axis, opposite), partner))
    for copy in across:
        copy.wait_recv()
    for copy in sent:
        copy.wait_send()


def gather_call(own, targets, factor):
    copies = 9 + 9 + 12 + 3 + 6 + 6 + 6
    pts, held = factor.shape
    wanted, tiles, steps = targets.shape[1], held // 128, pts // TILE_PTS
    bf, f32, vmem = jnp.bfloat16, jnp.float32, pltpu.VMEM
    out, cross, norms = pl.pallas_call(
        gather_kernel,
        out_shape=(
            jax.ShapeDtypeStruct((4, 2, 4, 4, *own.shape), bf),
            jax.ShapeDtypeStruct((2, tiles * 8, 16, 128), bf),
            jax.ShapeDtypeStruct((tiles, 128), f32),
        ),
        in_specs=[pl.BlockSpec(memory_space=vmem)] * 2 + [pl.BlockSpec(memory_space=pl.ANY)],
        out_specs=[pl.BlockSpec(memory_space=vmem)] * 3,
        scratch_shapes=[
            vmem((steps, TILE_PTS, held), bf),
            vmem((wanted, held), f32),
            pltpu.SemaphoreType.DMA((copies,)),
            pltpu.SemaphoreType.DMA((copies,)),
            pltpu.SemaphoreType.DMA((steps,)),
        ],
        compiler_params=pltpu.CompilerParams(
            collective_id=2, has_side_effects=True, vmem_limit_bytes=48 << 20
        ),
        name="gather_rows",
    )(own, targets, factor)
    return out.reshape(128, *own.shape), cross, norms


MICRO = 16


def eliminate(rows, first):
    groups = len(rows)
    sub = lax.broadcasted_iota(jnp.int32, (SUB, PANEL), 0)
    rows = [list(values) for values in rows]

    def over_sublanes(value, k):
        return jnp.broadcast_to(value[k : k + 1, :], (SUB, PANEL))

    for m in range(0, groups, MICRO // SUB):
        cols = {}
        for r in range(m, groups):
            for k in range(MICRO):
                lane = first + m * SUB + k
                cols[r, k] = jnp.broadcast_to(rows[r][0][:, lane : lane + 1], (SUB, PANEL))
        for k in range(MICRO):
            g, at = m + k // SUB, k % SUB
            if at == 0:
                roots = jnp.ones((SUB, PANEL), jnp.float32)
            root = lax.rsqrt(over_sublanes(cols[g, k], at))
            roots = jnp.where(sub == at, root, roots)
            scale = root * root
            ahead = {j: over_sublanes(cols[g, j], at) for j in range(k + 1, MICRO)}
            pivot_rows = [over_sublanes(value, at) for value in rows[g]]
            for r in range(g, groups):
                if r == g and at == SUB - 1:
                    continue
                c = cols[r, k] * scale
                if r == g:
                    c = jnp.where(sub > at, c, 0.0)
                for j in range(k + 1, MICRO):
                    cols[r, j] = cols[r, j] - c * ahead[j]
                rows[r] = [value - c * row for value, row in zip(rows[r], pivot_rows)]
            if at == SUB - 1:
                rows[g] = [value * roots for value in rows[g]]
    return rows


def panel_inverse(block):
    half, groups = PANEL // 2, PANEL // 2 // SUB
    sub = lax.broadcasted_iota(jnp.int32, (SUB, PANEL), 0)
    lane = lax.broadcasted_iota(jnp.int32, (SUB, PANEL), 1)

    def unit(row):
        return (lane == sub + row).astype(jnp.float32)

    pieces = [block[SUB * r : SUB * (r + 1), :] for r in range(2 * groups)]
    top = eliminate([(pieces[r], unit(SUB * r)) for r in range(groups)], 0)
    right = jnp.concatenate([values[0] for values in top], axis=0)
    upper = jnp.concatenate([values[1] for values in top], axis=0)
    wide = lax.broadcasted_iota(jnp.int32, (half, PANEL), 1)
    both = jnp.where(wide < half, upper, right)
    change = jnp.dot(right.T, both, precision=HIGHEST, preferred_element_type=jnp.float32)
    low = []
    for r in range(groups, 2 * groups):
        piece = jnp.where(lane < half, 0.0, pieces[r])
        low.append((piece - change[SUB * r : SUB * (r + 1), :], unit(SUB * r)))
    low = eliminate(low, half)
    lower = [jnp.where(lane < half, values[0], values[1]) for values in low]
    return jnp.concatenate([upper, *lower], axis=0)


def local_kernel(
    pad_ref, pos_ref, targets_ref, points_ref, factor_ref,
    new_ref, cross_ref, norm_ref,
    ps_ref, pf_ref, sel_ref, a_ref, w_ref, lo_ref, hi_ref, down_hi, down_lo, fbuf, fsem,
):
    tiles = fbuf.shape[0]
    copies = []
    for i in range(tiles):
        at = pl.ds(i * TILE_PTS, TILE_PTS)
        copy = pltpu.make_async_copy(factor_ref.at[at, :], fbuf.at[i], fsem.at[i])
        copy.start()
        copies.append(copy)

    padded = pos_ref.shape[1]
    sel_ref[...] = jnp.where(
        lax.broadcasted_iota(jnp.int32, (BLOCK, padded), 0) == pos_ref[...], 1.0, 0.0
    ).astype(jnp.bfloat16)
    ahead = ps_ref.shape[1] // 128
    for t in range(0, pad_ref.shape[1], 2):
        pair = [
            pad_ref[:, k].astype(jnp.float32).reshape(padded, 128).astype(jnp.bfloat16)
            for k in (t, t + 1)
        ]
        rows = dot_nn(sel_ref[...], jnp.concatenate(pair, axis=1)).astype(jnp.bfloat16)
        if t < ahead:
            ps_ref[:, t * 128 : (t + 2) * 128] = rows
        else:
            pf_ref[:, (t - ahead) * 128 : (t - ahead + 2) * 128] = rows

    panels = BLOCK // PANEL
    total = jnp.zeros((1, BLOCK), jnp.float32)
    for r in range(panels):
        at = slice(r * PANEL, (r + 1) * PANEL)
        inter = dot_nt(pf_ref[at, :], pf_ref[...])
        total = total + jnp.sum(jnp.abs(inter), axis=0, keepdims=True)
        kern = jnp.exp(dot_nt(ps_ref[at, :], ps_ref[...]) / ps_ref.shape[1] - 1.0)
        a_ref[at, :] = kern - inter
    shift = ridge_shift + jnp.max(total)
    eye = lax.broadcasted_iota(jnp.int32, (PANEL, PANEL), 0) == lax.broadcasted_iota(
        jnp.int32, (PANEL, PANEL), 1
    )
    for copy in copies:
        copy.wait()

    def exact(a, b):
        return jnp.dot(a, b, precision=HIGHEST, preferred_element_type=jnp.float32)

    for j in range(panels):
        at = slice(j * PANEL, (j + 1) * PANEL)
        inv = panel_inverse(a_ref[at, at] + jnp.where(eye, shift, 0.0))
        if j:
            done = jnp.concatenate([exact(inv, w_ref[at, : j * PANEL]), inv], axis=1)
        else:
            done = inv
        high = done.astype(jnp.bfloat16)
        hi_ref[at, : (j + 1) * PANEL] = high
        lo_ref[at, : (j + 1) * PANEL] = (done - high.astype(jnp.float32)).astype(jnp.bfloat16)
        if j + 1 < panels:
            rest = slice((j + 1) * PANEL, BLOCK)
            hi_ref[at, rest] = jnp.zeros((PANEL, BLOCK - (j + 1) * PANEL), jnp.bfloat16)
            lo_ref[at, rest] = jnp.zeros((PANEL, BLOCK - (j + 1) * PANEL), jnp.bfloat16)
            right = exact(inv, a_ref[at, rest])
            for r in range(j + 1, panels):
                rows = slice(r * PANEL, (r + 1) * PANEL)
                skip = (r - j - 1) * PANEL
                left = right[:, skip : skip + PANEL].T
                a_ref[rows, r * PANEL :] = a_ref[rows, r * PANEL :] - exact(left, right[:, skip:])
                gone = exact(left, done)
                if j:
                    w_ref[rows, : j * PANEL] = w_ref[rows, : j * PANEL] - gone[:, : j * PANEL]
                w_ref[rows, at] = -gone[:, j * PANEL :]
        tile = slice(j * TILE_PTS, (j + 1) * TILE_PTS)
        scaled = normalize(points_ref[tile, :])
        down = jnp.exp(dot_nt(ps_ref[...], scaled) / scaled.shape[1] - 1.0) - dot_nt(
            pf_ref[...], fbuf[j]
        )
        high = down.astype(jnp.bfloat16)
        down_hi[:, tile] = high
        down_lo[:, tile] = (down - high.astype(jnp.float32)).astype(jnp.bfloat16)

    half = BLOCK // 2
    wanted = targets_ref.shape[1]
    acc = jnp.zeros((wanted, BLOCK), jnp.float32)
    nsq = jnp.zeros((BLOCK, 128), jnp.float32)
    for i in range(tiles):
        tile = slice(i * TILE_PTS, (i + 1) * TILE_PTS)
        for top, wide in ((0, half), (half, BLOCK)):
            at = slice(top, top + half)
            value = (
                dot_nn(hi_ref[at, :wide], down_hi[:wide, tile])
                + dot_nn(hi_ref[at, :wide], down_lo[:wide, tile])
                + dot_nn(lo_ref[at, :wide], down_hi[:wide, tile])
            )
            new_ref[at, tile] = value.astype(jnp.bfloat16)
        new = new_ref[:, tile]
        acc = acc + dot_nt(targets_ref[tile, :].T, new)
        wide_new = new.astype(jnp.float32)
        squares = wide_new * wide_new
        for t in range(TILE_PTS // 128):
            nsq = nsq + squares[:, t * 128 : (t + 1) * 128]
    norms = jnp.sum(nsq.T, axis=0, keepdims=True)
    put_blocks(acc, norms, cross_ref, norm_ref)


def local_call(padded, positions, points, factor, targets):
    pts, held = factor.shape
    features = points.shape[1]
    tiles = BLOCK // 128
    bf, f32, vmem = jnp.bfloat16, jnp.float32, pltpu.VMEM
    steps = pts // TILE_PTS
    return pl.pallas_call(
        local_kernel,
        out_shape=(
            jax.ShapeDtypeStruct((BLOCK, pts), bf),
            jax.ShapeDtypeStruct((2, tiles * 8, 16, 128), bf),
            jax.ShapeDtypeStruct((tiles, 128), f32),
        ),
        in_specs=[pl.BlockSpec(memory_space=vmem)] * 4 + [pl.BlockSpec(memory_space=pl.ANY)],
        out_specs=[pl.BlockSpec(memory_space=vmem)] * 3,
        scratch_shapes=[
            vmem((BLOCK, features), bf),
            vmem((BLOCK, held), bf),
            vmem((BLOCK, positions.shape[1]), bf),
            vmem((BLOCK, BLOCK), f32),
            vmem((BLOCK, BLOCK), f32),
            vmem((BLOCK, BLOCK), bf),
            vmem((BLOCK, BLOCK), bf),
            vmem((BLOCK, pts), bf),
            vmem((BLOCK, pts), bf),
            vmem((steps, TILE_PTS, held), bf),
            pltpu.SemaphoreType.DMA((steps,)),
        ],
        compiler_params=pltpu.CompilerParams(vmem_limit_bytes=44 << 20),
        name="local_block",
    )(padded, positions, targets, points, factor)


def sums_kernel(
    xf_ref, xn_ref, nf_ref, nn_ref, out_ref, got0, sum0, out0, norm_got0, norm_sum, norm_got, coef, got_last,
    a0, a1, a2, b0, b1, b2, c0, c1, c2, s1, s2, s3, t1, t2, t3, u1, u2, u3,
    send, recv,
):
    core, coords = place()
    partner = device_at(1 - core, coords)
    enter(core, coords)
    count = [0]
    sent = []

    def start(src, dst, device):
        k = count[0]
        count[0] += 1
        copy = pltpu.make_async_remote_copy(
            src_ref=src, dst_ref=dst, send_sem=send.at[k], recv_sem=recv.at[k],
            device_id=device, device_id_type=MESH,
        )
        copy.start()
        sent.append(copy)
        return copy

    def arrive(copies):
        for copy in copies:
            copy.wait_recv()

    wide = lambda v: v.astype(jnp.float32)
    narrow = lambda v: v.astype(jnp.bfloat16)

    split, tiles = xf_ref.shape[1], nf_ref.shape[0]
    arrive([
        start(xf_ref.at[1 - core], got0.at[:split], partner),
        start(xn_ref.at[1 - core], got0.at[split:], partner),
        start(nf_ref, norm_got0.at[:tiles], partner),
        start(nn_ref, norm_got0.at[tiles : tiles + nn_ref.shape[0]], partner),
    ])
    for src, at in ((xf_ref, slice(0, split)), (xn_ref, slice(split, got0.shape[0]))):
        value = wide(src[core]) + wide(got0[at])
        sum0[at] = value
        out0[at] = narrow(value)
    last_tile = tiles + nn_ref.shape[0]
    norm_sum[0, :tiles] = nf_ref[...] + norm_got0[:tiles]
    norm_sum[0, tiles:last_tile] = nn_ref[...] + norm_got0[tiles:last_tile]
    norm_sum[0, last_tile:] = jnp.zeros_like(norm_sum[0, last_tile:])

    got = ((a0, a1, a2), (b0, b1, b2), (c0, c1, c2))
    sums = ((s1, s2, s3), (t1, t2, t3))
    outs = (u1, u2, u3)

    copies, starts = [], []
    for p, (order, base, size) in enumerate(PARTS):
        here, quarter = coords[order[0]], size // 4
        for o in range(1, 4):
            there = lax.rem(here + o, 4)
            copies.append(
                start(
                    out0.at[pl.ds(base + there * quarter, quarter)],
                    got[0][p].at[o - 1],
                    device_at(core, coords, order[0], o),
                )
            )
        starts.append(base + here * quarter)
    for o in range(1, 4):
        copies.append(
            start(norm_sum.at[0], norm_got.at[0, o - 1], device_at(core, coords, 0, o))
        )
    arrive(copies)
    for p, (order, base, size) in enumerate(PARTS):
        quarter = size // 4
        value = sum0[pl.ds(starts[p], quarter)]
        for o in range(3):
            value = value + wide(got[0][p][o])
        sums[0][p][...] = value
        outs[p][...] = narrow(value)
    norm_sum[1] = norm_sum[0] + norm_got[0, 0] + norm_got[0, 1] + norm_got[0, 2]

    copies = []
    for p, (order, base, size) in enumerate(PARTS):
        here, piece = coords[order[1]], size // 16
        for o in range(1, 4):
            there = lax.rem(here + o, 4)
            copies.append(
                start(
                    outs[p].at[pl.ds(there * piece, piece)],
                    got[1][p].at[o - 1],
                    device_at(core, coords, order[1], o),
                )
            )
        starts[p] = starts[p] + here * piece
    for o in range(1, 4):
        copies.append(
            start(norm_sum.at[1], norm_got.at[1, o - 1], device_at(core, coords, 1, o))
        )
    arrive(copies)
    for p, (order, base, size) in enumerate(PARTS):
        here, piece = coords[order[1]], size // 16
        value = sums[0][p][pl.ds(here * piece, piece)]
        for o in range(3):
            value = value + wide(got[1][p][o])
        sums[1][p][0] = value
        coef[pl.ds(starts[p], piece)] = narrow(value)
    norm_sum[2] = norm_sum[1] + norm_got[1, 0] + norm_got[1, 1] + norm_got[1, 2]

    copies = []
    for p, (order, base, size) in enumerate(PARTS):
        piece = size // 16
        for o in range(1, 4):
            copies.append(
                start(
                    coef.at[pl.ds(starts[p], piece)],
                    got[2][p].at[o - 1],
                    device_at(core, coords, order[2], o),
                )
            )
    for o in range(1, 4):
        copies.append(
            start(norm_sum.at[2], norm_got.at[2, o - 1], device_at(core, coords, 2, o))
        )
    arrive(copies)
    for copy in copies:
        copy.wait_send()
    del sent[-len(copies):]
    norm_sum[3] = norm_sum[2] + norm_got[2, 0] + norm_got[2, 1] + norm_got[2, 2]
    for p, (order, base, size) in enumerate(PARTS):
        piece = size // 16
        value = sums[1][p][0]
        for o in range(3):
            value = value + wide(got[2][p][o])
        for i in range(piece):
            tile = lax.div(starts[p] + i, 8)
            norm = norm_sum[3, pl.ds(tile, 1), :]
            coef[starts[p] + i] = narrow(value[i] / (norm + damping))

    for stage, parts_of in ((1, 16), (0, 4)):
        copies = []
        for p, (order, base, size) in enumerate(PARTS):
            piece = size // parts_of
            if stage == 0:
                starts[p] = base + coords[order[0]] * piece
            block = coef.at[pl.ds(starts[p], piece)]
            for o in range(1, 4):
                copies.append(start(block, block, device_at(core, coords, order[stage], o)))
        arrive(copies)
    last = start(coef, got_last, partner)
    out_ref[core] = coef[...]
    last.wait_recv()
    out_ref[1 - core] = got_last[...]
    for copy in sent:
        copy.wait_send()


def sums_call(cross_f, cross_n, norms_f, norms_n):
    blocks = cross_f.shape[1] + cross_n.shape[1]
    tiles = 24
    bf, f32, vmem = jnp.bfloat16, jnp.float32, pltpu.VMEM
    piece = lambda lead, n, kind: vmem((*lead, n, 16, 128), kind)
    sizes = [size for _, _, size in PARTS]
    scratch = [
        vmem((blocks, 16, 128), bf), vmem((blocks, 16, 128), f32), vmem((blocks, 16, 128), bf),
        vmem((tiles, 128), f32), vmem((4, tiles, 128), f32), vmem((3, 3, tiles, 128), f32),
        vmem((blocks, 16, 128), bf), vmem((blocks, 16, 128), bf),
    ]
    scratch += [piece((3,), s // 4, bf) for s in sizes]
    scratch += [piece((3,), s // 16, bf) for s in sizes]
    scratch += [piece((3,), s // 16, bf) for s in sizes]
    scratch += [piece((), s // 4, f32) for s in sizes]
    scratch += [piece((1,), s // 16, f32) for s in sizes]
    scratch += [piece((), s // 4, bf) for s in sizes]
    copies = 4 + 12 * 3 + 9 * 2 + 1
    scratch += [pltpu.SemaphoreType.DMA((copies,))] * 2
    return pl.pallas_call(
        sums_kernel,
        out_shape=jax.ShapeDtypeStruct((2, blocks, 16, 128), bf),
        in_specs=[pl.BlockSpec(memory_space=vmem)] * 4,
        out_specs=pl.BlockSpec(memory_space=vmem),
        scratch_shapes=scratch,
        compiler_params=pltpu.CompilerParams(
            collective_id=1, has_side_effects=True, vmem_limit_bytes=24 << 20
        ),
        name="sums",
    )(cross_f, cross_n, norms_f, norms_n)


def residual_kernel(factor_ref, new_ref, targets_ref, coef_ref, out_ref, turned_ref):
    held = factor_ref.shape[1]

    @pl.when(pl.program_id(0) == 0)
    def _():
        for t in range(turned_ref.shape[1] // 128):
            lanes = slice(t * 128, (t + 1) * 128)
            turned_ref[:, lanes] = coef_ref[:, t * 8 : (t + 1) * 8].reshape(-1, 128)

    fitted = dot_nt(factor_ref[...], turned_ref[:, :held])
    fitted = fitted + dot_nn(turned_ref[:, held:], new_ref[...]).T
    out_ref[...] = targets_ref[...].astype(jnp.float32) - fitted


def residual_call(factor, new, targets, coef):
    pts, held = factor.shape
    wanted = targets.shape[1]
    return pl.pallas_call(
        residual_kernel,
        grid=(pts // TILE_PTS,),
        out_shape=jax.ShapeDtypeStruct((pts, wanted), jnp.float32),
        in_specs=[
            pl.BlockSpec((TILE_PTS, held), lambda i: (i, 0)),
            pl.BlockSpec((BLOCK, TILE_PTS), lambda i: (0, i)),
            pl.BlockSpec((TILE_PTS, wanted), lambda i: (i, 0)),
            pl.BlockSpec(coef.shape, lambda i: (0, 0, 0, 0), pipeline_mode=pl.Buffered(1)),
        ],
        out_specs=pl.BlockSpec((TILE_PTS, wanted), lambda i: (i, 0)),
        scratch_shapes=[pltpu.VMEM((wanted, held + BLOCK), jnp.bfloat16)],
        compiler_params=pltpu.CompilerParams(vmem_limit_bytes=24 << 20),
        name="residual",
    )(factor, new, targets, coef)


def on_device(points, factor, targets, pivot_slots, pivot_counts):
    own = rows_call(pivot_slots, points, factor)
    padded, cross_f, norms_f = gather_call(own, targets, factor)
    positions = padded_positions(pivot_counts, pivot_slots.shape[1])
    new_columns, cross_n, norms_n = local_call(padded, positions, points, factor, targets)
    coef = sums_call(cross_f, cross_n, norms_f, norms_n)
    residual_next = residual_call(factor, new_columns, targets, coef)
    return (new_columns, residual_next)


def solution(mesh):
    return jax.shard_map(
        on_device,
        mesh=mesh,
        in_specs=(
            P(("row", "col"), None),
            P(("row", "col"), None),
            P(("row", "col"), None),
            P(("row", "col"), None),
            P(),
        ),
        out_specs=(P(None, ("row", "col")), P(("row", "col"), None)),
        check_vma=False,
    )
```

```python
import functools

import jax
import jax.numpy as jnp
from jax import lax
from jax.experimental import pallas as pl
from jax.experimental.pallas import tpu as pltpu
from jax.sharding import PartitionSpec as P

BLOCK = 512
PANEL = 128
SUB = 8
TILE_PTS = 512
ROWS_VMEM, GATHER_VMEM, LOCAL_VMEM, SUMS_VMEM, RESIDUAL_VMEM = (
    mib << 20 for mib in (60, 40, 38, 16, 16)
)
MESH = pl.DeviceIdType.MESH
HIGHEST = lax.Precision.HIGHEST

ridge_shift = 0.01
damping = 1.0
epsilon = 1e-06


def normalize(points):
    values = points.astype(jnp.float32)
    factor_scale = lax.rsqrt(jnp.mean(values * values, axis=1, keepdims=True) + epsilon)
    return (values * factor_scale).astype(jnp.bfloat16)


def padded_positions(pivot_counts, slot_cap):
    starts = jnp.cumsum(pivot_counts) - pivot_counts
    slot = jnp.arange(slot_cap, dtype=jnp.int32)[None, :]
    place_of = jnp.where(slot < pivot_counts[:, None], starts[:, None] + slot, -1)
    return place_of.astype(jnp.int32).reshape(1, -1)


def dot_nt(a, b):
    return lax.dot_general(a, b, (((1,), (1,)), ((), ())), preferred_element_type=jnp.float32)


def dot_nn(a, b):
    return jnp.dot(a, b, preferred_element_type=jnp.float32)


def put_blocks(acc, norms, cross_ref, norm_ref):
    for t in range(norms.shape[1] // 128):
        lanes = slice(t * 128, (t + 1) * 128)
        norm_ref[t : t + 1, :] = norms[:, lanes]
        cross_ref[:, t * 8 : (t + 1) * 8] = (
            acc[:, lanes].astype(jnp.bfloat16).reshape(2, 8, 16, 128)
        )


ORDERS = ((0, 1, 2), (1, 2, 0), (2, 0, 1))
HELD_PARTS = ((0, 48), (48, 48), (96, 32))
NEW_PARTS = ((0, 12), (12, 12), (24, 8))


def place():
    row, col = lax.axis_index("row"), lax.axis_index("col")
    core = lax.rem(row, 2)
    coords = (lax.div(col, 4), lax.div(row, 2), lax.rem(col, 4))
    return core, coords


def device_at(core, coords, axis=0, offset=0):
    x, y, z = (
        lax.rem(c + offset, 4) if (a == axis and offset) else c for a, c in enumerate(coords)
    )
    return (y * 2 + core, x * 4 + z)


def enter(core, coords):
    barrier = pltpu.get_barrier_semaphore()
    peers = [device_at(1 - core, coords)]
    peers += [device_at(core, coords, a, o) for a in range(3) for o in range(1, 4)]
    for peer in peers:
        pl.semaphore_signal(barrier, inc=1, device_id=peer, device_id_type=MESH)
    pl.semaphore_wait(barrier, len(peers))


def load_tiles(src, buf, sem):
    loads = []
    for i in range(buf.shape[0]):
        tile = src.at[pl.ds(i * TILE_PTS, TILE_PTS), :]
        loads.append(pltpu.make_async_copy(tile, buf.at[i], sem.at[i]))
        loads[i].start()
    return loads


class Copies:
    def __init__(self, send, recv):
        self.send, self.recv, self.started = send, recv, []

    def start(self, src, dst, device):
        k = len(self.started)
        copy = pltpu.make_async_remote_copy(
            src_ref=src, dst_ref=dst, send_sem=self.send.at[k], recv_sem=self.recv.at[k],
            device_id=device, device_id_type=MESH,
        )
        copy.start()
        self.started.append(copy)
        return copy

    def finish(self):
        for copy in self.started:
            copy.wait_send()


def arrive(copies):
    for copy in copies:
        copy.wait_recv()


def wide(value):
    return value.astype(jnp.float32)


def narrow(value):
    return value.astype(jnp.bfloat16)


def rows_kernel(slots_ref, points_ref, factor_ref, out_ref, pbuf, fbuf, psem, fsem):
    cap = pbuf.shape[0]
    copies = []
    for s in range(cap):
        base = pl.multiple_of(lax.div(slots_ref[0, s], SUB) * SUB, SUB)
        for src, buf, sem in ((points_ref, pbuf, psem), (factor_ref, fbuf, fsem)):
            copy = pltpu.make_async_copy(src.at[pl.ds(base, SUB), :], buf.at[s], sem.at[s])
            copy.start()
            copies.append(copy)
    for copy in copies:
        copy.wait()

    def picked(buf):
        sub = lax.broadcasted_iota(jnp.int32, buf.shape[1:], 0)
        out = jnp.zeros(buf.shape[1:], jnp.float32)
        for s in range(cap):
            offset = lax.rem(slots_ref[0, s], SUB)
            row = jnp.sum(
                jnp.where(sub == offset, buf[s].astype(jnp.float32), 0.0), axis=0, keepdims=True
            )
            out = jnp.where(sub == s, row, out)
        return out

    both = (normalize(picked(pbuf)), picked(fbuf).astype(jnp.bfloat16))
    t = 0
    for rows in both:
        for k in range(rows.shape[1] // 128):
            out_ref[t] = rows[:, k * 128 : (k + 1) * 128]
            t += 1


def rows_call(pivot_slots, points, factor):
    cap = pivot_slots.shape[1]
    features, held = points.shape[1], factor.shape[1]
    return pl.pallas_call(
        rows_kernel,
        out_shape=jax.ShapeDtypeStruct(((features + held) // 128, cap, 128), jnp.bfloat16),
        in_specs=[
            pl.BlockSpec(memory_space=pltpu.SMEM),
            pl.BlockSpec(memory_space=pl.ANY),
            pl.BlockSpec(memory_space=pl.ANY),
        ],
        out_specs=pl.BlockSpec(memory_space=pltpu.VMEM),
        scratch_shapes=[
            pltpu.VMEM((cap, SUB, features), jnp.bfloat16),
            pltpu.VMEM((cap, SUB, held), jnp.bfloat16),
            pltpu.SemaphoreType.DMA((cap,)),
            pltpu.SemaphoreType.DMA((cap,)),
        ],
        compiler_params=pltpu.CompilerParams(vmem_limit_bytes=ROWS_VMEM),
        name="pivot_rows",
    )(pivot_slots, points, factor)


SPANS = ((0, 4, 7), (7, 11, 14), (14, 17, 20))


def gather_kernel(
    own_ref, targets_ref, factor_ref, out_ref, shard_ref, acc_ref, x_ref, n_ref, got0, norm_got0,
    sum0, out0, norm_sum, norm_got, a0, a1, a2, b0, b1, b2, c0, c1, c2, s0, s1, s2, u0, u1, u2,
    v0, v1, v2, fbuf, fsem, send, recv,
):
    core, coords = place()
    partner = device_at(1 - core, coords)
    loads = load_tiles(factor_ref, fbuf, fsem)
    enter(core, coords)
    copies = Copies(send, recv)

    def peer(axis, offset):
        return device_at(core, coords, axis, offset)

    def region(low, high, whole=(), axis=None, at=None):
        x, y, z = (
            slice(None) if a in whole else (at if a == axis else c)
            for a, c in enumerate(coords)
        )
        return out_ref.at[y, core, x, z, low:high]

    def push(block, device):
        return copies.start(block, block, device)

    first = []
    for order, (low, _, high) in zip(ORDERS, SPANS):
        first.append([
            copies.start(own_ref.at[low:high], region(low, high), peer(order[0], o))
            for o in (2, 1, 3)
        ])
    x, y, z = coords
    out_ref[y, core, x, z] = own_ref[...]
    squares = jnp.zeros((SUB, factor_ref.shape[1]), jnp.float32)
    chunks = factor_ref.shape[0] // TILE_PTS

    def add_chunk(i, squares):
        at = slice(i * TILE_PTS, (i + 1) * TILE_PTS)
        loads[i].wait()
        value = dot_nn(targets_ref[at, :].T, fbuf[i])
        acc_ref[...] = value if i == 0 else acc_ref[...] + value
        values = wide(fbuf[i])
        return squares + jnp.sum((values * values).reshape(-1, SUB, values.shape[1]), axis=0)

    squares = add_chunk(0, squares)
    second = []
    for p, (order, (low, _, high)) in enumerate(zip(ORDERS, SPANS)):
        arrive(first[p])
        block = region(low, high, order[:1])
        second.append([push(block, peer(order[1], o)) for o in (2, 1, 3)])
    for i in range(1, chunks):
        squares = add_chunk(i, squares)
    put_blocks(acc_ref[...], jnp.sum(squares, axis=0, keepdims=True), x_ref, n_ref)
    zero = [
        copies.start(x_ref.at[1 - core], got0, partner),
        copies.start(n_ref, norm_got0, partner),
    ]
    third, across = [], []
    for p, (order, (low, mid, high)) in enumerate(zip(ORDERS, SPANS)):
        arrive(second[p])
        left, right = peer(order[2], 3), peer(order[2], 1)
        halves = [region(a, b, order[:2]) for a, b in ((low, mid), (mid, high))]
        right_low = push(halves[0], right)
        left_high = push(halves[1], left)
        right_high = push(halves[1], right)
        left_low = push(halves[0], left)
        third.append((right_low, left_high, right_high, left_low))
        across.append(push(region(low, high, order[:2]), partner))

    arrive(zero)
    sum0[...] = wide(x_ref[core]) + wide(got0[...])
    out0[...] = narrow(sum0[...])
    norm_sum[0] = n_ref[...] + norm_got0[...]
    one, starts = [], []
    for p, (order, (base, size)) in enumerate(zip(ORDERS, HELD_PARTS)):
        here, piece = coords[order[0]], size // 4
        for o in range(1, 4):
            there = lax.rem(here + o, 4)
            one.append(
                copies.start(
                    out0.at[pl.ds(base + there * piece, piece)],
                    (a0, a1, a2)[p].at[o - 1],
                    peer(order[0], o),
                )
            )
        starts.append(base + here * piece)
    for o in range(1, 4):
        one.append(copies.start(norm_sum.at[0], norm_got.at[0, o - 1], peer(0, o)))

    relays = []
    for p, (order, (low, mid, high)) in enumerate(zip(ORDERS, SPANS)):
        axis = order[2]
        before, after = (lax.rem(coords[axis] + o, 4) for o in (3, 1))
        third[p][0].wait_recv()
        relay = push(region(low, mid, order[:2], axis, before), peer(axis, 1))
        third[p][1].wait_recv()
        relays.append((relay, push(region(mid, high, order[:2], axis, after), peer(axis, 3))))

    arrive(one)
    two = []
    for p, (order, (base, size)) in enumerate(zip(ORDERS, HELD_PARTS)):
        here, piece, fours = coords[order[1]], size // 16, size // 4
        value = sum0[pl.ds(starts[p], fours)]
        for o in range(3):
            value = value + wide((a0, a1, a2)[p][o])
        (s0, s1, s2)[p][...] = value
        (u0, u1, u2)[p][...] = narrow(value)
        for o in range(1, 4):
            there = lax.rem(here + o, 4)
            two.append(
                copies.start(
                    (u0, u1, u2)[p].at[pl.ds(there * piece, piece)],
                    (b0, b1, b2)[p].at[o - 1],
                    peer(order[1], o),
                )
            )
        starts[p] = starts[p] + here * piece
    norm_sum[1] = norm_sum[0] + norm_got[0, 0] + norm_got[0, 1] + norm_got[0, 2]
    for o in range(1, 4):
        two.append(copies.start(norm_sum.at[1], norm_got.at[1, o - 1], peer(1, o)))

    for p, (order, (low, mid, high)) in enumerate(zip(ORDERS, SPANS)):
        axis = order[2]
        before, after = (lax.rem(coords[axis] + o, 4) for o in (3, 1))
        third[p][2].wait_recv()
        across.append(push(region(low, high, order[:2], axis, before), partner))
        third[p][3].wait_recv()
        across.append(push(region(low, high, order[:2], axis, after), partner))

    arrive(two)
    three, values = [], []
    for p, (order, (base, size)) in enumerate(zip(ORDERS, HELD_PARTS)):
        here, piece = coords[order[1]], size // 16
        value = (s0, s1, s2)[p][pl.ds(here * piece, piece)]
        for o in range(3):
            value = value + wide((b0, b1, b2)[p][o])
        values.append(value)
        (v0, v1, v2)[p][...] = narrow(value)
        for o in range(1, 4):
            three.append(
                copies.start((v0, v1, v2)[p], (c0, c1, c2)[p].at[o - 1], peer(order[2], o))
            )
    norm_sum[2] = norm_sum[1] + norm_got[1, 0] + norm_got[1, 1] + norm_got[1, 2]
    for o in range(1, 4):
        three.append(copies.start(norm_sum.at[2], norm_got.at[2, o - 1], peer(2, o)))

    for p, (order, (low, mid, high)) in enumerate(zip(ORDERS, SPANS)):
        axis = order[2]
        opposite = lax.rem(coords[axis] + 2, 4)
        for copy, (a, b) in zip(relays[p], ((low, mid), (mid, high))):
            copy.wait_recv()
            across.append(push(region(a, b, order[:2], axis, opposite), partner))

    arrive(three)
    norm_sum[3] = norm_sum[2] + norm_got[2, 0] + norm_got[2, 1] + norm_got[2, 2]
    at = 0
    for p, (order, (base, size)) in enumerate(zip(ORDERS, HELD_PARTS)):
        value = values[p]
        for o in range(3):
            value = value + wide((c0, c1, c2)[p][o])
        for i in range(size // 16):
            norm = norm_sum[3, pl.ds(lax.div(starts[p] + i, 8), 1), :]
            shard_ref[at] = narrow(value[i] / (norm + damping))
            at += 1
    arrive(across)
    copies.finish()


def pieces(parts, lead, share, kind):
    return [pltpu.VMEM((*lead, size // share, 16, 128), kind) for _, size in parts]


def gather_call(own, targets, factor):
    copies = 9 + 9 + 12 + 3 + 6 + 6 + 6 + 2 + 3 * 12
    held, wanted = factor.shape[1], targets.shape[1]
    tiles = held // 128
    blocks = tiles * 8
    bf, f32, vmem = jnp.bfloat16, jnp.float32, pltpu.VMEM
    scratch = [
        vmem((wanted, held), f32),
        vmem((2, blocks, 16, 128), bf),
        vmem((tiles, 128), f32),
        vmem((blocks, 16, 128), bf),
        vmem((tiles, 128), f32),
        vmem((blocks, 16, 128), f32),
        vmem((blocks, 16, 128), bf),
        vmem((4, tiles, 128), f32),
        vmem((3, 3, tiles, 128), f32),
    ]
    scratch += pieces(HELD_PARTS, (3,), 4, bf) + pieces(HELD_PARTS, (3,), 16, bf)
    scratch += pieces(HELD_PARTS, (3,), 16, bf) + pieces(HELD_PARTS, (), 4, f32)
    scratch += pieces(HELD_PARTS, (), 4, bf) + pieces(HELD_PARTS, (), 16, bf)
    steps = factor.shape[0] // TILE_PTS
    scratch += [vmem((steps, TILE_PTS, held), bf), pltpu.SemaphoreType.DMA((steps,))]
    scratch += [pltpu.SemaphoreType.DMA((copies,))] * 2
    out, shard = pl.pallas_call(
        gather_kernel,
        out_shape=(
            jax.ShapeDtypeStruct((4, 2, 4, 4, *own.shape), bf),
            jax.ShapeDtypeStruct((blocks // 16, 16, 128), bf),
        ),
        in_specs=[pl.BlockSpec(memory_space=vmem)] * 2 + [pl.BlockSpec(memory_space=pl.ANY)],
        out_specs=[pl.BlockSpec(memory_space=vmem)] * 2,
        scratch_shapes=scratch,
        compiler_params=pltpu.CompilerParams(
            collective_id=2, has_side_effects=True, vmem_limit_bytes=GATHER_VMEM
        ),
        name="gather_rows",
    )(own, targets, factor)
    return out.reshape(128, *own.shape), shard


MICRO = 16


def eliminate(rows, first):
    groups = len(rows)
    sub = lax.broadcasted_iota(jnp.int32, (SUB, PANEL), 0)
    rows = [list(values) for values in rows]

    def over_sublanes(value, k):
        return jnp.broadcast_to(value[k : k + 1, :], (SUB, PANEL))

    for m in range(0, groups, MICRO // SUB):
        cols = {}
        for r in range(m, groups):
            for k in range(MICRO):
                lane = first + m * SUB + k
                cols[r, k] = jnp.broadcast_to(rows[r][0][:, lane : lane + 1], (SUB, PANEL))
        for k in range(MICRO):
            g, at = m + k // SUB, k % SUB
            if at == 0:
                roots = jnp.ones((SUB, PANEL), jnp.float32)
            root = lax.rsqrt(over_sublanes(cols[g, k], at))
            roots = jnp.where(sub == at, root, roots)
            scale = root * root
            ahead = {j: over_sublanes(cols[g, j], at) for j in range(k + 1, MICRO)}
            pivot_rows = [over_sublanes(value, at) for value in rows[g]]
            for r in range(g, groups):
                if r == g and at == SUB - 1:
                    continue
                c = cols[r, k] * scale
                if r == g:
                    c = jnp.where(sub > at, c, 0.0)
                for j in range(k + 1, MICRO):
                    cols[r, j] = cols[r, j] - c * ahead[j]
                rows[r] = [value - c * row for value, row in zip(rows[r], pivot_rows)]
            if at == SUB - 1:
                rows[g] = [value * roots for value in rows[g]]
    return rows


def panel_inverse(block):
    half, groups = PANEL // 2, PANEL // 2 // SUB
    sub = lax.broadcasted_iota(jnp.int32, (SUB, PANEL), 0)
    lane = lax.broadcasted_iota(jnp.int32, (SUB, PANEL), 1)

    def unit(row):
        return (lane == sub + row).astype(jnp.float32)

    pieces = [block[SUB * r : SUB * (r + 1), :] for r in range(2 * groups)]
    top = eliminate([(pieces[r], unit(SUB * r)) for r in range(groups)], 0)
    right = jnp.concatenate([values[0] for values in top], axis=0)
    upper = jnp.concatenate([values[1] for values in top], axis=0)
    wide = lax.broadcasted_iota(jnp.int32, (half, PANEL), 1)
    both = jnp.where(wide < half, upper, right)
    change = jnp.dot(right.T, both, precision=HIGHEST, preferred_element_type=jnp.float32)
    low = []
    for r in range(groups, 2 * groups):
        piece = jnp.where(lane < half, 0.0, pieces[r])
        low.append((piece - change[SUB * r : SUB * (r + 1), :], unit(SUB * r)))
    low = eliminate(low, half)
    lower = [jnp.where(lane < half, values[0], values[1]) for values in low]
    return jnp.concatenate([upper, *lower], axis=0)


def local_kernel(
    pad_ref, pos_ref, targets_ref, points_ref, factor_ref,
    new_ref, cross_ref, norm_ref,
    ps_ref, pf_ref, sel_ref, a_ref, w_ref, lo_ref, hi_ref, down_hi, down_lo, fbuf, fsem,
):
    tiles = fbuf.shape[0]
    loads = load_tiles(factor_ref, fbuf, fsem)
    padded = pos_ref.shape[1]
    sel_ref[...] = jnp.where(
        lax.broadcasted_iota(jnp.int32, (BLOCK, padded), 0) == pos_ref[...], 1.0, 0.0
    ).astype(jnp.bfloat16)
    ahead = ps_ref.shape[1] // 128
    for t in range(0, pad_ref.shape[1], 2):
        pair = [
            pad_ref[:, k].astype(jnp.float32).reshape(padded, 128).astype(jnp.bfloat16)
            for k in (t, t + 1)
        ]
        rows = dot_nn(sel_ref[...], jnp.concatenate(pair, axis=1)).astype(jnp.bfloat16)
        if t < ahead:
            ps_ref[:, t * 128 : (t + 2) * 128] = rows
        else:
            pf_ref[:, (t - ahead) * 128 : (t - ahead + 2) * 128] = rows

    panels = BLOCK // PANEL
    total = jnp.zeros((1, BLOCK), jnp.float32)
    for r in range(panels):
        at = slice(r * PANEL, (r + 1) * PANEL)
        inter = dot_nt(pf_ref[at, :], pf_ref[...])
        total = total + jnp.sum(jnp.abs(inter), axis=0, keepdims=True)
        kern = jnp.exp(dot_nt(ps_ref[at, :], ps_ref[...]) / ps_ref.shape[1] - 1.0)
        a_ref[at, :] = kern - inter
    shift = ridge_shift + jnp.max(total)
    eye = lax.broadcasted_iota(jnp.int32, (PANEL, PANEL), 0) == lax.broadcasted_iota(
        jnp.int32, (PANEL, PANEL), 1
    )
    for load in loads:
        load.wait()

    def exact(a, b):
        return jnp.dot(a, b, precision=HIGHEST, preferred_element_type=jnp.float32)

    for j in range(panels):
        at = slice(j * PANEL, (j + 1) * PANEL)
        inv = panel_inverse(a_ref[at, at] + jnp.where(eye, shift, 0.0))
        if j:
            done = jnp.concatenate([exact(inv, w_ref[at, : j * PANEL]), inv], axis=1)
        else:
            done = inv
        high = done.astype(jnp.bfloat16)
        hi_ref[at, : (j + 1) * PANEL] = high
        lo_ref[at, : (j + 1) * PANEL] = (done - high.astype(jnp.float32)).astype(jnp.bfloat16)
        if j + 1 < panels:
            rest = slice((j + 1) * PANEL, BLOCK)
            hi_ref[at, rest] = jnp.zeros((PANEL, BLOCK - (j + 1) * PANEL), jnp.bfloat16)
            lo_ref[at, rest] = jnp.zeros((PANEL, BLOCK - (j + 1) * PANEL), jnp.bfloat16)
            right = exact(inv, a_ref[at, rest])
            for r in range(j + 1, panels):
                rows = slice(r * PANEL, (r + 1) * PANEL)
                skip = (r - j - 1) * PANEL
                left = right[:, skip : skip + PANEL].T
                a_ref[rows, r * PANEL :] = a_ref[rows, r * PANEL :] - exact(left, right[:, skip:])
                gone = exact(left, done)
                if j:
                    w_ref[rows, : j * PANEL] = w_ref[rows, : j * PANEL] - gone[:, : j * PANEL]
                w_ref[rows, at] = -gone[:, j * PANEL :]
        tile = slice(j * TILE_PTS, (j + 1) * TILE_PTS)
        scaled = normalize(points_ref[tile, :])
        down = jnp.exp(dot_nt(ps_ref[...], scaled) / scaled.shape[1] - 1.0) - dot_nt(
            pf_ref[...], fbuf[j]
        )
        high = down.astype(jnp.bfloat16)
        down_hi[:, tile] = high
        down_lo[:, tile] = (down - high.astype(jnp.float32)).astype(jnp.bfloat16)

    half = BLOCK // 2
    wanted = targets_ref.shape[1]
    acc = jnp.zeros((wanted, BLOCK), jnp.float32)
    nsq = jnp.zeros((BLOCK, 128), jnp.float32)
    for i in range(tiles):
        tile = slice(i * TILE_PTS, (i + 1) * TILE_PTS)
        for top, wide in ((0, half), (half, BLOCK)):
            at = slice(top, top + half)
            value = (
                dot_nn(hi_ref[at, :wide], down_hi[:wide, tile])
                + dot_nn(hi_ref[at, :wide], down_lo[:wide, tile])
                + dot_nn(lo_ref[at, :wide], down_hi[:wide, tile])
            )
            new_ref[at, tile] = value.astype(jnp.bfloat16)
        new = new_ref[:, tile]
        acc = acc + dot_nt(targets_ref[tile, :].T, new)
        wide_new = new.astype(jnp.float32)
        squares = wide_new * wide_new
        for t in range(TILE_PTS // 128):
            nsq = nsq + squares[:, t * 128 : (t + 1) * 128]
    norms = jnp.sum(nsq.T, axis=0, keepdims=True)
    put_blocks(acc, norms, cross_ref, norm_ref)


def local_call(padded, positions, points, factor, targets):
    pts, held = factor.shape
    features = points.shape[1]
    tiles = BLOCK // 128
    bf, f32, vmem = jnp.bfloat16, jnp.float32, pltpu.VMEM
    return pl.pallas_call(
        local_kernel,
        out_shape=(
            jax.ShapeDtypeStruct((BLOCK, pts), bf),
            jax.ShapeDtypeStruct((2, tiles * 8, 16, 128), bf),
            jax.ShapeDtypeStruct((tiles, 128), f32),
        ),
        in_specs=[pl.BlockSpec(memory_space=vmem)] * 4 + [pl.BlockSpec(memory_space=pl.ANY)],
        out_specs=[pl.BlockSpec(memory_space=vmem)] * 3,
        scratch_shapes=[
            vmem((BLOCK, features), bf),
            vmem((BLOCK, held), bf),
            vmem((BLOCK, positions.shape[1]), bf),
            vmem((BLOCK, BLOCK), f32),
            vmem((BLOCK, BLOCK), f32),
            vmem((BLOCK, BLOCK), bf),
            vmem((BLOCK, BLOCK), bf),
            vmem((BLOCK, pts), bf),
            vmem((BLOCK, pts), bf),
            vmem((pts // TILE_PTS, TILE_PTS, held), bf),
            pltpu.SemaphoreType.DMA((pts // TILE_PTS,)),
        ],
        compiler_params=pltpu.CompilerParams(vmem_limit_bytes=LOCAL_VMEM),
        name="local_block",
    )(padded, positions, targets, points, factor)


def sums_kernel(
    shard_ref, x_ref, n_ref, out_ref, coef, got_last, got0, norm_got0, sum0, out0, norm_sum,
    norm_got, a0, a1, a2, b0, b1, b2, c0, c1, c2, u0, u1, u2, v0, v1, v2, send, recv,
):
    core, coords = place()
    partner = device_at(1 - core, coords)
    enter(core, coords)
    copies = Copies(send, recv)
    split = coef.shape[0] - x_ref.shape[1]

    def peer(axis, offset):
        return device_at(core, coords, axis, offset)

    zero = [
        copies.start(x_ref.at[1 - core], got0, partner),
        copies.start(n_ref, norm_got0, partner),
    ]
    held, at = [], 0
    for order, (base, size) in zip(ORDERS, HELD_PARTS):
        piece = size // 16
        place_of = base + coords[order[0]] * (size // 4) + coords[order[1]] * piece
        for o in range(1, 4):
            held.append(
                copies.start(
                    shard_ref.at[at : at + piece], coef.at[pl.ds(place_of, piece)],
                    peer(order[1], o),
                )
            )
        coef[pl.ds(place_of, piece)] = shard_ref[at : at + piece]
        at += piece

    arrive(zero)
    sum0[...] = wide(x_ref[core]) + wide(got0[...])
    out0[...] = narrow(sum0[...])
    norm_sum[0] = n_ref[...] + norm_got0[...]
    one = []
    for p, (order, (base, size)) in enumerate(zip(ORDERS, NEW_PARTS)):
        here, piece = coords[order[0]], size // 4
        for o in range(1, 4):
            there = lax.rem(here + o, 4)
            one.append(
                copies.start(
                    out0.at[pl.ds(base + there * piece, piece)],
                    (a0, a1, a2)[p].at[o - 1],
                    peer(order[0], o),
                )
            )
    for o in range(1, 4):
        one.append(copies.start(norm_sum.at[0], norm_got.at[0, o - 1], peer(0, o)))

    arrive(held)
    held = []
    for order, (base, size) in zip(ORDERS, HELD_PARTS):
        block = coef.at[pl.ds(base + coords[order[0]] * (size // 4), size // 4)]
        for o in range(1, 4):
            held.append(copies.start(block, block, peer(order[0], o)))

    values = []
    arrive(one)
    for p, (order, (base, size)) in enumerate(zip(ORDERS, NEW_PARTS)):
        piece = size // 4
        value = sum0[pl.ds(base + coords[order[0]] * piece, piece)]
        for o in range(3):
            value = value + wide((a0, a1, a2)[p][o])
        values.append(value)
    norm_sum[1] = norm_sum[0] + norm_got[0, 0] + norm_got[0, 1] + norm_got[0, 2]
    last = []
    for stage, sent, landed in ((1, (u0, u1, u2), (b0, b1, b2)), (2, (v0, v1, v2), (c0, c1, c2))):
        line = []
        for p, order in enumerate(ORDERS):
            sent[p][...] = narrow(values[p])
            for o in range(1, 4):
                line.append(
                    copies.start(sent[p], landed[p].at[o - 1], peer(order[stage], o))
                )
        for o in range(1, 4):
            line.append(
                copies.start(norm_sum.at[stage], norm_got.at[stage, o - 1], peer(stage, o))
            )
        if stage == 1:
            arrive(held)
            last.append(copies.start(coef.at[:split], got_last.at[:split], partner))
        arrive(line)
        for p in range(len(ORDERS)):
            for o in range(3):
                values[p] = values[p] + wide(landed[p][o])
        norm_sum[stage + 1] = (
            norm_sum[stage] + norm_got[stage, 0] + norm_got[stage, 1] + norm_got[stage, 2]
        )

    back = []
    for p, (order, (base, size)) in enumerate(zip(ORDERS, NEW_PARTS)):
        piece = size // 4
        start = base + coords[order[0]] * piece
        for i in range(piece):
            norm = norm_sum[3, pl.ds(lax.div(start + i, 8), 1), :]
            coef[split + start + i] = narrow(values[p][i] / (norm + damping))
        block = coef.at[pl.ds(split + start, piece)]
        for o in range(1, 4):
            back.append(copies.start(block, block, peer(order[0], o)))
    out_ref[core, :split] = coef[:split]
    last[0].wait_recv()
    out_ref[1 - core, :split] = got_last[:split]
    arrive(back)
    last.append(copies.start(coef.at[split:], got_last.at[split:], partner))
    out_ref[core, split:] = coef[split:]
    last[1].wait_recv()
    out_ref[1 - core, split:] = got_last[split:]
    copies.finish()


def sums_call(shard, cross, norms):
    fresh, tiles = cross.shape[1], norms.shape[0]
    blocks = shard.shape[0] * 16 + fresh
    bf, f32, vmem = jnp.bfloat16, jnp.float32, pltpu.VMEM
    scratch = [
        vmem((blocks, 16, 128), bf),
        vmem((blocks, 16, 128), bf),
        vmem((fresh, 16, 128), bf),
        vmem((tiles, 128), f32),
        vmem((fresh, 16, 128), f32),
        vmem((fresh, 16, 128), bf),
        vmem((4, tiles, 128), f32),
        vmem((3, 3, tiles, 128), f32),
    ]
    scratch += pieces(NEW_PARTS, (3,), 4, bf) * 3 + pieces(NEW_PARTS, (), 4, bf) * 2
    copies = 2 + 9 + 12 + 9 + 12 + 12 + 9 + 2
    scratch += [pltpu.SemaphoreType.DMA((copies,))] * 2
    return pl.pallas_call(
        sums_kernel,
        out_shape=jax.ShapeDtypeStruct((2, blocks, 16, 128), bf),
        in_specs=[pl.BlockSpec(memory_space=vmem)] * 3,
        out_specs=pl.BlockSpec(memory_space=vmem),
        scratch_shapes=scratch,
        compiler_params=pltpu.CompilerParams(
            collective_id=1, has_side_effects=True, vmem_limit_bytes=SUMS_VMEM
        ),
        name="sums",
    )(shard, cross, norms)


def residual_kernel(factor_ref, new_ref, targets_ref, coef_ref, out_ref, turned_ref):
    held = factor_ref.shape[1]

    @pl.when(pl.program_id(0) == 0)
    def _():
        for t in range(turned_ref.shape[1] // 128):
            lanes = slice(t * 128, (t + 1) * 128)
            turned_ref[:, lanes] = coef_ref[:, t * 8 : (t + 1) * 8].reshape(-1, 128)

    fitted = dot_nt(factor_ref[...], turned_ref[:, :held])
    fitted = fitted + dot_nn(turned_ref[:, held:], new_ref[...]).T
    out_ref[...] = targets_ref[...].astype(jnp.float32) - fitted


def residual_call(factor, new, targets, coef):
    pts, held = factor.shape
    wanted = targets.shape[1]
    return pl.pallas_call(
        residual_kernel,
        grid=(pts // TILE_PTS,),
        out_shape=jax.ShapeDtypeStruct((pts, wanted), jnp.float32),
        in_specs=[
            pl.BlockSpec((TILE_PTS, held), lambda i: (i, 0)),
            pl.BlockSpec((BLOCK, TILE_PTS), lambda i: (0, i)),
            pl.BlockSpec((TILE_PTS, wanted), lambda i: (i, 0)),
            pl.BlockSpec(coef.shape, lambda i: (0, 0, 0, 0), pipeline_mode=pl.Buffered(1)),
        ],
        out_specs=pl.BlockSpec((TILE_PTS, wanted), lambda i: (i, 0)),
        scratch_shapes=[pltpu.VMEM((wanted, held + BLOCK), jnp.bfloat16)],
        compiler_params=pltpu.CompilerParams(vmem_limit_bytes=RESIDUAL_VMEM),
        name="residual",
    )(factor, new, targets, coef)


def on_device(points, factor, targets, pivot_slots, pivot_counts):
    own = rows_call(pivot_slots, points, factor)
    padded, shard = gather_call(own, targets, factor)
    positions = padded_positions(pivot_counts, pivot_slots.shape[1])
    new_columns, cross, norms = local_call(padded, positions, points, factor, targets)
    coef = sums_call(shard, cross, norms)
    residual_next = residual_call(factor, new_columns, targets, coef)
    return (new_columns, residual_next)


def solution(mesh):
    return jax.shard_map(
        on_device,
        mesh=mesh,
        in_specs=(
            P(("row", "col"), None),
            P(("row", "col"), None),
            P(("row", "col"), None),
            P(("row", "col"), None),
            P(),
        ),
        out_specs=(P(None, ("row", "col")), P(("row", "col"), None)),
        check_vma=False,
    )
```

```python
import functools

import jax
import jax.numpy as jnp
from jax import lax
from jax.experimental import pallas as pl
from jax.experimental.pallas import tpu as pltpu
from jax.sharding import PartitionSpec as P

BLOCK = 512
PANEL = 128
SUB = 8
TILE_PTS = 512
ROWS_VMEM, GATHER_VMEM, LOCAL_VMEM, SUMS_VMEM, RESIDUAL_VMEM = (
    mib << 20 for mib in (62, 40, 38, 20, 16)
)
MESH = pl.DeviceIdType.MESH
HIGHEST = lax.Precision.HIGHEST

ridge_shift = 0.01
damping = 1.0
epsilon = 1e-06


def normalize(points):
    values = points.astype(jnp.float32)
    factor_scale = lax.rsqrt(jnp.mean(values * values, axis=1, keepdims=True) + epsilon)
    return (values * factor_scale).astype(jnp.bfloat16)


def padded_positions(pivot_counts, slot_cap):
    starts = jnp.cumsum(pivot_counts) - pivot_counts
    slot = jnp.arange(slot_cap, dtype=jnp.int32)[None, :]
    place_of = jnp.where(slot < pivot_counts[:, None], starts[:, None] + slot, -1)
    return place_of.astype(jnp.int32).reshape(1, -1)


def dot_nt(a, b):
    return lax.dot_general(a, b, (((1,), (1,)), ((), ())), preferred_element_type=jnp.float32)


def dot_nn(a, b):
    return jnp.dot(a, b, preferred_element_type=jnp.float32)


def put_blocks(acc, norms, cross_ref, norm_ref):
    for t in range(norms.shape[1] // 128):
        lanes = slice(t * 128, (t + 1) * 128)
        norm_ref[t : t + 1, :] = norms[:, lanes]
        cross_ref[:, t * 8 : (t + 1) * 8] = (
            acc[:, lanes].astype(jnp.bfloat16).reshape(2, 8, 16, 128)
        )


ORDERS = ((0, 1, 2), (1, 2, 0), (2, 0, 1))
HELD_PARTS = ((0, 48), (48, 48), (96, 32))
NEW_PARTS = ((0, 12), (12, 12), (24, 8))


def place():
    row, col = lax.axis_index("row"), lax.axis_index("col")
    core = lax.rem(row, 2)
    coords = (lax.div(col, 4), lax.div(row, 2), lax.rem(col, 4))
    return core, coords


def device_at(core, coords, axis=0, offset=0):
    x, y, z = (
        lax.rem(c + offset, 4) if (a == axis and offset) else c for a, c in enumerate(coords)
    )
    return (y * 2 + core, x * 4 + z)


def enter(core, coords):
    barrier = pltpu.get_barrier_semaphore()
    peers = [device_at(1 - core, coords)]
    peers += [device_at(core, coords, a, o) for a in range(3) for o in range(1, 4)]
    for peer in peers:
        pl.semaphore_signal(barrier, inc=1, device_id=peer, device_id_type=MESH)
    pl.semaphore_wait(barrier, len(peers))


def load_tiles(src, buf, sem):
    loads = []
    for i in range(buf.shape[0]):
        tile = src.at[pl.ds(i * TILE_PTS, TILE_PTS), :]
        loads.append(pltpu.make_async_copy(tile, buf.at[i], sem.at[i]))
        loads[i].start()
    return loads


class Copies:
    def __init__(self, send, recv):
        self.send, self.recv, self.started = send, recv, []

    def start(self, src, dst, device):
        k = len(self.started)
        copy = pltpu.make_async_remote_copy(
            src_ref=src, dst_ref=dst, send_sem=self.send.at[k], recv_sem=self.recv.at[k],
            device_id=device, device_id_type=MESH,
        )
        copy.start()
        self.started.append(copy)
        return copy

    def finish(self):
        for copy in self.started:
            copy.wait_send()


def arrive(copies):
    for copy in copies:
        copy.wait_recv()


def wide(value):
    return value.astype(jnp.float32)


def narrow(value):
    return value.astype(jnp.bfloat16)


def rows_kernel(slots_ref, points_ref, factor_ref, out_ref, pbuf, fbuf, psem, fsem):
    cap = pbuf.shape[0]
    copies = []
    for s in range(cap):
        base = pl.multiple_of(lax.div(slots_ref[0, s], SUB) * SUB, SUB)
        for src, buf, sem in ((points_ref, pbuf, psem), (factor_ref, fbuf, fsem)):
            copy = pltpu.make_async_copy(src.at[pl.ds(base, SUB), :], buf.at[s], sem.at[s])
            copy.start()
            copies.append(copy)
    for copy in copies:
        copy.wait()

    def picked(buf):
        sub = lax.broadcasted_iota(jnp.int32, buf.shape[1:], 0)
        out = jnp.zeros(buf.shape[1:], jnp.float32)
        for s in range(cap):
            offset = lax.rem(slots_ref[0, s], SUB)
            row = jnp.sum(
                jnp.where(sub == offset, buf[s].astype(jnp.float32), 0.0), axis=0, keepdims=True
            )
            out = jnp.where(sub == s, row, out)
        return out

    both = (normalize(picked(pbuf)), picked(fbuf).astype(jnp.bfloat16))
    t = 0
    for rows in both:
        for k in range(rows.shape[1] // 128):
            out_ref[t] = rows[:, k * 128 : (k + 1) * 128]
            t += 1


def rows_call(pivot_slots, points, factor):
    cap = pivot_slots.shape[1]
    features, held = points.shape[1], factor.shape[1]
    return pl.pallas_call(
        rows_kernel,
        out_shape=jax.ShapeDtypeStruct(((features + held) // 128, cap, 128), jnp.bfloat16),
        in_specs=[
            pl.BlockSpec(memory_space=pltpu.SMEM),
            pl.BlockSpec(memory_space=pl.ANY),
            pl.BlockSpec(memory_space=pl.ANY),
        ],
        out_specs=pl.BlockSpec(memory_space=pltpu.VMEM),
        scratch_shapes=[
            pltpu.VMEM((cap, SUB, features), jnp.bfloat16),
            pltpu.VMEM((cap, SUB, held), jnp.bfloat16),
            pltpu.SemaphoreType.DMA((cap,)),
            pltpu.SemaphoreType.DMA((cap,)),
        ],
        compiler_params=pltpu.CompilerParams(vmem_limit_bytes=ROWS_VMEM),
        name="pivot_rows",
    )(pivot_slots, points, factor)


SPANS = ((0, 4, 7), (7, 11, 14), (14, 17, 20))


def gather_kernel(
    own_ref, targets_ref, factor_ref, out_ref, shard_ref, acc_ref, x_ref, n_ref, got0, norm_got0,
    sum0, out0, norm_sum, norm_got, a0, a1, a2, b0, b1, b2, c0, c1, c2, s0, s1, s2, u0, u1, u2,
    v0, v1, v2, fbuf, fsem, send, recv,
):
    core, coords = place()
    partner = device_at(1 - core, coords)
    loads = load_tiles(factor_ref, fbuf, fsem)
    enter(core, coords)
    copies = Copies(send, recv)

    def peer(axis, offset):
        return device_at(core, coords, axis, offset)

    def region(low, high, whole=(), axis=None, at=None):
        x, y, z = (
            slice(None) if a in whole else (at if a == axis else c)
            for a, c in enumerate(coords)
        )
        return out_ref.at[y, core, x, z, low:high]

    def push(block, device):
        return copies.start(block, block, device)

    first = []
    for order, (low, _, high) in zip(ORDERS, SPANS):
        first.append([
            copies.start(own_ref.at[low:high], region(low, high), peer(order[0], o))
            for o in (2, 1, 3)
        ])
    x, y, z = coords
    out_ref[y, core, x, z] = own_ref[...]
    squares = jnp.zeros((SUB, factor_ref.shape[1]), jnp.float32)
    chunks = factor_ref.shape[0] // TILE_PTS

    def add_chunk(i, squares):
        at = slice(i * TILE_PTS, (i + 1) * TILE_PTS)
        loads[i].wait()
        value = dot_nn(targets_ref[at, :].T, fbuf[i])
        acc_ref[...] = value if i == 0 else acc_ref[...] + value
        values = wide(fbuf[i])
        return squares + jnp.sum((values * values).reshape(-1, SUB, values.shape[1]), axis=0)

    squares = add_chunk(0, squares)
    second = []
    for p, (order, (low, _, high)) in enumerate(zip(ORDERS, SPANS)):
        arrive(first[p])
        block = region(low, high, order[:1])
        second.append([push(block, peer(order[1], o)) for o in (2, 1, 3)])
    for i in range(1, chunks):
        squares = add_chunk(i, squares)
    put_blocks(acc_ref[...], jnp.sum(squares, axis=0, keepdims=True), x_ref, n_ref)
    zero = [
        copies.start(x_ref.at[1 - core], got0, partner),
        copies.start(n_ref, norm_got0, partner),
    ]
    third, across = [], []
    for p, (order, (low, mid, high)) in enumerate(zip(ORDERS, SPANS)):
        arrive(second[p])
        left, right = peer(order[2], 3), peer(order[2], 1)
        halves = [region(a, b, order[:2]) for a, b in ((low, mid), (mid, high))]
        right_low = push(halves[0], right)
        left_high = push(halves[1], left)
        right_high = push(halves[1], right)
        left_low = push(halves[0], left)
        third.append((right_low, left_high, right_high, left_low))
        across.append(push(region(low, high, order[:2]), partner))

    arrive(zero)
    sum0[...] = wide(x_ref[core]) + wide(got0[...])
    out0[...] = narrow(sum0[...])
    norm_sum[0] = n_ref[...] + norm_got0[...]
    one, starts = [], []
    for p, (order, (base, size)) in enumerate(zip(ORDERS, HELD_PARTS)):
        here, piece = coords[order[0]], size // 4
        for o in range(1, 4):
            there = lax.rem(here + o, 4)
            one.append(
                copies.start(
                    out0.at[pl.ds(base + there * piece, piece)],
                    (a0, a1, a2)[p].at[o - 1],
                    peer(order[0], o),
                )
            )
        starts.append(base + here * piece)
    for o in range(1, 4):
        one.append(copies.start(norm_sum.at[0], norm_got.at[0, o - 1], peer(0, o)))

    relays = []
    for p, (order, (low, mid, high)) in enumerate(zip(ORDERS, SPANS)):
        axis = order[2]
        before, after = (lax.rem(coords[axis] + o, 4) for o in (3, 1))
        third[p][0].wait_recv()
        relay = push(region(low, mid, order[:2], axis, before), peer(axis, 1))
        third[p][1].wait_recv()
        relays.append((relay, push(region(mid, high, order[:2], axis, after), peer(axis, 3))))

    arrive(one)
    two = []
    for p, (order, (base, size)) in enumerate(zip(ORDERS, HELD_PARTS)):
        here, piece, fours = coords[order[1]], size // 16, size // 4
        value = sum0[pl.ds(starts[p], fours)]
        for o in range(3):
            value = value + wide((a0, a1, a2)[p][o])
        (s0, s1, s2)[p][...] = value
        (u0, u1, u2)[p][...] = narrow(value)
        for o in range(1, 4):
            there = lax.rem(here + o, 4)
            two.append(
                copies.start(
                    (u0, u1, u2)[p].at[pl.ds(there * piece, piece)],
                    (b0, b1, b2)[p].at[o - 1],
                    peer(order[1], o),
                )
            )
        starts[p] = starts[p] + here * piece
    norm_sum[1] = norm_sum[0] + norm_got[0, 0] + norm_got[0, 1] + norm_got[0, 2]
    for o in range(1, 4):
        two.append(copies.start(norm_sum.at[1], norm_got.at[1, o - 1], peer(1, o)))

    for p, (order, (low, mid, high)) in enumerate(zip(ORDERS, SPANS)):
        axis = order[2]
        before, after = (lax.rem(coords[axis] + o, 4) for o in (3, 1))
        third[p][2].wait_recv()
        across.append(push(region(low, high, order[:2], axis, before), partner))
        third[p][3].wait_recv()
        across.append(push(region(low, high, order[:2], axis, after), partner))

    arrive(two)
    three, values = [], []
    for p, (order, (base, size)) in enumerate(zip(ORDERS, HELD_PARTS)):
        here, piece = coords[order[1]], size // 16
        value = (s0, s1, s2)[p][pl.ds(here * piece, piece)]
        for o in range(3):
            value = value + wide((b0, b1, b2)[p][o])
        values.append(value)
        (v0, v1, v2)[p][...] = narrow(value)
        for o in range(1, 4):
            three.append(
                copies.start((v0, v1, v2)[p], (c0, c1, c2)[p].at[o - 1], peer(order[2], o))
            )
    norm_sum[2] = norm_sum[1] + norm_got[1, 0] + norm_got[1, 1] + norm_got[1, 2]
    for o in range(1, 4):
        three.append(copies.start(norm_sum.at[2], norm_got.at[2, o - 1], peer(2, o)))

    for p, (order, (low, mid, high)) in enumerate(zip(ORDERS, SPANS)):
        axis = order[2]
        opposite = lax.rem(coords[axis] + 2, 4)
        for copy, (a, b) in zip(relays[p], ((low, mid), (mid, high))):
            copy.wait_recv()
            across.append(push(region(a, b, order[:2], axis, opposite), partner))

    arrive(three)
    norm_sum[3] = norm_sum[2] + norm_got[2, 0] + norm_got[2, 1] + norm_got[2, 2]
    at = 0
    for p, (order, (base, size)) in enumerate(zip(ORDERS, HELD_PARTS)):
        value = values[p]
        for o in range(3):
            value = value + wide((c0, c1, c2)[p][o])
        for i in range(size // 16):
            norm = norm_sum[3, pl.ds(lax.div(starts[p] + i, 8), 1), :]
            shard_ref[at] = narrow(value[i] / (norm + damping))
            at += 1
    arrive(across)
    copies.finish()


def pieces(parts, lead, share, kind):
    return [pltpu.VMEM((*lead, size // share, 16, 128), kind) for _, size in parts]


def gather_call(own, targets, factor):
    copies = 9 + 9 + 12 + 3 + 6 + 6 + 6 + 2 + 3 * 12
    held, wanted = factor.shape[1], targets.shape[1]
    tiles = held // 128
    blocks = tiles * 8
    bf, f32, vmem = jnp.bfloat16, jnp.float32, pltpu.VMEM
    scratch = [
        vmem((wanted, held), f32),
        vmem((2, blocks, 16, 128), bf),
        vmem((tiles, 128), f32),
        vmem((blocks, 16, 128), bf),
        vmem((tiles, 128), f32),
        vmem((blocks, 16, 128), f32),
        vmem((blocks, 16, 128), bf),
        vmem((4, tiles, 128), f32),
        vmem((3, 3, tiles, 128), f32),
    ]
    scratch += pieces(HELD_PARTS, (3,), 4, bf) + pieces(HELD_PARTS, (3,), 16, bf)
    scratch += pieces(HELD_PARTS, (3,), 16, bf) + pieces(HELD_PARTS, (), 4, f32)
    scratch += pieces(HELD_PARTS, (), 4, bf) + pieces(HELD_PARTS, (), 16, bf)
    steps = factor.shape[0] // TILE_PTS
    scratch += [vmem((steps, TILE_PTS, held), bf), pltpu.SemaphoreType.DMA((steps,))]
    scratch += [pltpu.SemaphoreType.DMA((copies,))] * 2
    out, shard = pl.pallas_call(
        gather_kernel,
        out_shape=(
            jax.ShapeDtypeStruct((4, 2, 4, 4, *own.shape), bf),
            jax.ShapeDtypeStruct((blocks // 16, 16, 128), bf),
        ),
        in_specs=[pl.BlockSpec(memory_space=vmem)] * 2 + [pl.BlockSpec(memory_space=pl.ANY)],
        out_specs=[pl.BlockSpec(memory_space=vmem)] * 2,
        scratch_shapes=scratch,
        compiler_params=pltpu.CompilerParams(
            collective_id=2, has_side_effects=True, vmem_limit_bytes=GATHER_VMEM
        ),
        name="gather_rows",
    )(own, targets, factor)
    return out.reshape(128, *own.shape), shard


MICRO = 16


def eliminate(rows, first):
    groups = len(rows)
    sub = lax.broadcasted_iota(jnp.int32, (SUB, PANEL), 0)
    rows = [list(values) for values in rows]

    def over_sublanes(value, k):
        return jnp.broadcast_to(value[k : k + 1, :], (SUB, PANEL))

    for m in range(0, groups, MICRO // SUB):
        cols = {}
        for r in range(m, groups):
            for k in range(MICRO):
                lane = first + m * SUB + k
                cols[r, k] = jnp.broadcast_to(rows[r][0][:, lane : lane + 1], (SUB, PANEL))
        for k in range(MICRO):
            g, at = m + k // SUB, k % SUB
            if at == 0:
                roots = jnp.ones((SUB, PANEL), jnp.float32)
            root = lax.rsqrt(over_sublanes(cols[g, k], at))
            roots = jnp.where(sub == at, root, roots)
            scale = root * root
            ahead = {j: over_sublanes(cols[g, j], at) for j in range(k + 1, MICRO)}
            pivot_rows = [over_sublanes(value, at) for value in rows[g]]
            for r in range(g, groups):
                if r == g and at == SUB - 1:
                    continue
                c = cols[r, k] * scale
                if r == g:
                    c = jnp.where(sub > at, c, 0.0)
                for j in range(k + 1, MICRO):
                    cols[r, j] = cols[r, j] - c * ahead[j]
                rows[r] = [value - c * row for value, row in zip(rows[r], pivot_rows)]
            if at == SUB - 1:
                rows[g] = [value * roots for value in rows[g]]
    return rows


def panel_inverse(block):
    half, groups = PANEL // 2, PANEL // 2 // SUB
    sub = lax.broadcasted_iota(jnp.int32, (SUB, PANEL), 0)
    lane = lax.broadcasted_iota(jnp.int32, (SUB, PANEL), 1)

    def unit(row):
        return (lane == sub + row).astype(jnp.float32)

    pieces = [block[SUB * r : SUB * (r + 1), :] for r in range(2 * groups)]
    top = eliminate([(pieces[r], unit(SUB * r)) for r in range(groups)], 0)
    right = jnp.concatenate([values[0] for values in top], axis=0)
    upper = jnp.concatenate([values[1] for values in top], axis=0)
    wide = lax.broadcasted_iota(jnp.int32, (half, PANEL), 1)
    both = jnp.where(wide < half, upper, right)
    change = jnp.dot(right.T, both, precision=HIGHEST, preferred_element_type=jnp.float32)
    low = []
    for r in range(groups, 2 * groups):
        piece = jnp.where(lane < half, 0.0, pieces[r])
        low.append((piece - change[SUB * r : SUB * (r + 1), :], unit(SUB * r)))
    low = eliminate(low, half)
    lower = [jnp.where(lane < half, values[0], values[1]) for values in low]
    return jnp.concatenate([upper, *lower], axis=0)


def local_kernel(
    pad_ref, pos_ref, targets_ref, points_ref, factor_ref,
    new_ref, cross_ref, norm_ref,
    ps_ref, pf_ref, sel_ref, a_ref, w_ref, lo_ref, hi_ref, down_hi, down_lo, fbuf, fsem,
):
    tiles = fbuf.shape[0]
    loads = load_tiles(factor_ref, fbuf, fsem)
    padded = pos_ref.shape[1]
    sel_ref[...] = jnp.where(
        lax.broadcasted_iota(jnp.int32, (BLOCK, padded), 0) == pos_ref[...], 1.0, 0.0
    ).astype(jnp.bfloat16)
    ahead = ps_ref.shape[1] // 128
    for t in range(0, pad_ref.shape[1], 2):
        pair = [
            pad_ref[:, k].astype(jnp.float32).reshape(padded, 128).astype(jnp.bfloat16)
            for k in (t, t + 1)
        ]
        rows = dot_nn(sel_ref[...], jnp.concatenate(pair, axis=1)).astype(jnp.bfloat16)
        if t < ahead:
            ps_ref[:, t * 128 : (t + 2) * 128] = rows
        else:
            pf_ref[:, (t - ahead) * 128 : (t - ahead + 2) * 128] = rows

    panels = BLOCK // PANEL
    total = jnp.zeros((1, BLOCK), jnp.float32)
    for r in range(panels):
        at = slice(r * PANEL, (r + 1) * PANEL)
        inter = dot_nt(pf_ref[at, :], pf_ref[...])
        total = total + jnp.sum(jnp.abs(inter), axis=0, keepdims=True)
        kern = jnp.exp(dot_nt(ps_ref[at, :], ps_ref[...]) / ps_ref.shape[1] - 1.0)
        a_ref[at, :] = kern - inter
    shift = ridge_shift + jnp.max(total)
    eye = lax.broadcasted_iota(jnp.int32, (PANEL, PANEL), 0) == lax.broadcasted_iota(
        jnp.int32, (PANEL, PANEL), 1
    )
    for load in loads:
        load.wait()

    def exact(a, b):
        return jnp.dot(a, b, precision=HIGHEST, preferred_element_type=jnp.float32)

    for j in range(panels):
        at = slice(j * PANEL, (j + 1) * PANEL)
        inv = panel_inverse(a_ref[at, at] + jnp.where(eye, shift, 0.0))
        if j:
            done = jnp.concatenate([exact(inv, w_ref[at, : j * PANEL]), inv], axis=1)
        else:
            done = inv
        high = done.astype(jnp.bfloat16)
        hi_ref[at, : (j + 1) * PANEL] = high
        lo_ref[at, : (j + 1) * PANEL] = (done - high.astype(jnp.float32)).astype(jnp.bfloat16)
        if j + 1 < panels:
            rest = slice((j + 1) * PANEL, BLOCK)
            hi_ref[at, rest] = jnp.zeros((PANEL, BLOCK - (j + 1) * PANEL), jnp.bfloat16)
            lo_ref[at, rest] = jnp.zeros((PANEL, BLOCK - (j + 1) * PANEL), jnp.bfloat16)
            right = exact(inv, a_ref[at, rest])
            for r in range(j + 1, panels):
                rows = slice(r * PANEL, (r + 1) * PANEL)
                skip = (r - j - 1) * PANEL
                left = right[:, skip : skip + PANEL].T
                a_ref[rows, r * PANEL :] = a_ref[rows, r * PANEL :] - exact(left, right[:, skip:])
                gone = exact(left, done)
                if j:
                    w_ref[rows, : j * PANEL] = w_ref[rows, : j * PANEL] - gone[:, : j * PANEL]
                w_ref[rows, at] = -gone[:, j * PANEL :]
        tile = slice(j * TILE_PTS, (j + 1) * TILE_PTS)
        scaled = normalize(points_ref[tile, :])
        down = jnp.exp(dot_nt(ps_ref[...], scaled) / scaled.shape[1] - 1.0) - dot_nt(
            pf_ref[...], fbuf[j]
        )
        high = down.astype(jnp.bfloat16)
        down_hi[:, tile] = high
        down_lo[:, tile] = (down - high.astype(jnp.float32)).astype(jnp.bfloat16)

    half = BLOCK // 2
    wanted = targets_ref.shape[1]
    acc = jnp.zeros((wanted, BLOCK), jnp.float32)
    nsq = jnp.zeros((BLOCK, 128), jnp.float32)
    for i in range(tiles):
        tile = slice(i * TILE_PTS, (i + 1) * TILE_PTS)
        for top, wide in ((0, half), (half, BLOCK)):
            at = slice(top, top + half)
            value = (
                dot_nn(hi_ref[at, :wide], down_hi[:wide, tile])
                + dot_nn(hi_ref[at, :wide], down_lo[:wide, tile])
                + dot_nn(lo_ref[at, :wide], down_hi[:wide, tile])
            )
            new_ref[at, tile] = value.astype(jnp.bfloat16)
        new = new_ref[:, tile]
        acc = acc + dot_nt(targets_ref[tile, :].T, new)
        wide_new = new.astype(jnp.float32)
        squares = wide_new * wide_new
        for t in range(TILE_PTS // 128):
            nsq = nsq + squares[:, t * 128 : (t + 1) * 128]
    norms = jnp.sum(nsq.T, axis=0, keepdims=True)
    put_blocks(acc, norms, cross_ref, norm_ref)


def local_call(padded, positions, points, factor, targets):
    pts, held = factor.shape
    features = points.shape[1]
    tiles = BLOCK // 128
    bf, f32, vmem = jnp.bfloat16, jnp.float32, pltpu.VMEM
    return pl.pallas_call(
        local_kernel,
        out_shape=(
            jax.ShapeDtypeStruct((BLOCK, pts), bf),
            jax.ShapeDtypeStruct((2, tiles * 8, 16, 128), bf),
            jax.ShapeDtypeStruct((tiles, 128), f32),
        ),
        in_specs=[pl.BlockSpec(memory_space=vmem)] * 4 + [pl.BlockSpec(memory_space=pl.ANY)],
        out_specs=[pl.BlockSpec(memory_space=vmem)] * 3,
        scratch_shapes=[
            vmem((BLOCK, features), bf),
            vmem((BLOCK, held), bf),
            vmem((BLOCK, positions.shape[1]), bf),
            vmem((BLOCK, BLOCK), f32),
            vmem((BLOCK, BLOCK), f32),
            vmem((BLOCK, BLOCK), bf),
            vmem((BLOCK, BLOCK), bf),
            vmem((BLOCK, pts), bf),
            vmem((BLOCK, pts), bf),
            vmem((pts // TILE_PTS, TILE_PTS, held), bf),
            pltpu.SemaphoreType.DMA((pts // TILE_PTS,)),
        ],
        compiler_params=pltpu.CompilerParams(vmem_limit_bytes=LOCAL_VMEM),
        name="local_block",
    )(padded, positions, targets, points, factor)


def sums_kernel(
    shard_ref, x_ref, n_ref, factor_ref, out_ref, fit_ref, turned_ref, coef, got_last, got0, norm_got0, sum0, out0, norm_sum,
    norm_got, a0, a1, a2, b0, b1, b2, c0, c1, c2, u0, u1, u2, v0, v1, v2, send, recv,
):
    core, coords = place()
    partner = device_at(1 - core, coords)
    enter(core, coords)
    copies = Copies(send, recv)
    split = coef.shape[0] - x_ref.shape[1]
    tiles = factor_ref.shape[0] // TILE_PTS

    def peer(axis, offset):
        return device_at(core, coords, axis, offset)

    zero = [
        copies.start(x_ref.at[1 - core], got0, partner),
        copies.start(n_ref, norm_got0, partner),
    ]
    held, at = [], 0
    for order, (base, size) in zip(ORDERS, HELD_PARTS):
        piece = size // 16
        place_of = base + coords[order[0]] * (size // 4) + coords[order[1]] * piece
        for o in range(1, 4):
            held.append(
                copies.start(
                    shard_ref.at[at : at + piece], coef.at[pl.ds(place_of, piece)],
                    peer(order[1], o),
                )
            )
        coef[pl.ds(place_of, piece)] = shard_ref[at : at + piece]
        at += piece

    def fit(tiles):
        for i in tiles:
            at = slice(i * TILE_PTS, (i + 1) * TILE_PTS)
            fit_ref[at, :] = dot_nt(factor_ref[at, :], turned_ref[...])

    arrive(zero)
    sum0[...] = wide(x_ref[core]) + wide(got0[...])
    out0[...] = narrow(sum0[...])
    norm_sum[0] = n_ref[...] + norm_got0[...]
    one = []
    for p, (order, (base, size)) in enumerate(zip(ORDERS, NEW_PARTS)):
        here, piece = coords[order[0]], size // 4
        for o in range(1, 4):
            there = lax.rem(here + o, 4)
            one.append(
                copies.start(
                    out0.at[pl.ds(base + there * piece, piece)],
                    (a0, a1, a2)[p].at[o - 1],
                    peer(order[0], o),
                )
            )
    for o in range(1, 4):
        one.append(copies.start(norm_sum.at[0], norm_got.at[0, o - 1], peer(0, o)))

    arrive(held)
    held = []
    for order, (base, size) in zip(ORDERS, HELD_PARTS):
        block = coef.at[pl.ds(base + coords[order[0]] * (size // 4), size // 4)]
        for o in range(1, 4):
            held.append(copies.start(block, block, peer(order[0], o)))

    values = []
    arrive(one)
    for p, (order, (base, size)) in enumerate(zip(ORDERS, NEW_PARTS)):
        piece = size // 4
        value = sum0[pl.ds(base + coords[order[0]] * piece, piece)]
        for o in range(3):
            value = value + wide((a0, a1, a2)[p][o])
        values.append(value)
    norm_sum[1] = norm_sum[0] + norm_got[0, 0] + norm_got[0, 1] + norm_got[0, 2]
    last = []
    for stage, sent, landed in ((1, (u0, u1, u2), (b0, b1, b2)), (2, (v0, v1, v2), (c0, c1, c2))):
        line = []
        for p, order in enumerate(ORDERS):
            sent[p][...] = narrow(values[p])
            for o in range(1, 4):
                line.append(
                    copies.start(sent[p], landed[p].at[o - 1], peer(order[stage], o))
                )
        for o in range(1, 4):
            line.append(
                copies.start(norm_sum.at[stage], norm_got.at[stage, o - 1], peer(stage, o))
            )
        if stage == 1:
            arrive(held)
            last.append(copies.start(coef.at[:split], got_last.at[:split], partner))
        else:
            last[0].wait_recv()
            rows = turned_ref.shape[0] // 2
            for t in range(split // 8):
                lanes = slice(t * 128, (t + 1) * 128)
                for half, blocks in ((core, coef), (1 - core, got_last)):
                    at = pl.ds(pl.multiple_of(half * rows, rows), rows)
                    turned_ref[at, lanes] = blocks[t * 8 : (t + 1) * 8].reshape(rows, 128)
            fit(range(tiles // 2))
        arrive(line)
        for p in range(len(ORDERS)):
            for o in range(3):
                values[p] = values[p] + wide(landed[p][o])
        norm_sum[stage + 1] = (
            norm_sum[stage] + norm_got[stage, 0] + norm_got[stage, 1] + norm_got[stage, 2]
        )

    back = []
    for p, (order, (base, size)) in enumerate(zip(ORDERS, NEW_PARTS)):
        piece = size // 4
        start = base + coords[order[0]] * piece
        for i in range(piece):
            norm = norm_sum[3, pl.ds(lax.div(start + i, 8), 1), :]
            coef[split + start + i] = narrow(values[p][i] / (norm + damping))
        block = coef.at[pl.ds(split + start, piece)]
        for o in range(1, 4):
            back.append(copies.start(block, block, peer(order[0], o)))
    fit(range(tiles // 2, tiles))
    arrive(back)
    last.append(copies.start(coef.at[split:], got_last.at[split:], partner))
    out_ref[core] = coef[split:]
    last[1].wait_recv()
    out_ref[1 - core] = got_last[split:]
    copies.finish()


def sums_call(shard, cross, norms, factor, wanted):
    fresh, tiles = cross.shape[1], norms.shape[0]
    blocks = shard.shape[0] * 16 + fresh
    bf, f32, vmem = jnp.bfloat16, jnp.float32, pltpu.VMEM
    pts, held = factor.shape
    scratch = [
        vmem((wanted, held), bf),
        vmem((blocks, 16, 128), bf),
        vmem((blocks, 16, 128), bf),
        vmem((fresh, 16, 128), bf),
        vmem((tiles, 128), f32),
        vmem((fresh, 16, 128), f32),
        vmem((fresh, 16, 128), bf),
        vmem((4, tiles, 128), f32),
        vmem((3, 3, tiles, 128), f32),
    ]
    scratch += pieces(NEW_PARTS, (3,), 4, bf) * 3 + pieces(NEW_PARTS, (), 4, bf) * 2
    copies = 2 + 9 + 12 + 9 + 12 + 12 + 9 + 2
    scratch += [pltpu.SemaphoreType.DMA((copies,))] * 2
    return pl.pallas_call(
        sums_kernel,
        out_shape=(
            jax.ShapeDtypeStruct((2, fresh, 16, 128), bf),
            jax.ShapeDtypeStruct((pts, wanted), f32),
        ),
        in_specs=[pl.BlockSpec(memory_space=vmem)] * 4,
        out_specs=[pl.BlockSpec(memory_space=vmem)] * 2,
        scratch_shapes=scratch,
        compiler_params=pltpu.CompilerParams(
            collective_id=1, has_side_effects=True, vmem_limit_bytes=SUMS_VMEM
        ),
        name="sums",
    )(shard, cross, norms, factor)


def residual_kernel(new_ref, targets_ref, fit_ref, coef_ref, out_ref):
    turned = jnp.concatenate(
        [
            coef_ref[:, t * 8 : (t + 1) * 8].reshape(-1, 128)
            for t in range(coef_ref.shape[1] // 8)
        ],
        axis=1,
    )
    fitted = fit_ref[...] + dot_nn(turned, new_ref[...]).T
    out_ref[...] = wide(targets_ref[...]) - fitted


def residual_call(new, targets, fit, coef):
    pts, wanted = targets.shape
    return pl.pallas_call(
        residual_kernel,
        grid=(pts // TILE_PTS,),
        out_shape=jax.ShapeDtypeStruct((pts, wanted), jnp.float32),
        in_specs=[
            pl.BlockSpec((BLOCK, TILE_PTS), lambda i: (0, i)),
            pl.BlockSpec((TILE_PTS, wanted), lambda i: (i, 0)),
            pl.BlockSpec((TILE_PTS, wanted), lambda i: (i, 0)),
            pl.BlockSpec(coef.shape, lambda i: (0, 0, 0, 0), pipeline_mode=pl.Buffered(1)),
        ],
        out_specs=pl.BlockSpec((TILE_PTS, wanted), lambda i: (i, 0)),
        compiler_params=pltpu.CompilerParams(vmem_limit_bytes=RESIDUAL_VMEM),
        name="residual",
    )(new, targets, fit, coef)


def on_device(points, factor, targets, pivot_slots, pivot_counts):
    own = rows_call(pivot_slots, points, factor)
    padded, shard = gather_call(own, targets, factor)
    positions = padded_positions(pivot_counts, pivot_slots.shape[1])
    new_columns, cross, norms = local_call(padded, positions, points, factor, targets)
    coef, fit = sums_call(shard, cross, norms, factor, targets.shape[1])
    residual_next = residual_call(new_columns, targets, fit, coef)
    return (new_columns, residual_next)


def solution(mesh):
    return jax.shard_map(
        on_device,
        mesh=mesh,
        in_specs=(
            P(("row", "col"), None),
            P(("row", "col"), None),
            P(("row", "col"), None),
            P(("row", "col"), None),
            P(),
        ),
        out_specs=(P(None, ("row", "col")), P(("row", "col"), None)),
        check_vma=False,
    )
```

```python
import functools

import jax
import jax.numpy as jnp
from jax import lax
from jax.experimental import pallas as pl
from jax.experimental.pallas import tpu as pltpu
from jax.sharding import PartitionSpec as P

BLOCK = 512
PANEL = 128
SUB = 8
TILE_PTS = 512
ROWS_VMEM, GATHER_VMEM, LOCAL_VMEM, SUMS_VMEM, RESIDUAL_VMEM = (
    mib << 20 for mib in (62, 40, 38, 20, 16)
)
MESH = pl.DeviceIdType.MESH
HIGHEST = lax.Precision.HIGHEST

ridge_shift = 0.01
damping = 1.0
epsilon = 1e-06


def normalize(points):
    values = points.astype(jnp.float32)
    factor_scale = lax.rsqrt(jnp.mean(values * values, axis=1, keepdims=True) + epsilon)
    return (values * factor_scale).astype(jnp.bfloat16)


def padded_positions(pivot_counts, slot_cap):
    starts = jnp.cumsum(pivot_counts) - pivot_counts
    slot = jnp.arange(slot_cap, dtype=jnp.int32)[None, :]
    place_of = jnp.where(slot < pivot_counts[:, None], starts[:, None] + slot, -1)
    return place_of.astype(jnp.int32).reshape(1, -1)


def dot_nt(a, b):
    return lax.dot_general(a, b, (((1,), (1,)), ((), ())), preferred_element_type=jnp.float32)


def dot_nn(a, b):
    return jnp.dot(a, b, preferred_element_type=jnp.float32)


def put_blocks(acc, norms, cross_ref, norm_ref):
    for t in range(norms.shape[1] // 128):
        lanes = slice(t * 128, (t + 1) * 128)
        norm_ref[t : t + 1, :] = norms[:, lanes]
        cross_ref[:, t * 8 : (t + 1) * 8] = (
            acc[:, lanes].astype(jnp.bfloat16).reshape(2, 8, 16, 128)
        )


ORDERS = ((0, 1, 2), (1, 2, 0), (2, 0, 1))
HELD_PARTS = ((0, 48), (48, 48), (96, 32))
NEW_PARTS = ((0, 12), (12, 12), (24, 8))


def place():
    row, col = lax.axis_index("row"), lax.axis_index("col")
    core = lax.rem(row, 2)
    coords = (lax.div(col, 4), lax.div(row, 2), lax.rem(col, 4))
    return core, coords


def device_at(core, coords, axis=0, offset=0):
    x, y, z = (
        lax.rem(c + offset, 4) if (a == axis and offset) else c for a, c in enumerate(coords)
    )
    return (y * 2 + core, x * 4 + z)


def enter(core, coords):
    barrier = pltpu.get_barrier_semaphore()
    peers = [device_at(1 - core, coords)]
    peers += [device_at(core, coords, a, o) for a in range(3) for o in range(1, 4)]
    for peer in peers:
        pl.semaphore_signal(barrier, inc=1, device_id=peer, device_id_type=MESH)
    pl.semaphore_wait(barrier, len(peers))


def load_tiles(src, buf, sem):
    loads = []
    for i in range(buf.shape[0]):
        tile = src.at[pl.ds(i * TILE_PTS, TILE_PTS), :]
        loads.append(pltpu.make_async_copy(tile, buf.at[i], sem.at[i]))
        loads[i].start()
    return loads


class Copies:
    def __init__(self, send, recv):
        self.send, self.recv, self.started = send, recv, []

    def start(self, src, dst, device):
        k = len(self.started)
        copy = pltpu.make_async_remote_copy(
            src_ref=src, dst_ref=dst, send_sem=self.send.at[k], recv_sem=self.recv.at[k],
            device_id=device, device_id_type=MESH,
        )
        copy.start()
        self.started.append(copy)
        return copy

    def finish(self):
        for copy in self.started:
            copy.wait_send()


def arrive(copies):
    for copy in copies:
        copy.wait_recv()


def wide(value):
    return value.astype(jnp.float32)


def narrow(value):
    return value.astype(jnp.bfloat16)


def rows_kernel(slots_ref, points_ref, factor_ref, out_ref, pbuf, fbuf, psem, fsem):
    cap = pbuf.shape[0]
    copies = []
    for s in range(cap):
        base = pl.multiple_of(lax.div(slots_ref[0, s], SUB) * SUB, SUB)
        for src, buf, sem in ((points_ref, pbuf, psem), (factor_ref, fbuf, fsem)):
            copy = pltpu.make_async_copy(src.at[pl.ds(base, SUB), :], buf.at[s], sem.at[s])
            copy.start()
            copies.append(copy)
    for copy in copies:
        copy.wait()

    def picked(buf):
        sub = lax.broadcasted_iota(jnp.int32, buf.shape[1:], 0)
        out = jnp.zeros(buf.shape[1:], jnp.float32)
        for s in range(cap):
            offset = lax.rem(slots_ref[0, s], SUB)
            row = jnp.sum(
                jnp.where(sub == offset, buf[s].astype(jnp.float32), 0.0), axis=0, keepdims=True
            )
            out = jnp.where(sub == s, row, out)
        return out

    both = (normalize(picked(pbuf)), picked(fbuf).astype(jnp.bfloat16))
    t = 0
    for rows in both:
        for k in range(rows.shape[1] // 128):
            out_ref[t] = rows[:, k * 128 : (k + 1) * 128]
            t += 1


def rows_call(pivot_slots, points, factor):
    cap = pivot_slots.shape[1]
    features, held = points.shape[1], factor.shape[1]
    return pl.pallas_call(
        rows_kernel,
        out_shape=jax.ShapeDtypeStruct(((features + held) // 128, cap, 128), jnp.bfloat16),
        in_specs=[
            pl.BlockSpec(memory_space=pltpu.SMEM),
            pl.BlockSpec(memory_space=pl.ANY),
            pl.BlockSpec(memory_space=pl.ANY),
        ],
        out_specs=pl.BlockSpec(memory_space=pltpu.VMEM),
        scratch_shapes=[
            pltpu.VMEM((cap, SUB, features), jnp.bfloat16),
            pltpu.VMEM((cap, SUB, held), jnp.bfloat16),
            pltpu.SemaphoreType.DMA((cap,)),
            pltpu.SemaphoreType.DMA((cap,)),
        ],
        compiler_params=pltpu.CompilerParams(vmem_limit_bytes=ROWS_VMEM),
        name="pivot_rows",
    )(pivot_slots, points, factor)


SPANS = ((0, 4, 7), (7, 11, 14), (14, 17, 20))


def gather_kernel(
    own_ref, targets_ref, factor_ref, out_ref, shard_ref, acc_ref, x_ref, n_ref, got0, norm_got0,
    sum0, out0, norm_sum, norm_got, a0, a1, a2, b0, b1, b2, c0, c1, c2, s0, s1, s2, u0, u1, u2,
    v0, v1, v2, fbuf, fsem, send, recv,
):
    core, coords = place()
    partner = device_at(1 - core, coords)
    loads = load_tiles(factor_ref, fbuf, fsem)
    enter(core, coords)
    copies = Copies(send, recv)

    def peer(axis, offset):
        return device_at(core, coords, axis, offset)

    def region(low, high, whole=(), axis=None, at=None):
        x, y, z = (
            slice(None) if a in whole else (at if a == axis else c)
            for a, c in enumerate(coords)
        )
        return out_ref.at[y, core, x, z, low:high]

    def push(block, device):
        return copies.start(block, block, device)

    first = []
    for order, (low, _, high) in zip(ORDERS, SPANS):
        first.append([
            copies.start(own_ref.at[low:high], region(low, high), peer(order[0], o))
            for o in (2, 1, 3)
        ])
    x, y, z = coords
    out_ref[y, core, x, z] = own_ref[...]
    squares = jnp.zeros((SUB, factor_ref.shape[1]), jnp.float32)
    chunks = factor_ref.shape[0] // TILE_PTS

    def add_chunk(i, squares):
        at = slice(i * TILE_PTS, (i + 1) * TILE_PTS)
        loads[i].wait()
        value = dot_nn(targets_ref[at, :].T, fbuf[i])
        acc_ref[...] = value if i == 0 else acc_ref[...] + value
        values = wide(fbuf[i])
        return squares + jnp.sum((values * values).reshape(-1, SUB, values.shape[1]), axis=0)

    squares = add_chunk(0, squares)
    second = []
    for p, (order, (low, _, high)) in enumerate(zip(ORDERS, SPANS)):
        arrive(first[p])
        block = region(low, high, order[:1])
        second.append([push(block, peer(order[1], o)) for o in (2, 1, 3)])
    for i in range(1, chunks):
        squares = add_chunk(i, squares)
    put_blocks(acc_ref[...], jnp.sum(squares, axis=0, keepdims=True), x_ref, n_ref)
    zero = [
        copies.start(x_ref.at[1 - core], got0, partner),
        copies.start(n_ref, norm_got0, partner),
    ]
    arrive(zero)
    sum0[...] = wide(x_ref[core]) + wide(got0[...])
    out0[...] = narrow(sum0[...])
    norm_sum[0] = n_ref[...] + norm_got0[...]
    one, starts = [], []
    for p, (order, (base, size)) in enumerate(zip(ORDERS, HELD_PARTS)):
        here, piece = coords[order[0]], size // 4
        for o in range(1, 4):
            there = lax.rem(here + o, 4)
            one.append(
                copies.start(
                    out0.at[pl.ds(base + there * piece, piece)],
                    (a0, a1, a2)[p].at[o - 1],
                    peer(order[0], o),
                )
            )
        starts.append(base + here * piece)
    for o in range(1, 4):
        one.append(copies.start(norm_sum.at[0], norm_got.at[0, o - 1], peer(0, o)))

    third, across = [], []
    for p, (order, (low, mid, high)) in enumerate(zip(ORDERS, SPANS)):
        arrive(second[p])
        left, right = peer(order[2], 3), peer(order[2], 1)
        halves = [region(a, b, order[:2]) for a, b in ((low, mid), (mid, high))]
        right_low = push(halves[0], right)
        left_high = push(halves[1], left)
        right_high = push(halves[1], right)
        left_low = push(halves[0], left)
        third.append((right_low, left_high, right_high, left_low))
        across.append(push(region(low, high, order[:2]), partner))

    relays = []
    for p, (order, (low, mid, high)) in enumerate(zip(ORDERS, SPANS)):
        axis = order[2]
        before, after = (lax.rem(coords[axis] + o, 4) for o in (3, 1))
        third[p][0].wait_recv()
        relay = push(region(low, mid, order[:2], axis, before), peer(axis, 1))
        third[p][1].wait_recv()
        relays.append((relay, push(region(mid, high, order[:2], axis, after), peer(axis, 3))))

    arrive(one)
    two = []
    for p, (order, (base, size)) in enumerate(zip(ORDERS, HELD_PARTS)):
        here, piece, fours = coords[order[1]], size // 16, size // 4
        value = sum0[pl.ds(starts[p], fours)]
        for o in range(3):
            value = value + wide((a0, a1, a2)[p][o])
        (s0, s1, s2)[p][...] = value
        (u0, u1, u2)[p][...] = narrow(value)
        for o in range(1, 4):
            there = lax.rem(here + o, 4)
            two.append(
                copies.start(
                    (u0, u1, u2)[p].at[pl.ds(there * piece, piece)],
                    (b0, b1, b2)[p].at[o - 1],
                    peer(order[1], o),
                )
            )
        starts[p] = starts[p] + here * piece
    norm_sum[1] = norm_sum[0] + norm_got[0, 0] + norm_got[0, 1] + norm_got[0, 2]
    for o in range(1, 4):
        two.append(copies.start(norm_sum.at[1], norm_got.at[1, o - 1], peer(1, o)))

    for p, (order, (low, mid, high)) in enumerate(zip(ORDERS, SPANS)):
        axis = order[2]
        before, after = (lax.rem(coords[axis] + o, 4) for o in (3, 1))
        third[p][2].wait_recv()
        across.append(push(region(low, high, order[:2], axis, before), partner))
        third[p][3].wait_recv()
        across.append(push(region(low, high, order[:2], axis, after), partner))

    arrive(two)
    three, values = [], []
    for p, (order, (base, size)) in enumerate(zip(ORDERS, HELD_PARTS)):
        here, piece = coords[order[1]], size // 16
        value = (s0, s1, s2)[p][pl.ds(here * piece, piece)]
        for o in range(3):
            value = value + wide((b0, b1, b2)[p][o])
        values.append(value)
        (v0, v1, v2)[p][...] = narrow(value)
        for o in range(1, 4):
            three.append(
                copies.start((v0, v1, v2)[p], (c0, c1, c2)[p].at[o - 1], peer(order[2], o))
            )
    norm_sum[2] = norm_sum[1] + norm_got[1, 0] + norm_got[1, 1] + norm_got[1, 2]
    for o in range(1, 4):
        three.append(copies.start(norm_sum.at[2], norm_got.at[2, o - 1], peer(2, o)))

    for p, (order, (low, mid, high)) in enumerate(zip(ORDERS, SPANS)):
        axis = order[2]
        opposite = lax.rem(coords[axis] + 2, 4)
        for copy, (a, b) in zip(relays[p], ((low, mid), (mid, high))):
            copy.wait_recv()
            across.append(push(region(a, b, order[:2], axis, opposite), partner))

    arrive(three)
    norm_sum[3] = norm_sum[2] + norm_got[2, 0] + norm_got[2, 1] + norm_got[2, 2]
    at = 0
    for p, (order, (base, size)) in enumerate(zip(ORDERS, HELD_PARTS)):
        value = values[p]
        for o in range(3):
            value = value + wide((c0, c1, c2)[p][o])
        for i in range(size // 16):
            norm = norm_sum[3, pl.ds(lax.div(starts[p] + i, 8), 1), :]
            shard_ref[at] = narrow(value[i] / (norm + damping))
            at += 1
    arrive(across)
    copies.finish()


def pieces(parts, lead, share, kind):
    return [pltpu.VMEM((*lead, size // share, 16, 128), kind) for _, size in parts]


def gather_call(own, targets, factor):
    copies = 9 + 9 + 12 + 3 + 6 + 6 + 6 + 2 + 3 * 12
    held, wanted = factor.shape[1], targets.shape[1]
    tiles = held // 128
    blocks = tiles * 8
    bf, f32, vmem = jnp.bfloat16, jnp.float32, pltpu.VMEM
    scratch = [
        vmem((wanted, held), f32),
        vmem((2, blocks, 16, 128), bf),
        vmem((tiles, 128), f32),
        vmem((blocks, 16, 128), bf),
        vmem((tiles, 128), f32),
        vmem((blocks, 16, 128), f32),
        vmem((blocks, 16, 128), bf),
        vmem((4, tiles, 128), f32),
        vmem((3, 3, tiles, 128), f32),
    ]
    scratch += pieces(HELD_PARTS, (3,), 4, bf) + pieces(HELD_PARTS, (3,), 16, bf)
    scratch += pieces(HELD_PARTS, (3,), 16, bf) + pieces(HELD_PARTS, (), 4, f32)
    scratch += pieces(HELD_PARTS, (), 4, bf) + pieces(HELD_PARTS, (), 16, bf)
    steps = factor.shape[0] // TILE_PTS
    scratch += [vmem((steps, TILE_PTS, held), bf), pltpu.SemaphoreType.DMA((steps,))]
    scratch += [pltpu.SemaphoreType.DMA((copies,))] * 2
    out, shard = pl.pallas_call(
        gather_kernel,
        out_shape=(
            jax.ShapeDtypeStruct((4, 2, 4, 4, *own.shape), bf),
            jax.ShapeDtypeStruct((blocks // 16, 16, 128), bf),
        ),
        in_specs=[pl.BlockSpec(memory_space=vmem)] * 2 + [pl.BlockSpec(memory_space=pl.ANY)],
        out_specs=[pl.BlockSpec(memory_space=vmem)] * 2,
        scratch_shapes=scratch,
        compiler_params=pltpu.CompilerParams(
            collective_id=2, has_side_effects=True, vmem_limit_bytes=GATHER_VMEM
        ),
        name="gather_rows",
    )(own, targets, factor)
    return out.reshape(128, *own.shape), shard


MICRO = 16


def eliminate(rows, first):
    groups = len(rows)
    sub = lax.broadcasted_iota(jnp.int32, (SUB, PANEL), 0)
    rows = [list(values) for values in rows]

    def over_sublanes(value, k):
        return jnp.broadcast_to(value[k : k + 1, :], (SUB, PANEL))

    for m in range(0, groups, MICRO // SUB):
        cols = {}
        for r in range(m, groups):
            for k in range(MICRO):
                lane = first + m * SUB + k
                cols[r, k] = jnp.broadcast_to(rows[r][0][:, lane : lane + 1], (SUB, PANEL))
        for k in range(MICRO):
            g, at = m + k // SUB, k % SUB
            if at == 0:
                roots = jnp.ones((SUB, PANEL), jnp.float32)
            root = lax.rsqrt(over_sublanes(cols[g, k], at))
            roots = jnp.where(sub == at, root, roots)
            scale = root * root
            ahead = {j: over_sublanes(cols[g, j], at) for j in range(k + 1, MICRO)}
            pivot_rows = [over_sublanes(value, at) for value in rows[g]]
            for r in range(g, groups):
                if r == g and at == SUB - 1:
                    continue
                c = cols[r, k] * scale
                if r == g:
                    c = jnp.where(sub > at, c, 0.0)
                for j in range(k + 1, MICRO):
                    cols[r, j] = cols[r, j] - c * ahead[j]
                rows[r] = [value - c * row for value, row in zip(rows[r], pivot_rows)]
            if at == SUB - 1:
                rows[g] = [value * roots for value in rows[g]]
    return rows


def panel_inverse(block):
    half, groups = PANEL // 2, PANEL // 2 // SUB
    sub = lax.broadcasted_iota(jnp.int32, (SUB, PANEL), 0)
    lane = lax.broadcasted_iota(jnp.int32, (SUB, PANEL), 1)

    def unit(row):
        return (lane == sub + row).astype(jnp.float32)

    pieces = [block[SUB * r : SUB * (r + 1), :] for r in range(2 * groups)]
    top = eliminate([(pieces[r], unit(SUB * r)) for r in range(groups)], 0)
    right = jnp.concatenate([values[0] for values in top], axis=0)
    upper = jnp.concatenate([values[1] for values in top], axis=0)
    wide = lax.broadcasted_iota(jnp.int32, (half, PANEL), 1)
    both = jnp.where(wide < half, upper, right)
    change = jnp.dot(right.T, both, precision=HIGHEST, preferred_element_type=jnp.float32)
    low = []
    for r in range(groups, 2 * groups):
        piece = jnp.where(lane < half, 0.0, pieces[r])
        low.append((piece - change[SUB * r : SUB * (r + 1), :], unit(SUB * r)))
    low = eliminate(low, half)
    lower = [jnp.where(lane < half, values[0], values[1]) for values in low]
    return jnp.concatenate([upper, *lower], axis=0)


def local_kernel(
    pad_ref, pos_ref, targets_ref, points_ref, factor_ref,
    new_ref, cross_ref, norm_ref,
    ps_ref, pf_ref, sel_ref, a_ref, w_ref, lo_ref, hi_ref, down_hi, down_lo, fbuf, fsem,
):
    tiles = fbuf.shape[0]
    loads = load_tiles(factor_ref, fbuf, fsem)
    padded = pos_ref.shape[1]
    sel_ref[...] = jnp.where(
        lax.broadcasted_iota(jnp.int32, (BLOCK, padded), 0) == pos_ref[...], 1.0, 0.0
    ).astype(jnp.bfloat16)
    ahead = ps_ref.shape[1] // 128
    for t in range(0, pad_ref.shape[1], 2):
        pair = [
            pad_ref[:, k].astype(jnp.float32).reshape(padded, 128).astype(jnp.bfloat16)
            for k in (t, t + 1)
        ]
        rows = dot_nn(sel_ref[...], jnp.concatenate(pair, axis=1)).astype(jnp.bfloat16)
        if t < ahead:
            ps_ref[:, t * 128 : (t + 2) * 128] = rows
        else:
            pf_ref[:, (t - ahead) * 128 : (t - ahead + 2) * 128] = rows

    panels = BLOCK // PANEL
    total = jnp.zeros((1, BLOCK), jnp.float32)
    for r in range(panels):
        at = slice(r * PANEL, (r + 1) * PANEL)
        inter = dot_nt(pf_ref[at, :], pf_ref[...])
        total = total + jnp.sum(jnp.abs(inter), axis=0, keepdims=True)
        kern = jnp.exp(dot_nt(ps_ref[at, :], ps_ref[...]) / ps_ref.shape[1] - 1.0)
        a_ref[at, :] = kern - inter
    shift = ridge_shift + jnp.max(total)
    eye = lax.broadcasted_iota(jnp.int32, (PANEL, PANEL), 0) == lax.broadcasted_iota(
        jnp.int32, (PANEL, PANEL), 1
    )
    for load in loads:
        load.wait()

    def exact(a, b):
        return jnp.dot(a, b, precision=HIGHEST, preferred_element_type=jnp.float32)

    for j in range(panels):
        at = slice(j * PANEL, (j + 1) * PANEL)
        inv = panel_inverse(a_ref[at, at] + jnp.where(eye, shift, 0.0))
        if j:
            done = jnp.concatenate([exact(inv, w_ref[at, : j * PANEL]), inv], axis=1)
        else:
            done = inv
        high = done.astype(jnp.bfloat16)
        hi_ref[at, : (j + 1) * PANEL] = high
        lo_ref[at, : (j + 1) * PANEL] = (done - high.astype(jnp.float32)).astype(jnp.bfloat16)
        if j + 1 < panels:
            rest = slice((j + 1) * PANEL, BLOCK)
            hi_ref[at, rest] = jnp.zeros((PANEL, BLOCK - (j + 1) * PANEL), jnp.bfloat16)
            lo_ref[at, rest] = jnp.zeros((PANEL, BLOCK - (j + 1) * PANEL), jnp.bfloat16)
            right = exact(inv, a_ref[at, rest])
            for r in range(j + 1, panels):
                rows = slice(r * PANEL, (r + 1) * PANEL)
                skip = (r - j - 1) * PANEL
                left = right[:, skip : skip + PANEL].T
                a_ref[rows, r * PANEL :] = a_ref[rows, r * PANEL :] - exact(left, right[:, skip:])
                gone = exact(left, done)
                if j:
                    w_ref[rows, : j * PANEL] = w_ref[rows, : j * PANEL] - gone[:, : j * PANEL]
                w_ref[rows, at] = -gone[:, j * PANEL :]
        tile = slice(j * TILE_PTS, (j + 1) * TILE_PTS)
        scaled = normalize(points_ref[tile, :])
        down = jnp.exp(dot_nt(ps_ref[...], scaled) / scaled.shape[1] - 1.0) - dot_nt(
            pf_ref[...], fbuf[j]
        )
        high = down.astype(jnp.bfloat16)
        down_hi[:, tile] = high
        down_lo[:, tile] = (down - high.astype(jnp.float32)).astype(jnp.bfloat16)

    half = BLOCK // 2
    wanted = targets_ref.shape[1]
    acc = jnp.zeros((wanted, BLOCK), jnp.float32)
    nsq = jnp.zeros((BLOCK, 128), jnp.float32)
    for i in range(tiles):
        tile = slice(i * TILE_PTS, (i + 1) * TILE_PTS)
        for top, wide in ((0, half), (half, BLOCK)):
            at = slice(top, top + half)
            value = (
                dot_nn(hi_ref[at, :wide], down_hi[:wide, tile])
                + dot_nn(hi_ref[at, :wide], down_lo[:wide, tile])
                + dot_nn(lo_ref[at, :wide], down_hi[:wide, tile])
            )
            new_ref[at, tile] = value.astype(jnp.bfloat16)
        new = new_ref[:, tile]
        acc = acc + dot_nt(targets_ref[tile, :].T, new)
        wide_new = new.astype(jnp.float32)
        squares = wide_new * wide_new
        for t in range(TILE_PTS // 128):
            nsq = nsq + squares[:, t * 128 : (t + 1) * 128]
    norms = jnp.sum(nsq.T, axis=0, keepdims=True)
    put_blocks(acc, norms, cross_ref, norm_ref)


def local_call(padded, positions, points, factor, targets):
    pts, held = factor.shape
    features = points.shape[1]
    tiles = BLOCK // 128
    bf, f32, vmem = jnp.bfloat16, jnp.float32, pltpu.VMEM
    return pl.pallas_call(
        local_kernel,
        out_shape=(
            jax.ShapeDtypeStruct((BLOCK, pts), bf),
            jax.ShapeDtypeStruct((2, tiles * 8, 16, 128), bf),
            jax.ShapeDtypeStruct((tiles, 128), f32),
        ),
        in_specs=[pl.BlockSpec(memory_space=vmem)] * 4 + [pl.BlockSpec(memory_space=pl.ANY)],
        out_specs=[pl.BlockSpec(memory_space=vmem)] * 3,
        scratch_shapes=[
            vmem((BLOCK, features), bf),
            vmem((BLOCK, held), bf),
            vmem((BLOCK, positions.shape[1]), bf),
            vmem((BLOCK, BLOCK), f32),
            vmem((BLOCK, BLOCK), f32),
            vmem((BLOCK, BLOCK), bf),
            vmem((BLOCK, BLOCK), bf),
            vmem((BLOCK, pts), bf),
            vmem((BLOCK, pts), bf),
            vmem((pts // TILE_PTS, TILE_PTS, held), bf),
            pltpu.SemaphoreType.DMA((pts // TILE_PTS,)),
        ],
        compiler_params=pltpu.CompilerParams(vmem_limit_bytes=LOCAL_VMEM),
        name="local_block",
    )(padded, positions, targets, points, factor)


def sums_kernel(
    shard_ref, x_ref, n_ref, factor_ref, out_ref, fit_ref, turned_ref, coef, got_last, got0, norm_got0, sum0, out0, norm_sum,
    norm_got, a0, a1, a2, b0, b1, b2, c0, c1, c2, u0, u1, u2, v0, v1, v2, send, recv,
):
    core, coords = place()
    partner = device_at(1 - core, coords)
    enter(core, coords)
    copies = Copies(send, recv)
    split = coef.shape[0] - x_ref.shape[1]
    tiles = factor_ref.shape[0] // TILE_PTS

    def peer(axis, offset):
        return device_at(core, coords, axis, offset)

    zero = [
        copies.start(x_ref.at[1 - core], got0, partner),
        copies.start(n_ref, norm_got0, partner),
    ]
    held, at = [], 0
    for order, (base, size) in zip(ORDERS, HELD_PARTS):
        piece = size // 16
        place_of = base + coords[order[0]] * (size // 4) + coords[order[1]] * piece
        for o in range(1, 4):
            held.append(
                copies.start(
                    shard_ref.at[at : at + piece], coef.at[pl.ds(place_of, piece)],
                    peer(order[1], o),
                )
            )
        coef[pl.ds(place_of, piece)] = shard_ref[at : at + piece]
        at += piece

    def fit(tiles):
        for i in tiles:
            at = slice(i * TILE_PTS, (i + 1) * TILE_PTS)
            fit_ref[at, :] = dot_nt(factor_ref[at, :], turned_ref[...])

    arrive(zero)
    sum0[...] = wide(x_ref[core]) + wide(got0[...])
    out0[...] = narrow(sum0[...])
    norm_sum[0] = n_ref[...] + norm_got0[...]
    one = []
    for p, (order, (base, size)) in enumerate(zip(ORDERS, NEW_PARTS)):
        here, piece = coords[order[0]], size // 4
        for o in range(1, 4):
            there = lax.rem(here + o, 4)
            one.append(
                copies.start(
                    out0.at[pl.ds(base + there * piece, piece)],
                    (a0, a1, a2)[p].at[o - 1],
                    peer(order[0], o),
                )
            )
    for o in range(1, 4):
        one.append(copies.start(norm_sum.at[0], norm_got.at[0, o - 1], peer(0, o)))

    arrive(held)
    held = []
    for order, (base, size) in zip(ORDERS, HELD_PARTS):
        block = coef.at[pl.ds(base + coords[order[0]] * (size // 4), size // 4)]
        for o in range(1, 4):
            held.append(copies.start(block, block, peer(order[0], o)))

    values = []
    arrive(one)
    for p, (order, (base, size)) in enumerate(zip(ORDERS, NEW_PARTS)):
        piece = size // 4
        value = sum0[pl.ds(base + coords[order[0]] * piece, piece)]
        for o in range(3):
            value = value + wide((a0, a1, a2)[p][o])
        values.append(value)
    norm_sum[1] = norm_sum[0] + norm_got[0, 0] + norm_got[0, 1] + norm_got[0, 2]
    last = []
    for stage, sent, landed in ((1, (u0, u1, u2), (b0, b1, b2)), (2, (v0, v1, v2), (c0, c1, c2))):
        line = []
        for p, order in enumerate(ORDERS):
            sent[p][...] = narrow(values[p])
            for o in range(1, 4):
                line.append(
                    copies.start(sent[p], landed[p].at[o - 1], peer(order[stage], o))
                )
        for o in range(1, 4):
            line.append(
                copies.start(norm_sum.at[stage], norm_got.at[stage, o - 1], peer(stage, o))
            )
        if stage == 1:
            arrive(held)
            last.append(copies.start(coef.at[:split], got_last.at[:split], partner))
        else:
            last[0].wait_recv()
            rows = turned_ref.shape[0] // 2
            for t in range(split // 8):
                lanes = slice(t * 128, (t + 1) * 128)
                for half, blocks in ((core, coef), (1 - core, got_last)):
                    at = pl.ds(pl.multiple_of(half * rows, rows), rows)
                    turned_ref[at, lanes] = blocks[t * 8 : (t + 1) * 8].reshape(rows, 128)
            fit(range(tiles // 2))
        arrive(line)
        for p in range(len(ORDERS)):
            for o in range(3):
                values[p] = values[p] + wide(landed[p][o])
        norm_sum[stage + 1] = (
            norm_sum[stage] + norm_got[stage, 0] + norm_got[stage, 1] + norm_got[stage, 2]
        )

    back = []
    for p, (order, (base, size)) in enumerate(zip(ORDERS, NEW_PARTS)):
        piece = size // 4
        start = base + coords[order[0]] * piece
        for i in range(piece):
            norm = norm_sum[3, pl.ds(lax.div(start + i, 8), 1), :]
            coef[split + start + i] = narrow(values[p][i] / (norm + damping))
        block = coef.at[pl.ds(split + start, piece)]
        for o in range(1, 4):
            back.append(copies.start(block, block, peer(order[0], o)))
    fit(range(tiles // 2, tiles))
    arrive(back)
    last.append(copies.start(coef.at[split:], got_last.at[split:], partner))
    out_ref[core] = coef[split:]
    last[1].wait_recv()
    out_ref[1 - core] = got_last[split:]
    copies.finish()


def sums_call(shard, cross, norms, factor, wanted):
    fresh, tiles = cross.shape[1], norms.shape[0]
    blocks = shard.shape[0] * 16 + fresh
    bf, f32, vmem = jnp.bfloat16, jnp.float32, pltpu.VMEM
    pts, held = factor.shape
    scratch = [
        vmem((wanted, held), bf),
        vmem((blocks, 16, 128), bf),
        vmem((blocks, 16, 128), bf),
        vmem((fresh, 16, 128), bf),
        vmem((tiles, 128), f32),
        vmem((fresh, 16, 128), f32),
        vmem((fresh, 16, 128), bf),
        vmem((4, tiles, 128), f32),
        vmem((3, 3, tiles, 128), f32),
    ]
    scratch += pieces(NEW_PARTS, (3,), 4, bf) * 3 + pieces(NEW_PARTS, (), 4, bf) * 2
    copies = 2 + 9 + 12 + 9 + 12 + 12 + 9 + 2
    scratch += [pltpu.SemaphoreType.DMA((copies,))] * 2
    return pl.pallas_call(
        sums_kernel,
        out_shape=(
            jax.ShapeDtypeStruct((2, fresh, 16, 128), bf),
            jax.ShapeDtypeStruct((pts, wanted), f32),
        ),
        in_specs=[pl.BlockSpec(memory_space=vmem)] * 4,
        out_specs=[pl.BlockSpec(memory_space=vmem)] * 2,
        scratch_shapes=scratch,
        compiler_params=pltpu.CompilerParams(
            collective_id=1, has_side_effects=True, vmem_limit_bytes=SUMS_VMEM
        ),
        name="sums",
    )(shard, cross, norms, factor)


def residual_kernel(new_ref, targets_ref, fit_ref, coef_ref, out_ref):
    turned = jnp.concatenate(
        [
            coef_ref[:, t * 8 : (t + 1) * 8].reshape(-1, 128)
            for t in range(coef_ref.shape[1] // 8)
        ],
        axis=1,
    )
    fitted = fit_ref[...] + dot_nn(turned, new_ref[...]).T
    out_ref[...] = wide(targets_ref[...]) - fitted


def residual_call(new, targets, fit, coef):
    pts, wanted = targets.shape
    return pl.pallas_call(
        residual_kernel,
        grid=(pts // TILE_PTS,),
        out_shape=jax.ShapeDtypeStruct((pts, wanted), jnp.float32),
        in_specs=[
            pl.BlockSpec((BLOCK, TILE_PTS), lambda i: (0, i)),
            pl.BlockSpec((TILE_PTS, wanted), lambda i: (i, 0)),
            pl.BlockSpec((TILE_PTS, wanted), lambda i: (i, 0)),
            pl.BlockSpec(coef.shape, lambda i: (0, 0, 0, 0), pipeline_mode=pl.Buffered(1)),
        ],
        out_specs=pl.BlockSpec((TILE_PTS, wanted), lambda i: (i, 0)),
        compiler_params=pltpu.CompilerParams(vmem_limit_bytes=RESIDUAL_VMEM),
        name="residual",
    )(new, targets, fit, coef)


def on_device(points, factor, targets, pivot_slots, pivot_counts):
    own = rows_call(pivot_slots, points, factor)
    padded, shard = gather_call(own, targets, factor)
    positions = padded_positions(pivot_counts, pivot_slots.shape[1])
    new_columns, cross, norms = local_call(padded, positions, points, factor, targets)
    coef, fit = sums_call(shard, cross, norms, factor, targets.shape[1])
    residual_next = residual_call(new_columns, targets, fit, coef)
    return (new_columns, residual_next)


def solution(mesh):
    return jax.shard_map(
        on_device,
        mesh=mesh,
        in_specs=(
            P(("row", "col"), None),
            P(("row", "col"), None),
            P(("row", "col"), None),
            P(("row", "col"), None),
            P(),
        ),
        out_specs=(P(None, ("row", "col")), P(("row", "col"), None)),
        check_vma=False,
    )
```

```python
import functools

import jax
import jax.numpy as jnp
from jax import lax
from jax.experimental import pallas as pl
from jax.experimental.pallas import tpu as pltpu
from jax.sharding import PartitionSpec as P

BLOCK = 512
PANEL = 128
SUB = 8
TILE_PTS = 512
ROWS_VMEM, GATHER_VMEM, LOCAL_VMEM, SUMS_VMEM, RESIDUAL_VMEM = (
    mib << 20 for mib in (62, 40, 38, 20, 16)
)
MESH = pl.DeviceIdType.MESH
HIGHEST = lax.Precision.HIGHEST

ridge_shift = 0.01
damping = 1.0
epsilon = 1e-06


def normalize(points):
    values = points.astype(jnp.float32)
    factor_scale = lax.rsqrt(jnp.mean(values * values, axis=1, keepdims=True) + epsilon)
    return (values * factor_scale).astype(jnp.bfloat16)


def dot_nt(a, b):
    return lax.dot_general(a, b, (((1,), (1,)), ((), ())), preferred_element_type=jnp.float32)


def dot_nn(a, b):
    return jnp.dot(a, b, preferred_element_type=jnp.float32)


def put_blocks(acc, norms, cross_ref, norm_ref):
    for t in range(norms.shape[1] // 128):
        lanes = slice(t * 128, (t + 1) * 128)
        norm_ref[t : t + 1, :] = norms[:, lanes]
        cross_ref[:, t * 8 : (t + 1) * 8] = (
            acc[:, lanes].astype(jnp.bfloat16).reshape(2, 8, 16, 128)
        )


ORDERS = ((0, 1, 2), (1, 2, 0), (2, 0, 1))
HELD_PARTS = ((0, 48), (48, 48), (96, 32))
NEW_PARTS = ((0, 12), (12, 12), (24, 8))


def place():
    row, col = lax.axis_index("row"), lax.axis_index("col")
    core = lax.rem(row, 2)
    coords = (lax.div(col, 4), lax.div(row, 2), lax.rem(col, 4))
    return core, coords


def device_at(core, coords, axis=0, offset=0):
    x, y, z = (
        lax.rem(c + offset, 4) if (a == axis and offset) else c for a, c in enumerate(coords)
    )
    return (y * 2 + core, x * 4 + z)


def enter(core, coords):
    barrier = pltpu.get_barrier_semaphore()
    peers = [device_at(1 - core, coords)]
    peers += [device_at(core, coords, a, o) for a in range(3) for o in range(1, 4)]
    for peer in peers:
        pl.semaphore_signal(barrier, inc=1, device_id=peer, device_id_type=MESH)
    pl.semaphore_wait(barrier, len(peers))


def load_tiles(src, buf, sem):
    loads = []
    for i in range(buf.shape[0]):
        tile = src.at[pl.ds(i * TILE_PTS, TILE_PTS), :]
        loads.append(pltpu.make_async_copy(tile, buf.at[i], sem.at[i]))
        loads[i].start()
    return loads


class Copies:
    def __init__(self, send, recv):
        self.send, self.recv, self.started = send, recv, []

    def start(self, src, dst, device):
        k = len(self.started)
        copy = pltpu.make_async_remote_copy(
            src_ref=src, dst_ref=dst, send_sem=self.send.at[k], recv_sem=self.recv.at[k],
            device_id=device, device_id_type=MESH,
        )
        copy.start()
        self.started.append(copy)
        return copy

    def finish(self):
        for copy in self.started:
            copy.wait_send()


def arrive(copies):
    for copy in copies:
        copy.wait_recv()


def wide(value):
    return value.astype(jnp.float32)


def narrow(value):
    return value.astype(jnp.bfloat16)


def rows_kernel(
    slots_ref, counts_ref, points_ref, factor_ref, out_ref, pos_ref, pbuf, fbuf, psem, fsem
):
    cap = pbuf.shape[0]
    copies = []
    for s in range(cap):
        base = pl.multiple_of(lax.div(slots_ref[0, s], SUB) * SUB, SUB)
        for src, buf, sem in ((points_ref, pbuf, psem), (factor_ref, fbuf, fsem)):
            copy = pltpu.make_async_copy(src.at[pl.ds(base, SUB), :], buf.at[s], sem.at[s])
            copy.start()
            copies.append(copy)

    owners, padded = counts_ref.shape[1], pos_ref.shape[1]
    first = cap * lax.broadcasted_iota(jnp.int32, (owners, padded), 0)
    row = lax.broadcasted_iota(jnp.int32, (owners, padded), 1)
    counts = jnp.broadcast_to(wide(counts_ref[...]), (SUB, owners)).astype(jnp.bfloat16)

    def total(mask):
        ones = jnp.where(mask, 1.0, 0.0).astype(jnp.bfloat16)
        return dot_nn(counts, ones)[:1].astype(jnp.int32)

    before = total(first + cap <= row)
    here = total((first <= row) & (row < first + cap))
    slot = jnp.bitwise_and(lax.broadcasted_iota(jnp.int32, (1, padded), 1), cap - 1)
    pos_ref[...] = jnp.where(slot < here, before + slot, -1)

    for copy in copies:
        copy.wait()

    def picked(buf):
        sub = lax.broadcasted_iota(jnp.int32, buf.shape[1:], 0)
        out = jnp.zeros(buf.shape[1:], jnp.float32)
        for s in range(cap):
            offset = lax.rem(slots_ref[0, s], SUB)
            row = jnp.sum(
                jnp.where(sub == offset, buf[s].astype(jnp.float32), 0.0), axis=0, keepdims=True
            )
            out = jnp.where(sub == s, row, out)
        return out

    both = (normalize(picked(pbuf)), picked(fbuf).astype(jnp.bfloat16))
    t = 0
    for rows in both:
        for k in range(rows.shape[1] // 128):
            out_ref[t] = rows[:, k * 128 : (k + 1) * 128]
            t += 1


def rows_call(pivot_slots, pivot_counts, points, factor):
    cap = pivot_slots.shape[1]
    features, held = points.shape[1], factor.shape[1]
    counts = pivot_counts.reshape(1, -1)
    return pl.pallas_call(
        rows_kernel,
        out_shape=(
            jax.ShapeDtypeStruct(((features + held) // 128, cap, 128), jnp.bfloat16),
            jax.ShapeDtypeStruct((1, counts.shape[1] * cap), jnp.int32),
        ),
        in_specs=[
            pl.BlockSpec(memory_space=pltpu.SMEM),
            pl.BlockSpec(memory_space=pltpu.VMEM),
            pl.BlockSpec(memory_space=pl.ANY),
            pl.BlockSpec(memory_space=pl.ANY),
        ],
        out_specs=[pl.BlockSpec(memory_space=pltpu.VMEM)] * 2,
        scratch_shapes=[
            pltpu.VMEM((cap, SUB, features), jnp.bfloat16),
            pltpu.VMEM((cap, SUB, held), jnp.bfloat16),
            pltpu.SemaphoreType.DMA((cap,)),
            pltpu.SemaphoreType.DMA((cap,)),
        ],
        compiler_params=pltpu.CompilerParams(vmem_limit_bytes=ROWS_VMEM),
        name="pivot_rows",
    )(pivot_slots, counts, points, factor)


SPANS = ((0, 4, 7), (7, 11, 14), (14, 17, 20))


def gather_kernel(
    own_ref, targets_ref, factor_ref, out_ref, shard_ref, acc_ref, x_ref, n_ref, got0, norm_got0,
    sum0, out0, norm_sum, norm_got, a0, a1, a2, b0, b1, b2, c0, c1, c2, s0, s1, s2, u0, u1, u2,
    v0, v1, v2, fbuf, fsem, send, recv,
):
    core, coords = place()
    partner = device_at(1 - core, coords)
    loads = load_tiles(factor_ref, fbuf, fsem)
    enter(core, coords)
    copies = Copies(send, recv)

    def peer(axis, offset):
        return device_at(core, coords, axis, offset)

    def region(low, high, whole=(), axis=None, at=None):
        x, y, z = (
            slice(None) if a in whole else (at if a == axis else c)
            for a, c in enumerate(coords)
        )
        return out_ref.at[y, core, x, z, low:high]

    def push(block, device):
        return copies.start(block, block, device)

    first = []
    for order, (low, _, high) in zip(ORDERS, SPANS):
        first.append([
            copies.start(own_ref.at[low:high], region(low, high), peer(order[0], o))
            for o in (2, 1, 3)
        ])
    x, y, z = coords
    out_ref[y, core, x, z] = own_ref[...]
    squares = jnp.zeros((SUB, factor_ref.shape[1]), jnp.float32)
    chunks = factor_ref.shape[0] // TILE_PTS

    def add_chunk(i, squares):
        at = slice(i * TILE_PTS, (i + 1) * TILE_PTS)
        loads[i].wait()
        value = dot_nn(targets_ref[at, :].T, fbuf[i])
        acc_ref[...] = value if i == 0 else acc_ref[...] + value
        values = wide(fbuf[i])
        return squares + jnp.sum((values * values).reshape(-1, SUB, values.shape[1]), axis=0)

    squares = add_chunk(0, squares)
    second = []
    for p, (order, (low, _, high)) in enumerate(zip(ORDERS, SPANS)):
        arrive(first[p])
        block = region(low, high, order[:1])
        second.append([push(block, peer(order[1], o)) for o in (2, 1, 3)])
    for i in range(1, chunks):
        squares = add_chunk(i, squares)
    put_blocks(acc_ref[...], jnp.sum(squares, axis=0, keepdims=True), x_ref, n_ref)
    zero = [
        copies.start(x_ref.at[1 - core], got0, partner),
        copies.start(n_ref, norm_got0, partner),
    ]
    arrive(zero)
    sum0[...] = wide(x_ref[core]) + wide(got0[...])
    out0[...] = narrow(sum0[...])
    norm_sum[0] = n_ref[...] + norm_got0[...]
    one, starts = [], []
    for p, (order, (base, size)) in enumerate(zip(ORDERS, HELD_PARTS)):
        here, piece = coords[order[0]], size // 4
        for o in range(1, 4):
            there = lax.rem(here + o, 4)
            one.append(
                copies.start(
                    out0.at[pl.ds(base + there * piece, piece)],
                    (a0, a1, a2)[p].at[o - 1],
                    peer(order[0], o),
                )
            )
        starts.append(base + here * piece)
    for o in range(1, 4):
        one.append(copies.start(norm_sum.at[0], norm_got.at[0, o - 1], peer(0, o)))

    third, across = [], []
    for p, (order, (low, mid, high)) in enumerate(zip(ORDERS, SPANS)):
        arrive(second[p])
        left, right = peer(order[2], 3), peer(order[2], 1)
        halves = [region(a, b, order[:2]) for a, b in ((low, mid), (mid, high))]
        right_low = push(halves[0], right)
        left_high = push(halves[1], left)
        right_high = push(halves[1], right)
        left_low = push(halves[0], left)
        third.append((right_low, left_high, right_high, left_low))
        across.append(push(region(low, high, order[:2]), partner))

    relays = []
    for p, (order, (low, mid, high)) in enumerate(zip(ORDERS, SPANS)):
        axis = order[2]
        before, after = (lax.rem(coords[axis] + o, 4) for o in (3, 1))
        third[p][0].wait_recv()
        relay = push(region(low, mid, order[:2], axis, before), peer(axis, 1))
        third[p][1].wait_recv()
        relays.append((relay, push(region(mid, high, order[:2], axis, after), peer(axis, 3))))

    arrive(one)
    two = []
    for p, (order, (base, size)) in enumerate(zip(ORDERS, HELD_PARTS)):
        here, piece, fours = coords[order[1]], size // 16, size // 4
        value = sum0[pl.ds(starts[p], fours)]
        for o in range(3):
            value = value + wide((a0, a1, a2)[p][o])
        (s0, s1, s2)[p][...] = value
        (u0, u1, u2)[p][...] = narrow(value)
        for o in range(1, 4):
            there = lax.rem(here + o, 4)
            two.append(
                copies.start(
                    (u0, u1, u2)[p].at[pl.ds(there * piece, piece)],
                    (b0, b1, b2)[p].at[o - 1],
                    peer(order[1], o),
                )
            )
        starts[p] = starts[p] + here * piece
    norm_sum[1] = norm_sum[0] + norm_got[0, 0] + norm_got[0, 1] + norm_got[0, 2]
    for o in range(1, 4):
        two.append(copies.start(norm_sum.at[1], norm_got.at[1, o - 1], peer(1, o)))

    for p, (order, (low, mid, high)) in enumerate(zip(ORDERS, SPANS)):
        axis = order[2]
        before, after = (lax.rem(coords[axis] + o, 4) for o in (3, 1))
        third[p][2].wait_recv()
        across.append(push(region(low, high, order[:2], axis, before), partner))
        third[p][3].wait_recv()
        across.append(push(region(low, high, order[:2], axis, after), partner))

    arrive(two)
    three, values = [], []
    for p, (order, (base, size)) in enumerate(zip(ORDERS, HELD_PARTS)):
        here, piece = coords[order[1]], size // 16
        value = (s0, s1, s2)[p][pl.ds(here * piece, piece)]
        for o in range(3):
            value = value + wide((b0, b1, b2)[p][o])
        values.append(value)
        (v0, v1, v2)[p][...] = narrow(value)
        for o in range(1, 4):
            three.append(
                copies.start((v0, v1, v2)[p], (c0, c1, c2)[p].at[o - 1], peer(order[2], o))
            )
    norm_sum[2] = norm_sum[1] + norm_got[1, 0] + norm_got[1, 1] + norm_got[1, 2]
    for o in range(1, 4):
        three.append(copies.start(norm_sum.at[2], norm_got.at[2, o - 1], peer(2, o)))

    for p, (order, (low, mid, high)) in enumerate(zip(ORDERS, SPANS)):
        axis = order[2]
        opposite = lax.rem(coords[axis] + 2, 4)
        for copy, (a, b) in zip(relays[p], ((low, mid), (mid, high))):
            copy.wait_recv()
            across.append(push(region(a, b, order[:2], axis, opposite), partner))

    arrive(three)
    norm_sum[3] = norm_sum[2] + norm_got[2, 0] + norm_got[2, 1] + norm_got[2, 2]
    at = 0
    for p, (order, (base, size)) in enumerate(zip(ORDERS, HELD_PARTS)):
        value = values[p]
        for o in range(3):
            value = value + wide((c0, c1, c2)[p][o])
        for i in range(size // 16):
            norm = norm_sum[3, pl.ds(lax.div(starts[p] + i, 8), 1), :]
            shard_ref[at] = narrow(value[i] / (norm + damping))
            at += 1
    arrive(across)
    copies.finish()


def pieces(parts, lead, share, kind):
    return [pltpu.VMEM((*lead, size // share, 16, 128), kind) for _, size in parts]


def gather_call(own, targets, factor):
    copies = 9 + 9 + 12 + 3 + 6 + 6 + 6 + 2 + 3 * 12
    held, wanted = factor.shape[1], targets.shape[1]
    tiles = held // 128
    blocks = tiles * 8
    bf, f32, vmem = jnp.bfloat16, jnp.float32, pltpu.VMEM
    scratch = [
        vmem((wanted, held), f32),
        vmem((2, blocks, 16, 128), bf),
        vmem((tiles, 128), f32),
        vmem((blocks, 16, 128), bf),
        vmem((tiles, 128), f32),
        vmem((blocks, 16, 128), f32),
        vmem((blocks, 16, 128), bf),
        vmem((4, tiles, 128), f32),
        vmem((3, 3, tiles, 128), f32),
    ]
    scratch += pieces(HELD_PARTS, (3,), 4, bf) + pieces(HELD_PARTS, (3,), 16, bf)
    scratch += pieces(HELD_PARTS, (3,), 16, bf) + pieces(HELD_PARTS, (), 4, f32)
    scratch += pieces(HELD_PARTS, (), 4, bf) + pieces(HELD_PARTS, (), 16, bf)
    steps = factor.shape[0] // TILE_PTS
    scratch += [vmem((steps, TILE_PTS, held), bf), pltpu.SemaphoreType.DMA((steps,))]
    scratch += [pltpu.SemaphoreType.DMA((copies,))] * 2
    out, shard = pl.pallas_call(
        gather_kernel,
        out_shape=(
            jax.ShapeDtypeStruct((4, 2, 4, 4, *own.shape), bf),
            jax.ShapeDtypeStruct((blocks // 16, 16, 128), bf),
        ),
        in_specs=[pl.BlockSpec(memory_space=vmem)] * 2 + [pl.BlockSpec(memory_space=pl.ANY)],
        out_specs=[pl.BlockSpec(memory_space=vmem)] * 2,
        scratch_shapes=scratch,
        compiler_params=pltpu.CompilerParams(
            collective_id=2, has_side_effects=True, vmem_limit_bytes=GATHER_VMEM
        ),
        name="gather_rows",
    )(own, targets, factor)
    return out.reshape(128, *own.shape), shard


MICRO = 16


def eliminate(rows, first):
    groups = len(rows)
    sub = lax.broadcasted_iota(jnp.int32, (SUB, PANEL), 0)
    rows = [list(values) for values in rows]

    def over_sublanes(value, k):
        return jnp.broadcast_to(value[k : k + 1, :], (SUB, PANEL))

    for m in range(0, groups, MICRO // SUB):
        cols = {}
        for r in range(m, groups):
            for k in range(MICRO):
                lane = first + m * SUB + k
                cols[r, k] = jnp.broadcast_to(rows[r][0][:, lane : lane + 1], (SUB, PANEL))
        for k in range(MICRO):
            g, at = m + k // SUB, k % SUB
            if at == 0:
                roots = jnp.ones((SUB, PANEL), jnp.float32)
            root = lax.rsqrt(over_sublanes(cols[g, k], at))
            roots = jnp.where(sub == at, root, roots)
            scale = root * root
            ahead = {j: over_sublanes(cols[g, j], at) for j in range(k + 1, MICRO)}
            pivot_rows = [over_sublanes(value, at) for value in rows[g]]
            for r in range(g, groups):
                if r == g and at == SUB - 1:
                    continue
                c = cols[r, k] * scale
                if r == g:
                    c = jnp.where(sub > at, c, 0.0)
                for j in range(k + 1, MICRO):
                    cols[r, j] = cols[r, j] - c * ahead[j]
                rows[r] = [value - c * row for value, row in zip(rows[r], pivot_rows)]
            if at == SUB - 1:
                rows[g] = [value * roots for value in rows[g]]
    return rows


def panel_inverse(block):
    half, groups = PANEL // 2, PANEL // 2 // SUB
    sub = lax.broadcasted_iota(jnp.int32, (SUB, PANEL), 0)
    lane = lax.broadcasted_iota(jnp.int32, (SUB, PANEL), 1)

    def unit(row):
        return (lane == sub + row).astype(jnp.float32)

    pieces = [block[SUB * r : SUB * (r + 1), :] for r in range(2 * groups)]
    top = eliminate([(pieces[r], unit(SUB * r)) for r in range(groups)], 0)
    right = jnp.concatenate([values[0] for values in top], axis=0)
    upper = jnp.concatenate([values[1] for values in top], axis=0)
    wide = lax.broadcasted_iota(jnp.int32, (half, PANEL), 1)
    both = jnp.where(wide < half, upper, right)
    change = jnp.dot(right.T, both, precision=HIGHEST, preferred_element_type=jnp.float32)
    low = []
    for r in range(groups, 2 * groups):
        piece = jnp.where(lane < half, 0.0, pieces[r])
        low.append((piece - change[SUB * r : SUB * (r + 1), :], unit(SUB * r)))
    low = eliminate(low, half)
    lower = [jnp.where(lane < half, values[0], values[1]) for values in low]
    return jnp.concatenate([upper, *lower], axis=0)


def local_kernel(
    pad_ref, pos_ref, targets_ref, points_ref, factor_ref,
    new_ref, cross_ref, norm_ref,
    ps_ref, pf_ref, sel_ref, a_ref, w_ref, lo_ref, hi_ref, down_hi, down_lo, fbuf, fsem,
):
    tiles = fbuf.shape[0]
    loads = load_tiles(factor_ref, fbuf, fsem)
    padded = pos_ref.shape[1]
    sel_ref[...] = jnp.where(
        lax.broadcasted_iota(jnp.int32, (BLOCK, padded), 0) == pos_ref[...], 1.0, 0.0
    ).astype(jnp.bfloat16)
    ahead = ps_ref.shape[1] // 128
    for t in range(0, pad_ref.shape[1], 2):
        pair = [
            pad_ref[:, k].astype(jnp.float32).reshape(padded, 128).astype(jnp.bfloat16)
            for k in (t, t + 1)
        ]
        rows = dot_nn(sel_ref[...], jnp.concatenate(pair, axis=1)).astype(jnp.bfloat16)
        if t < ahead:
            ps_ref[:, t * 128 : (t + 2) * 128] = rows
        else:
            pf_ref[:, (t - ahead) * 128 : (t - ahead + 2) * 128] = rows

    panels = BLOCK // PANEL
    total = jnp.zeros((1, BLOCK), jnp.float32)
    for r in range(panels):
        at = slice(r * PANEL, (r + 1) * PANEL)
        inter = dot_nt(pf_ref[at, :], pf_ref[...])
        total = total + jnp.sum(jnp.abs(inter), axis=0, keepdims=True)
        kern = jnp.exp(dot_nt(ps_ref[at, :], ps_ref[...]) / ps_ref.shape[1] - 1.0)
        a_ref[at, :] = kern - inter
    shift = ridge_shift + jnp.max(total)
    eye = lax.broadcasted_iota(jnp.int32, (PANEL, PANEL), 0) == lax.broadcasted_iota(
        jnp.int32, (PANEL, PANEL), 1
    )
    for load in loads:
        load.wait()

    def exact(a, b):
        return jnp.dot(a, b, precision=HIGHEST, preferred_element_type=jnp.float32)

    for j in range(panels):
        at = slice(j * PANEL, (j + 1) * PANEL)
        inv = panel_inverse(a_ref[at, at] + jnp.where(eye, shift, 0.0))
        if j:
            done = jnp.concatenate([exact(inv, w_ref[at, : j * PANEL]), inv], axis=1)
        else:
            done = inv
        high = done.astype(jnp.bfloat16)
        hi_ref[at, : (j + 1) * PANEL] = high
        lo_ref[at, : (j + 1) * PANEL] = (done - high.astype(jnp.float32)).astype(jnp.bfloat16)
        if j + 1 < panels:
            rest = slice((j + 1) * PANEL, BLOCK)
            hi_ref[at, rest] = jnp.zeros((PANEL, BLOCK - (j + 1) * PANEL), jnp.bfloat16)
            lo_ref[at, rest] = jnp.zeros((PANEL, BLOCK - (j + 1) * PANEL), jnp.bfloat16)
            right = exact(inv, a_ref[at, rest])
            for r in range(j + 1, panels):
                rows = slice(r * PANEL, (r + 1) * PANEL)
                skip = (r - j - 1) * PANEL
                left = right[:, skip : skip + PANEL].T
                a_ref[rows, r * PANEL :] = a_ref[rows, r * PANEL :] - exact(left, right[:, skip:])
                gone = exact(left, done)
                if j:
                    w_ref[rows, : j * PANEL] = w_ref[rows, : j * PANEL] - gone[:, : j * PANEL]
                w_ref[rows, at] = -gone[:, j * PANEL :]
        tile = slice(j * TILE_PTS, (j + 1) * TILE_PTS)
        scaled = normalize(points_ref[tile, :])
        down = jnp.exp(dot_nt(ps_ref[...], scaled) / scaled.shape[1] - 1.0) - dot_nt(
            pf_ref[...], fbuf[j]
        )
        high = down.astype(jnp.bfloat16)
        down_hi[:, tile] = high
        down_lo[:, tile] = (down - high.astype(jnp.float32)).astype(jnp.bfloat16)

    half = BLOCK // 2
    wanted = targets_ref.shape[1]
    acc = jnp.zeros((wanted, BLOCK), jnp.float32)
    nsq = jnp.zeros((BLOCK, 128), jnp.float32)
    for i in range(tiles):
        tile = slice(i * TILE_PTS, (i + 1) * TILE_PTS)
        for top, wide in ((0, half), (half, BLOCK)):
            at = slice(top, top + half)
            value = (
                dot_nn(hi_ref[at, :wide], down_hi[:wide, tile])
                + dot_nn(hi_ref[at, :wide], down_lo[:wide, tile])
                + dot_nn(lo_ref[at, :wide], down_hi[:wide, tile])
            )
            new_ref[at, tile] = value.astype(jnp.bfloat16)
        new = new_ref[:, tile]
        acc = acc + dot_nt(targets_ref[tile, :].T, new)
        wide_new = new.astype(jnp.float32)
        squares = wide_new * wide_new
        for t in range(TILE_PTS // 128):
            nsq = nsq + squares[:, t * 128 : (t + 1) * 128]
    norms = jnp.sum(nsq.T, axis=0, keepdims=True)
    put_blocks(acc, norms, cross_ref, norm_ref)


def local_call(padded, positions, points, factor, targets):
    pts, held = factor.shape
    features = points.shape[1]
    tiles = BLOCK // 128
    bf, f32, vmem = jnp.bfloat16, jnp.float32, pltpu.VMEM
    return pl.pallas_call(
        local_kernel,
        out_shape=(
            jax.ShapeDtypeStruct((BLOCK, pts), bf),
            jax.ShapeDtypeStruct((2, tiles * 8, 16, 128), bf),
            jax.ShapeDtypeStruct((tiles, 128), f32),
        ),
        in_specs=[pl.BlockSpec(memory_space=vmem)] * 4 + [pl.BlockSpec(memory_space=pl.ANY)],
        out_specs=[pl.BlockSpec(memory_space=vmem)] * 3,
        scratch_shapes=[
            vmem((BLOCK, features), bf),
            vmem((BLOCK, held), bf),
            vmem((BLOCK, positions.shape[1]), bf),
            vmem((BLOCK, BLOCK), f32),
            vmem((BLOCK, BLOCK), f32),
            vmem((BLOCK, BLOCK), bf),
            vmem((BLOCK, BLOCK), bf),
            vmem((BLOCK, pts), bf),
            vmem((BLOCK, pts), bf),
            vmem((pts // TILE_PTS, TILE_PTS, held), bf),
            pltpu.SemaphoreType.DMA((pts // TILE_PTS,)),
        ],
        compiler_params=pltpu.CompilerParams(vmem_limit_bytes=LOCAL_VMEM),
        name="local_block",
    )(padded, positions, targets, points, factor)


def sums_kernel(
    shard_ref, x_ref, n_ref, factor_ref, out_ref, fit_ref, turned_ref, coef, got_last, got0, norm_got0, sum0, out0, norm_sum,
    norm_got, a0, a1, a2, b0, b1, b2, c0, c1, c2, u0, u1, u2, v0, v1, v2, send, recv,
):
    core, coords = place()
    partner = device_at(1 - core, coords)
    enter(core, coords)
    copies = Copies(send, recv)
    split = coef.shape[0] - x_ref.shape[1]
    tiles = factor_ref.shape[0] // TILE_PTS

    def peer(axis, offset):
        return device_at(core, coords, axis, offset)

    zero = [
        copies.start(x_ref.at[1 - core], got0, partner),
        copies.start(n_ref, norm_got0, partner),
    ]
    held, at = [], 0
    for order, (base, size) in zip(ORDERS, HELD_PARTS):
        piece = size // 16
        place_of = base + coords[order[0]] * (size // 4) + coords[order[1]] * piece
        for o in range(1, 4):
            held.append(
                copies.start(
                    shard_ref.at[at : at + piece], coef.at[pl.ds(place_of, piece)],
                    peer(order[1], o),
                )
            )
        coef[pl.ds(place_of, piece)] = shard_ref[at : at + piece]
        at += piece

    def fit(tiles):
        for i in tiles:
            at = slice(i * TILE_PTS, (i + 1) * TILE_PTS)
            fit_ref[at, :] = dot_nt(factor_ref[at, :], turned_ref[...])

    arrive(zero)
    sum0[...] = wide(x_ref[core]) + wide(got0[...])
    out0[...] = narrow(sum0[...])
    norm_sum[0] = n_ref[...] + norm_got0[...]
    one = []
    for p, (order, (base, size)) in enumerate(zip(ORDERS, NEW_PARTS)):
        here, piece = coords[order[0]], size // 4
        for o in range(1, 4):
            there = lax.rem(here + o, 4)
            one.append(
                copies.start(
                    out0.at[pl.ds(base + there * piece, piece)],
                    (a0, a1, a2)[p].at[o - 1],
                    peer(order[0], o),
                )
            )
    for o in range(1, 4):
        one.append(copies.start(norm_sum.at[0], norm_got.at[0, o - 1], peer(0, o)))

    arrive(held)
    held = []
    for order, (base, size) in zip(ORDERS, HELD_PARTS):
        block = coef.at[pl.ds(base + coords[order[0]] * (size // 4), size // 4)]
        for o in range(1, 4):
            held.append(copies.start(block, block, peer(order[0], o)))

    values = []
    arrive(one)
    for p, (order, (base, size)) in enumerate(zip(ORDERS, NEW_PARTS)):
        piece = size // 4
        value = sum0[pl.ds(base + coords[order[0]] * piece, piece)]
        for o in range(3):
            value = value + wide((a0, a1, a2)[p][o])
        values.append(value)
    norm_sum[1] = norm_sum[0] + norm_got[0, 0] + norm_got[0, 1] + norm_got[0, 2]
    last = []
    for stage, sent, landed in ((1, (u0, u1, u2), (b0, b1, b2)), (2, (v0, v1, v2), (c0, c1, c2))):
        line = []
        for p, order in enumerate(ORDERS):
            sent[p][...] = narrow(values[p])
            for o in range(1, 4):
                line.append(
                    copies.start(sent[p], landed[p].at[o - 1], peer(order[stage], o))
                )
        for o in range(1, 4):
            line.append(
                copies.start(norm_sum.at[stage], norm_got.at[stage, o - 1], peer(stage, o))
            )
        if stage == 1:
            arrive(held)
            last.append(copies.start(coef.at[:split], got_last.at[:split], partner))
        else:
            last[0].wait_recv()
            rows = turned_ref.shape[0] // 2
            for t in range(split // 8):
                lanes = slice(t * 128, (t + 1) * 128)
                for half, blocks in ((core, coef), (1 - core, got_last)):
                    at = pl.ds(pl.multiple_of(half * rows, rows), rows)
                    turned_ref[at, lanes] = blocks[t * 8 : (t + 1) * 8].reshape(rows, 128)
            fit(range(tiles // 2))
        arrive(line)
        for p in range(len(ORDERS)):
            for o in range(3):
                values[p] = values[p] + wide(landed[p][o])
        norm_sum[stage + 1] = (
            norm_sum[stage] + norm_got[stage, 0] + norm_got[stage, 1] + norm_got[stage, 2]
        )

    back = []
    for p, (order, (base, size)) in enumerate(zip(ORDERS, NEW_PARTS)):
        piece = size // 4
        start = base + coords[order[0]] * piece
        for i in range(piece):
            norm = norm_sum[3, pl.ds(lax.div(start + i, 8), 1), :]
            coef[split + start + i] = narrow(values[p][i] / (norm + damping))
        block = coef.at[pl.ds(split + start, piece)]
        for o in range(1, 4):
            back.append(copies.start(block, block, peer(order[0], o)))
    fit(range(tiles // 2, tiles))
    arrive(back)
    last.append(copies.start(coef.at[split:], got_last.at[split:], partner))
    out_ref[core] = coef[split:]
    last[1].wait_recv()
    out_ref[1 - core] = got_last[split:]
    copies.finish()


def sums_call(shard, cross, norms, factor, wanted):
    fresh, tiles = cross.shape[1], norms.shape[0]
    blocks = shard.shape[0] * 16 + fresh
    bf, f32, vmem = jnp.bfloat16, jnp.float32, pltpu.VMEM
    pts, held = factor.shape
    scratch = [
        vmem((wanted, held), bf),
        vmem((blocks, 16, 128), bf),
        vmem((blocks, 16, 128), bf),
        vmem((fresh, 16, 128), bf),
        vmem((tiles, 128), f32),
        vmem((fresh, 16, 128), f32),
        vmem((fresh, 16, 128), bf),
        vmem((4, tiles, 128), f32),
        vmem((3, 3, tiles, 128), f32),
    ]
    scratch += pieces(NEW_PARTS, (3,), 4, bf) * 3 + pieces(NEW_PARTS, (), 4, bf) * 2
    copies = 2 + 9 + 12 + 9 + 12 + 12 + 9 + 2
    scratch += [pltpu.SemaphoreType.DMA((copies,))] * 2
    return pl.pallas_call(
        sums_kernel,
        out_shape=(
            jax.ShapeDtypeStruct((2, fresh, 16, 128), bf),
            jax.ShapeDtypeStruct((pts, wanted), f32),
        ),
        in_specs=[pl.BlockSpec(memory_space=vmem)] * 4,
        out_specs=[pl.BlockSpec(memory_space=vmem)] * 2,
        scratch_shapes=scratch,
        compiler_params=pltpu.CompilerParams(
            collective_id=1, has_side_effects=True, vmem_limit_bytes=SUMS_VMEM
        ),
        name="sums",
    )(shard, cross, norms, factor)


def residual_kernel(new_ref, targets_ref, fit_ref, coef_ref, out_ref):
    turned = jnp.concatenate(
        [
            coef_ref[:, t * 8 : (t + 1) * 8].reshape(-1, 128)
            for t in range(coef_ref.shape[1] // 8)
        ],
        axis=1,
    )
    fitted = fit_ref[...] + dot_nn(turned, new_ref[...]).T
    out_ref[...] = wide(targets_ref[...]) - fitted


def residual_call(new, targets, fit, coef):
    pts, wanted = targets.shape
    return pl.pallas_call(
        residual_kernel,
        grid=(pts // TILE_PTS,),
        out_shape=jax.ShapeDtypeStruct((pts, wanted), jnp.float32),
        in_specs=[
            pl.BlockSpec((BLOCK, TILE_PTS), lambda i: (0, i)),
            pl.BlockSpec((TILE_PTS, wanted), lambda i: (i, 0)),
            pl.BlockSpec((TILE_PTS, wanted), lambda i: (i, 0)),
            pl.BlockSpec(coef.shape, lambda i: (0, 0, 0, 0), pipeline_mode=pl.Buffered(1)),
        ],
        out_specs=pl.BlockSpec((TILE_PTS, wanted), lambda i: (i, 0)),
        compiler_params=pltpu.CompilerParams(vmem_limit_bytes=RESIDUAL_VMEM),
        name="residual",
    )(new, targets, fit, coef)


def on_device(points, factor, targets, pivot_slots, pivot_counts):
    own, positions = rows_call(pivot_slots, pivot_counts, points, factor)
    padded, shard = gather_call(own, targets, factor)
    new_columns, cross, norms = local_call(padded, positions, points, factor, targets)
    coef, fit = sums_call(shard, cross, norms, factor, targets.shape[1])
    residual_next = residual_call(new_columns, targets, fit, coef)
    return (new_columns, residual_next)


def solution(mesh):
    return jax.shard_map(
        on_device,
        mesh=mesh,
        in_specs=(
            P(("row", "col"), None),
            P(("row", "col"), None),
            P(("row", "col"), None),
            P(("row", "col"), None),
            P(),
        ),
        out_specs=(P(None, ("row", "col")), P(("row", "col"), None)),
        check_vma=False,
    )
```
